32 devices in a mesh: dp: 1 (over z), tp: 4 (over y), ctx: 8 (over x, core).
Axes of the slice: x: 4, y: 4, z: 1, core: 2. Of those that a mesh axis runs over, the one named last changes fastest.
The devices are a block of a 4x4x8 slice.
Arguments:
- x_tokens: bfloat16 [2048, 7168], P(('dp', 'ctx'))
- positions: int32 [2048], P(('dp', 'ctx'))
- w_dq: bfloat16 [7168, 1536], replicated
- g_q: bfloat16 [1536], replicated
- w_uq: bfloat16 [1536, 16384], P(None, 'tp')
- w_qr: bfloat16 [1536, 8192], P(None, 'tp')
- w_dkv: bfloat16 [7168, 512], replicated
- g_kv: bfloat16 [512], replicated
- w_kr: bfloat16 [7168, 64], replicated
- w_uk: bfloat16 [512, 16384], P(None, 'tp')
- w_uv: bfloat16 [512, 16384], P(None, 'tp')
- w_o: bfloat16 [16384, 7168], P('tp')
Outputs:
- output: bfloat16 [2048, 7168], P(('dp', 'ctx'))
All inputs are finite; a program needn't handle non-finite values.
Results may differ from the reference program's by a relative error of at most 0.00851559.
Values are sent between devices in bfloat16 or wider.
A program may use at most 768 MiB of HBM per device.

```python
import jax
import jax.numpy as jnp
from jax import lax

MODEL_DIM = 7168
NUM_HEADS = 128
QUERY_RANK = 1536
LATENT_RANK = 512
NOPE_DIM = 128
ROPE_DIM = 64
VALUE_DIM = 128
CTX_SIZE = 8
SEQ_LEN = 2048
QUERY_BLOCK = 64
PIECE_LEN = SEQ_LEN // (2 * CTX_SIZE)
ROPE_BASE = 10000.0
NORM_EPS = 1e-6


def draw_weight(key, fan_in, fan_out, gain):
    return (jax.random.normal(key, (fan_in, fan_out), jnp.float32) * gain).astype(jnp.bfloat16)


def draw_positions(pos_key):
    step_key, start_key = jax.random.split(pos_key)
    pos_steps = jax.random.randint(step_key, (SEQ_LEN,), 1, 3, jnp.int32)
    pos_start = jax.random.randint(start_key, (), 0, SEQ_LEN, jnp.int32)
    logical = (pos_start + jnp.cumsum(pos_steps)).astype(jnp.int32)
    pos_pieces = logical.reshape(2 * CTX_SIZE, PIECE_LEN)
    stored = jnp.stack([pos_pieces[:CTX_SIZE], pos_pieces[CTX_SIZE:][::-1]], axis=1)
    return stored.reshape(SEQ_LEN)


def setup_inputs(seed: int = 0, part: int = 0) -> dict:
    base_key = jax.random.key(seed)
    weight_keys = jax.random.split(base_key, 10)
    part_key = jax.random.fold_in(base_key, part)
    tok_key, pos_key = jax.random.split(part_key)
    x_tokens = jax.random.normal(tok_key, (SEQ_LEN, MODEL_DIM), jnp.float32).astype(jnp.bfloat16)
    out_gain = (NUM_HEADS * VALUE_DIM) ** -0.5 * SEQ_LEN ** 0.25
    return {
        'x_tokens': x_tokens,
        'positions': draw_positions(pos_key),
        'w_dq': draw_weight(weight_keys[0], MODEL_DIM, QUERY_RANK, MODEL_DIM ** -0.5),
        'g_q': jax.random.uniform(weight_keys[1], (QUERY_RANK,), jnp.float32, 0.5, 1.5).astype(jnp.bfloat16),
        'w_uq': draw_weight(weight_keys[2], QUERY_RANK, NUM_HEADS * NOPE_DIM, QUERY_RANK ** -0.5),
        'w_qr': draw_weight(weight_keys[3], QUERY_RANK, NUM_HEADS * ROPE_DIM, QUERY_RANK ** -0.5),
        'w_dkv': draw_weight(weight_keys[4], MODEL_DIM, LATENT_RANK, MODEL_DIM ** -0.5),
        'g_kv': jax.random.uniform(weight_keys[5], (LATENT_RANK,), jnp.float32, 0.5, 1.5).astype(jnp.bfloat16),
        'w_kr': draw_weight(weight_keys[6], MODEL_DIM, ROPE_DIM, MODEL_DIM ** -0.5),
        'w_uk': draw_weight(weight_keys[7], LATENT_RANK, NUM_HEADS * NOPE_DIM, LATENT_RANK ** -0.5),
        'w_uv': draw_weight(weight_keys[8], LATENT_RANK, NUM_HEADS * VALUE_DIM, LATENT_RANK ** -0.5),
        'w_o': draw_weight(weight_keys[9], NUM_HEADS * VALUE_DIM, MODEL_DIM, out_gain),
    }


def rms_norm(act_in, gain_vec):
    inv_rms = lax.rsqrt(jnp.mean(act_in * act_in, axis=-1, keepdims=True) + NORM_EPS)
    return act_in * inv_rms * gain_vec.astype(jnp.float32)


def rope_tables(pos_vals):
    half_dim = ROPE_DIM // 2
    inv_freq = ROPE_BASE ** (-jnp.arange(half_dim, dtype=jnp.float32) * 2.0 / ROPE_DIM)
    angles = pos_vals.astype(jnp.float32)[..., None] * inv_freq
    return jnp.cos(angles), jnp.sin(angles)


def apply_rope(act_in, cos_t, sin_t):
    half_dim = act_in.shape[-1] // 2
    first_half = act_in[..., :half_dim]
    second_half = act_in[..., half_dim:]
    return jnp.concatenate([first_half * cos_t - second_half * sin_t, second_half * cos_t + first_half * sin_t], axis=-1)


def reference(x_tokens, positions, w_dq, g_q, w_uq, w_qr, w_dkv, g_kv, w_kr, w_uk, w_uv, w_o):
    cos_t, sin_t = rope_tables(positions)
    c_q = rms_norm(jnp.dot(x_tokens, w_dq, preferred_element_type=jnp.float32), g_q).astype(jnp.bfloat16)
    q_nope = jnp.dot(c_q, w_uq, preferred_element_type=jnp.float32).astype(jnp.bfloat16)
    q_rot = jnp.dot(c_q, w_qr, preferred_element_type=jnp.float32).reshape(SEQ_LEN, NUM_HEADS, ROPE_DIM)
    q_pe = apply_rope(q_rot, cos_t[:, None, :], sin_t[:, None, :]).astype(jnp.bfloat16)
    c_kv = rms_norm(jnp.dot(x_tokens, w_dkv, preferred_element_type=jnp.float32), g_kv).astype(jnp.bfloat16)
    k_pe = apply_rope(jnp.dot(x_tokens, w_kr, preferred_element_type=jnp.float32), cos_t, sin_t).astype(jnp.bfloat16).astype(jnp.float32)
    k_nope = jnp.dot(c_kv, w_uk, preferred_element_type=jnp.float32).astype(jnp.bfloat16).astype(jnp.float32).reshape(SEQ_LEN, NUM_HEADS, NOPE_DIM)
    values = jnp.dot(c_kv, w_uv, preferred_element_type=jnp.float32).astype(jnp.bfloat16).astype(jnp.float32).reshape(SEQ_LEN, NUM_HEADS, VALUE_DIM)
    score_scale = (NOPE_DIM + ROPE_DIM) ** -0.5
    block_count = SEQ_LEN // QUERY_BLOCK

    def attend_block(q_block):
        qn_blk, qp_blk, qpos_blk = q_block
        scores = jnp.einsum('qhn,khn->hqk', qn_blk.astype(jnp.float32), k_nope) + jnp.einsum('qhr,kr->hqk', qp_blk.astype(jnp.float32), k_pe)
        visible = positions[None, None, :] <= qpos_blk[None, :, None]
        scores = jnp.where(visible, scores * score_scale, -jnp.inf)
        prob_tile = jax.nn.softmax(scores, axis=-1)
        return jnp.einsum('hqk,khv->qhv', prob_tile, values).astype(jnp.bfloat16)

    attn_out = lax.map(attend_block, (q_nope.reshape(block_count, QUERY_BLOCK, NUM_HEADS, NOPE_DIM), q_pe.reshape(block_count, QUERY_BLOCK, NUM_HEADS, ROPE_DIM), positions.reshape(block_count, QUERY_BLOCK)))
    attn_out = attn_out.reshape(SEQ_LEN, NUM_HEADS * VALUE_DIM)
    return jnp.dot(attn_out, w_o, preferred_element_type=jnp.float32).astype(jnp.bfloat16)
```

```python
import functools

import jax
import jax.numpy as jnp
from jax import lax
from jax.experimental import pallas as pl
from jax.experimental.pallas import tpu as pltpu
from jax.sharding import PartitionSpec as P

ROPE_BASE = 10000.0
NORM_EPS = 1e-6
NEG_BIG = -1e30


def rms_norm(act_in, gain_vec):
    inv_rms = lax.rsqrt(jnp.mean(act_in * act_in, axis=-1, keepdims=True) + NORM_EPS)
    return act_in * inv_rms * gain_vec.astype(jnp.float32)


def rope_tables(pos_vals, rope_dim):
    half_dim = rope_dim // 2
    inv_freq = ROPE_BASE ** (-jnp.arange(half_dim, dtype=jnp.float32) * 2.0 / rope_dim)
    angles = pos_vals.astype(jnp.float32)[..., None] * inv_freq
    return jnp.cos(angles), jnp.sin(angles)


def apply_rope(act_in, cos_t, sin_t):
    half_dim = act_in.shape[-1] // 2
    first_half = act_in[..., :half_dim]
    second_half = act_in[..., half_dim:]
    return jnp.concatenate([first_half * cos_t - second_half * sin_t, second_half * cos_t + first_half * sin_t], axis=-1)


def project_tokens(tok_x, tok_pos, w_dq, g_q, w_uq, w_qr, w_dkv, g_kv, w_kr, heads_loc):
    rope_dim = w_kr.shape[1]
    tok_count = tok_x.shape[0]
    cos_t, sin_t = rope_tables(tok_pos, rope_dim)
    c_q = rms_norm(jnp.dot(tok_x, w_dq, preferred_element_type=jnp.float32), g_q).astype(jnp.bfloat16)
    q_nope = jnp.dot(c_q, w_uq, preferred_element_type=jnp.float32).astype(jnp.bfloat16).reshape(tok_count, heads_loc, -1)
    q_rot = jnp.dot(c_q, w_qr, preferred_element_type=jnp.float32).reshape(tok_count, heads_loc, rope_dim)
    q_pe = apply_rope(q_rot, cos_t[:, None, :], sin_t[:, None, :]).astype(jnp.bfloat16)
    c_kv = rms_norm(jnp.dot(tok_x, w_dkv, preferred_element_type=jnp.float32), g_kv).astype(jnp.bfloat16)
    k_pe = apply_rope(jnp.dot(tok_x, w_kr, preferred_element_type=jnp.float32), cos_t, sin_t).astype(jnp.bfloat16)
    return q_nope, q_pe, c_kv, k_pe


def up_project(lat_rows, w_uk, w_uv, heads_loc):
    row_count = lat_rows.shape[0]
    k_nope = jnp.dot(lat_rows, w_uk, preferred_element_type=jnp.float32).astype(jnp.bfloat16).reshape(row_count, heads_loc, -1)
    v_rows = jnp.dot(lat_rows, w_uv, preferred_element_type=jnp.float32).astype(jnp.bfloat16).reshape(row_count, heads_loc, -1)
    return k_nope, v_rows


def block_scores(q_nope, q_pe, k_nope, k_pe, score_scale):
    nope_part = jnp.einsum('qhn,khn->hqk', q_nope, k_nope, preferred_element_type=jnp.float32)
    rope_part = jnp.einsum('qhr,kr->hqk', q_pe, k_pe, preferred_element_type=jnp.float32)
    return (nope_part + rope_part) * score_scale


def block_stats(scores, v_rows):
    blk_max = jnp.max(scores, axis=-1)
    prob_tile = jnp.exp(scores - blk_max[..., None])
    blk_sum = jnp.sum(prob_tile, axis=-1)
    blk_acc = jnp.einsum('hqk,khv->hqv', prob_tile.astype(jnp.bfloat16), v_rows, preferred_element_type=jnp.float32)
    return blk_max, blk_sum, blk_acc


def merge_stats(run_state, update):
    old_max, old_sum, old_acc = run_state
    new_max, new_sum, new_acc = update
    top_max = jnp.maximum(old_max, new_max)
    old_w = jnp.exp(old_max - top_max)
    new_w = jnp.exp(new_max - top_max)
    return top_max, old_sum * old_w + new_sum * new_w, old_acc * old_w[..., None] + new_acc * new_w[..., None]


MESH = pl.DeviceIdType.MESH
OUT_BLOCK = 512
W_SLOTS = 3


def out_kernel(n_tp, n_blk, o_ref, w_hbm, out_hbm, wbuf, part, recv, ybuf, w_sem, rs_send, rs_recv, ag_send, ag_recv, out_sem):
    me = lax.axis_index('tp')
    right = lax.rem(me + 1, n_tp)
    left = lax.rem(me + n_tp - 1, n_tp)
    peer = (right, left)
    step_of = (n_tp - 1, 1)
    blk = wbuf.shape[2]
    rows = part.shape[2]
    n_pair = n_blk // 2

    def w_copy(b):
        return pltpu.make_async_copy(w_hbm.at[:, pl.ds(pl.multiple_of(b * blk, blk), blk)], wbuf.at[lax.rem(b, W_SLOTS)], w_sem.at[lax.rem(b, W_SLOTS)])

    def chunk_at(way, hop):
        return lax.rem(me + (hop + 1) * step_of[way], n_tp)

    def rs_copy(b, way, hop):
        src = part.at[b, chunk_at(way, 0)] if hop == 0 else recv.at[b, hop - 1]
        return pltpu.make_async_remote_copy(src_ref=src, dst_ref=recv.at[b, hop], send_sem=rs_send.at[b, hop], recv_sem=rs_recv.at[b, hop],
                                            device_id={'tp': peer[way]}, device_id_type=MESH)

    def ag_copy(b, slot, way, chunk):
        return pltpu.make_async_remote_copy(src_ref=ybuf.at[chunk, b], dst_ref=ybuf.at[chunk, b], send_sem=ag_send.at[b, slot], recv_sem=ag_recv.at[b, slot],
                                            device_id={'tp': peer[way]}, device_id_type=MESH)

    def out_copy(b, chunk):
        return pltpu.make_async_copy(ybuf.at[chunk, b], out_hbm.at[pl.ds(pl.multiple_of(chunk * rows, rows), rows), pl.ds(pl.multiple_of(b * blk, blk), blk)],
                                     out_sem.at[chunk, b])

    for b in range(W_SLOTS):
        w_copy(b).start()
    barrier = pltpu.get_barrier_semaphore()
    for neighbour in peer:
        pl.semaphore_signal(barrier, inc=1, device_id={'tp': neighbour}, device_id_type=MESH)
    pl.semaphore_wait(barrier, 2)

    def product(p, _):
        for way in range(2):
            b = 2 * p + way
            w_copy(b).wait()
            res = jnp.dot(o_ref[...], wbuf[lax.rem(b, W_SLOTS)], preferred_element_type=jnp.float32)
            part[b] = res.reshape(n_tp, rows, blk)

            @pl.when(b + W_SLOTS < n_blk)
            def _():
                w_copy(b + W_SLOTS).start()

            rs_copy(b, way, 0).start()
        return 0

    lax.fori_loop(0, n_pair, product, 0)

    for hop in range(1, n_tp - 1):
        def forward(p, _):
            for way in range(2):
                b = 2 * p + way
                rs_copy(b, way, hop - 1).wait_recv()
                recv[b, hop - 1] = recv[b, hop - 1] + part[b, chunk_at(way, hop)]
            for way in range(2):
                rs_copy(2 * p + way, way, hop).start()
            return 0

        lax.fori_loop(0, n_pair, forward, 0)

    def relay(p):
        ag_copy(2 * p, 0, 0, left).wait_recv()
        ag_copy(2 * p, 2, 0, left).start()
        ag_copy(2 * p + 1, 1, 1, right).wait_recv()
        ag_copy(2 * p + 1, 2, 1, right).start()
        out_copy(2 * p, left).start()
        out_copy(2 * p + 1, right).start()

    def finish(p, _):
        for way in range(2):
            b = 2 * p + way
            rs_copy(b, way, n_tp - 2).wait_recv()
            ybuf[me, b] = (recv[b, n_tp - 2] + part[b, me]).astype(ybuf.dtype)
        for way in range(2):
            b = 2 * p + way
            ag_copy(b, 0, 0, me).start()
            ag_copy(b, 1, 1, me).start()
            out_copy(b, me).start()

        @pl.when(p > 0)
        def _():
            relay(p - 1)
        return 0

    lax.fori_loop(0, n_pair, finish, 0)
    relay(n_pair - 1)

    def drain(p, _):
        ag_copy(2 * p, 1, 1, right).wait_recv()
        out_copy(2 * p, right).start()
        ag_copy(2 * p + 1, 0, 0, left).wait_recv()
        out_copy(2 * p + 1, left).start()
        for way in range(2):
            b = 2 * p + way
            ag_copy(b, 2, way, lax.rem(me + 2, n_tp)).wait_recv()
            out_copy(b, lax.rem(me + 2, n_tp)).start()
        return 0

    lax.fori_loop(0, n_pair, drain, 0)

    def settle(p, _):
        for way in range(2):
            b = 2 * p + way
            for hop in range(n_tp - 1):
                rs_copy(b, way, hop).wait_send()
            ag_copy(b, 0, 0, me).wait_send()
            ag_copy(b, 1, 1, me).wait_send()
            ag_copy(b, 2, way, left if way == 0 else right).wait_send()
            for chunk in range(n_tp):
                out_copy(b, chunk).wait()
        return 0

    lax.fori_loop(0, n_pair, settle, 0)


def project_out(attn_out, w_o, n_tp):
    tok_count, depth = attn_out.shape
    width = w_o.shape[1]
    n_blk = width // OUT_BLOCK
    assert n_tp == 4 and n_blk % 2 == 0 and width % OUT_BLOCK == 0
    rows = tok_count // n_tp
    dma = pltpu.SemaphoreType.DMA
    return pl.pallas_call(
        functools.partial(out_kernel, n_tp, n_blk),
        out_shape=jax.ShapeDtypeStruct((tok_count, width), jnp.bfloat16),
        in_specs=[pl.BlockSpec(memory_space=pltpu.VMEM), pl.BlockSpec(memory_space=pl.ANY)],
        out_specs=pl.BlockSpec(memory_space=pl.ANY),
        scratch_shapes=[
            pltpu.VMEM((W_SLOTS, depth, OUT_BLOCK), jnp.bfloat16),
            pltpu.VMEM((n_blk, n_tp, rows, OUT_BLOCK), jnp.float32),
            pltpu.VMEM((n_blk, n_tp - 1, rows, OUT_BLOCK), jnp.float32),
            pltpu.VMEM((n_tp, n_blk, rows, OUT_BLOCK), jnp.bfloat16),
            dma((W_SLOTS,)), dma((n_blk, n_tp - 1)), dma((n_blk, n_tp - 1)), dma((n_blk, 3)), dma((n_blk, 3)), dma((n_tp, n_blk)),
        ],
        compiler_params=pltpu.CompilerParams(collective_id=1, has_side_effects=True, vmem_limit_bytes=60 * 1024 * 1024),
        name='out_proj',
    )(attn_out, w_o)


def solution(mesh):
    ctx_count = mesh.shape['ctx']
    next_perm = [(src, (src + 1) % ctx_count) for src in range(ctx_count)]
    tok_spec = P(('dp', 'ctx'), None)
    pos_spec = P(('dp', 'ctx'))
    full_mat = P(None, None)
    full_vec = P(None)
    col_spec = P(None, 'tp')
    row_spec = P('tp', None)

    def local_step(tok_x, tok_pos, w_dq, g_q, w_uq, w_qr, w_dkv, g_kv, w_kr, w_uk, w_uv, w_o):
        my_index = lax.axis_index('ctx')
        half_len = tok_x.shape[0] // 2
        rope_dim = w_kr.shape[1]
        heads_loc = w_qr.shape[1] // rope_dim
        nope_dim = w_uq.shape[1] // heads_loc
        value_dim = w_uv.shape[1] // heads_loc
        score_scale = (nope_dim + rope_dim) ** -0.5
        q_nope, q_pe, c_kv, k_pe = project_tokens(tok_x, tok_pos, w_dq, g_q, w_uq, w_qr, w_dkv, g_kv, w_kr, heads_loc)
        k_nope, v_rows = up_project(c_kv, w_uk, w_uv, heads_loc)
        scores = block_scores(q_nope, q_pe, k_nope, k_pe, score_scale)
        visible = tok_pos[None, :] <= tok_pos[:, None]
        run_state = block_stats(jnp.where(visible[None], scores, NEG_BIG), v_rows)

        def attend_lower(lat_blk, rot_blk, run_state):
            k_low, v_low = up_project(lat_blk[:half_len], w_uk, w_uv, heads_loc)
            update = block_stats(block_scores(q_nope, q_pe, k_low, rot_blk[:half_len], score_scale), v_low)
            return merge_stats(run_state, update)

        def attend_upper(lat_blk, rot_blk, run_state):
            k_both, v_both = up_project(lat_blk, w_uk, w_uv, heads_loc)
            update = block_stats(block_scores(q_nope[half_len:], q_pe[half_len:], k_both, rot_blk, score_scale), v_both)
            old_max, old_sum, old_acc = run_state
            top_max, top_sum, top_acc = merge_stats((old_max[:, half_len:], old_sum[:, half_len:], old_acc[:, half_len:]), update)
            return (jnp.concatenate([old_max[:, :half_len], top_max], axis=1),
                    jnp.concatenate([old_sum[:, :half_len], top_sum], axis=1),
                    jnp.concatenate([old_acc[:, :half_len], top_acc], axis=1))

        def ctx_step(hop_idx, loop_carry):
            lat_blk, rot_blk, run_state = loop_carry
            lat_blk = lax.ppermute(lat_blk, 'ctx', next_perm)
            rot_blk = lax.ppermute(rot_blk, 'ctx', next_perm)
            src_index = (my_index - hop_idx) % ctx_count
            run_state = lax.cond(src_index < my_index, attend_lower, attend_upper, lat_blk, rot_blk, run_state)
            return lat_blk, rot_blk, run_state

        loop_carry = lax.fori_loop(1, ctx_count, ctx_step, (c_kv, k_pe, run_state))
        run_max, run_sum, run_acc = loop_carry[2]
        attn_out = (run_acc / run_sum[..., None]).astype(jnp.bfloat16)
        attn_out = jnp.transpose(attn_out, (1, 0, 2)).reshape(tok_x.shape[0], -1)
        return project_out(attn_out, w_o, mesh.shape['tp'])

    return jax.shard_map(local_step, mesh=mesh,
                         in_specs=(tok_spec, pos_spec, full_mat, full_vec, col_spec, col_spec, full_mat, full_vec, full_mat, col_spec, col_spec, row_spec),
                         out_specs=tok_spec, check_vma=False)
```

```python
import functools

import jax
import jax.numpy as jnp
from jax import lax
from jax.experimental import pallas as pl
from jax.experimental.pallas import tpu as pltpu
from jax.sharding import PartitionSpec as P

ROPE_BASE = 10000.0
NORM_EPS = 1e-6


def rms_norm(act_in, gain_vec):
    inv_rms = lax.rsqrt(jnp.mean(act_in * act_in, axis=-1, keepdims=True) + NORM_EPS)
    return act_in * inv_rms * gain_vec.astype(jnp.float32)


def rope_tables(pos_vals, rope_dim):
    half_dim = rope_dim // 2
    inv_freq = ROPE_BASE ** (-jnp.arange(half_dim, dtype=jnp.float32) * 2.0 / rope_dim)
    angles = pos_vals.astype(jnp.float32)[..., None] * inv_freq
    return jnp.cos(angles), jnp.sin(angles)


def apply_rope(act_in, cos_t, sin_t):
    half_dim = act_in.shape[-1] // 2
    first_half = act_in[..., :half_dim]
    second_half = act_in[..., half_dim:]
    return jnp.concatenate([first_half * cos_t - second_half * sin_t, second_half * cos_t + first_half * sin_t], axis=-1)


MESH = pl.DeviceIdType.MESH
OUT_BLOCK = 512
W_SLOTS = 3


def out_kernel(n_tp, n_blk, o_ref, w_hbm, out_hbm, wbuf, part, recv, ybuf, w_sem, rs_send, rs_recv, ag_send, ag_recv, out_sem):
    me = lax.axis_index('tp')
    right = lax.rem(me + 1, n_tp)
    left = lax.rem(me + n_tp - 1, n_tp)
    peer = (right, left)
    step_of = (n_tp - 1, 1)
    blk = wbuf.shape[2]
    rows = part.shape[2]
    n_pair = n_blk // 2

    def w_copy(b):
        return pltpu.make_async_copy(w_hbm.at[:, pl.ds(pl.multiple_of(b * blk, blk), blk)], wbuf.at[lax.rem(b, W_SLOTS)], w_sem.at[lax.rem(b, W_SLOTS)])

    def chunk_at(way, hop):
        return lax.rem(me + (hop + 1) * step_of[way], n_tp)

    def rs_copy(b, way, hop):
        src = part.at[b, chunk_at(way, 0)] if hop == 0 else recv.at[b, hop - 1]
        return pltpu.make_async_remote_copy(src_ref=src, dst_ref=recv.at[b, hop], send_sem=rs_send.at[b, hop], recv_sem=rs_recv.at[b, hop],
                                            device_id={'tp': peer[way]}, device_id_type=MESH)

    def ag_copy(b, slot, way, chunk):
        return pltpu.make_async_remote_copy(src_ref=ybuf.at[chunk, b], dst_ref=ybuf.at[chunk, b], send_sem=ag_send.at[b, slot], recv_sem=ag_recv.at[b, slot],
                                            device_id={'tp': peer[way]}, device_id_type=MESH)

    def out_copy(b, chunk):
        return pltpu.make_async_copy(ybuf.at[chunk, b], out_hbm.at[pl.ds(pl.multiple_of(chunk * rows, rows), rows), pl.ds(pl.multiple_of(b * blk, blk), blk)],
                                     out_sem.at[chunk, b])

    for b in range(W_SLOTS):
        w_copy(b).start()
    barrier = pltpu.get_barrier_semaphore()
    for neighbour in peer:
        pl.semaphore_signal(barrier, inc=1, device_id={'tp': neighbour}, device_id_type=MESH)
    pl.semaphore_wait(barrier, 2)

    def product(p, _):
        for way in range(2):
            b = 2 * p + way
            w_copy(b).wait()
            res = jnp.dot(o_ref[...], wbuf[lax.rem(b, W_SLOTS)], preferred_element_type=jnp.float32)
            part[b] = res.reshape(n_tp, rows, blk)

            @pl.when(b + W_SLOTS < n_blk)
            def _():
                w_copy(b + W_SLOTS).start()

            rs_copy(b, way, 0).start()
        return 0

    lax.fori_loop(0, n_pair, product, 0)

    for hop in range(1, n_tp - 1):
        def forward(p, _):
            for way in range(2):
                b = 2 * p + way
                rs_copy(b, way, hop - 1).wait_recv()
                recv[b, hop - 1] = recv[b, hop - 1] + part[b, chunk_at(way, hop)]
            for way in range(2):
                rs_copy(2 * p + way, way, hop).start()
            return 0

        lax.fori_loop(0, n_pair, forward, 0)

    def relay(p):
        ag_copy(2 * p, 0, 0, left).wait_recv()
        ag_copy(2 * p, 2, 0, left).start()
        ag_copy(2 * p + 1, 1, 1, right).wait_recv()
        ag_copy(2 * p + 1, 2, 1, right).start()
        out_copy(2 * p, left).start()
        out_copy(2 * p + 1, right).start()

    def finish(p, _):
        for way in range(2):
            b = 2 * p + way
            rs_copy(b, way, n_tp - 2).wait_recv()
            ybuf[me, b] = (recv[b, n_tp - 2] + part[b, me]).astype(ybuf.dtype)
        for way in range(2):
            b = 2 * p + way
            ag_copy(b, 0, 0, me).start()
            ag_copy(b, 1, 1, me).start()
            out_copy(b, me).start()

        @pl.when(p > 0)
        def _():
            relay(p - 1)
        return 0

    lax.fori_loop(0, n_pair, finish, 0)
    relay(n_pair - 1)

    def drain(p, _):
        ag_copy(2 * p, 1, 1, right).wait_recv()
        out_copy(2 * p, right).start()
        ag_copy(2 * p + 1, 0, 0, left).wait_recv()
        out_copy(2 * p + 1, left).start()
        for way in range(2):
            b = 2 * p + way
            ag_copy(b, 2, way, lax.rem(me + 2, n_tp)).wait_recv()
            out_copy(b, lax.rem(me + 2, n_tp)).start()
        return 0

    lax.fori_loop(0, n_pair, drain, 0)

    def settle(p, _):
        for way in range(2):
            b = 2 * p + way
            for hop in range(n_tp - 1):
                rs_copy(b, way, hop).wait_send()
            ag_copy(b, 0, 0, me).wait_send()
            ag_copy(b, 1, 1, me).wait_send()
            ag_copy(b, 2, way, left if way == 0 else right).wait_send()
            for chunk in range(n_tp):
                out_copy(b, chunk).wait()
        return 0

    lax.fori_loop(0, n_pair, settle, 0)


def project_out(attn_out, w_o, n_tp):
    tok_count, depth = attn_out.shape
    width = w_o.shape[1]
    n_blk = width // OUT_BLOCK
    assert n_tp == 4 and n_blk % 2 == 0 and width % OUT_BLOCK == 0
    rows = tok_count // n_tp
    dma = pltpu.SemaphoreType.DMA
    return pl.pallas_call(
        functools.partial(out_kernel, n_tp, n_blk),
        out_shape=jax.ShapeDtypeStruct((tok_count, width), jnp.bfloat16),
        in_specs=[pl.BlockSpec(memory_space=pltpu.VMEM), pl.BlockSpec(memory_space=pl.ANY)],
        out_specs=pl.BlockSpec(memory_space=pl.ANY),
        scratch_shapes=[
            pltpu.VMEM((W_SLOTS, depth, OUT_BLOCK), jnp.bfloat16),
            pltpu.VMEM((n_blk, n_tp, rows, OUT_BLOCK), jnp.float32),
            pltpu.VMEM((n_blk, n_tp - 1, rows, OUT_BLOCK), jnp.float32),
            pltpu.VMEM((n_tp, n_blk, rows, OUT_BLOCK), jnp.bfloat16),
            dma((W_SLOTS,)), dma((n_blk, n_tp - 1)), dma((n_blk, n_tp - 1)), dma((n_blk, 3)), dma((n_blk, 3)), dma((n_tp, n_blk)),
        ],
        compiler_params=pltpu.CompilerParams(collective_id=1, has_side_effects=True, vmem_limit_bytes=60 * 1024 * 1024),
        name='out_proj',
    )(attn_out, w_o)


KEY_BLOCK = 256


def attend_kernel(n_ctx, scale, q_ref, lat_ref, kpe_ref, wuk_hbm, wuv_hbm, o_ref, wuk, wuv, wuv_t, lat_t, kcat, v_t, s_buf, p_buf, w_sem):
    me = lax.axis_index('ctx')
    col = me // 2
    part = lax.rem(me, 2)
    n_col = n_ctx // 2
    heads = q_ref.shape[0]
    n_pair = heads // 2
    rank = lat_ref.shape[1]
    v_dim = v_t.shape[0] // 2
    nope = wuk.shape[2] // 2
    rope = kpe_ref.shape[1]
    exp_scale = scale * 1.4426950408889634

    def w_copy(src, dst, which, hp):
        cols = dst.shape[2]
        return pltpu.make_async_copy(src.at[:, pl.ds(pl.multiple_of((part * n_pair + hp) * cols, cols), cols)], dst.at[hp], w_sem.at[which, hp])

    for hp in range(n_pair):
        w_copy(wuk_hbm, wuk, 0, hp).start()
        w_copy(wuv_hbm, wuv, 1, hp).start()
    for blk in range(lat_ref.shape[0] // KEY_BLOCK):
        lat_t[:, blk * KEY_BLOCK:(blk + 1) * KEY_BLOCK] = lat_ref[blk * KEY_BLOCK:(blk + 1) * KEY_BLOCK].T
        for g in range(2):
            kcat[g, blk * KEY_BLOCK:(blk + 1) * KEY_BLOCK, nope:nope + rope] = kpe_ref[blk * KEY_BLOCK:(blk + 1) * KEY_BLOCK]
    for hp in range(n_pair):
        w_copy(wuk_hbm, wuk, 0, hp).wait()
        w_copy(wuv_hbm, wuv, 1, hp).wait()
        wuv_t[hp] = wuv[hp].T

    def phase(sel, n_blk):
        q_cols = slice(sel * KEY_BLOCK, (sel + 1) * KEY_BLOCK)
        key_i = lax.broadcasted_iota(jnp.int32, (KEY_BLOCK, KEY_BLOCK), 0)
        q_i = lax.broadcasted_iota(jnp.int32, (KEY_BLOCK, KEY_BLOCK), 1)
        visible = key_i <= q_i

        def pair_step(hp, _):
            for blk in range(n_blk):
                rows = slice(blk * KEY_BLOCK, (blk + 1) * KEY_BLOCK)
                k2 = jnp.dot(lat_ref[rows], wuk[hp], preferred_element_type=jnp.float32).astype(jnp.bfloat16)
                kcat[0, rows, 0:nope] = k2[:, :nope]
                kcat[1, rows, 0:nope] = k2[:, nope:]
                v_t[:, rows] = jnp.dot(wuv_t[hp], lat_t[:, rows], preferred_element_type=jnp.float32).astype(jnp.bfloat16)
            top = []
            for g in range(2):
                q_t = q_ref[2 * hp + g, :, q_cols]
                top8 = None
                for blk in range(n_blk):
                    rows = slice(blk * KEY_BLOCK, (blk + 1) * KEY_BLOCK)
                    s = jnp.dot(kcat[g, rows, 0:nope + rope], q_t, preferred_element_type=jnp.float32)
                    if blk == n_blk - 1:
                        s = jnp.where(visible, s, -1e30)
                    s_buf[g, rows] = s
                    blk8 = jnp.max(s.reshape(KEY_BLOCK // 8, 8, KEY_BLOCK), axis=0)
                    top8 = blk8 if top8 is None else jnp.maximum(top8, blk8)
                top.append(jnp.max(top8, axis=0, keepdims=True) * exp_scale)
            for g in range(2):
                sum8 = None
                for blk in range(n_blk):
                    rows = slice(blk * KEY_BLOCK, (blk + 1) * KEY_BLOCK)
                    p = jnp.exp2(s_buf[g, rows] * exp_scale - top[g])
                    blk8 = jnp.sum(p.reshape(KEY_BLOCK // 8, 8, KEY_BLOCK), axis=0)
                    sum8 = blk8 if sum8 is None else sum8 + blk8
                    p_buf[g, rows] = p.astype(jnp.bfloat16)
                total = jnp.sum(sum8, axis=0, keepdims=True)
                o_t = jnp.dot(v_t[g * v_dim:(g + 1) * v_dim, 0:n_blk * KEY_BLOCK], p_buf[g, 0:n_blk * KEY_BLOCK], preferred_element_type=jnp.float32)
                o_ref[q_cols, pl.ds(pl.multiple_of((2 * hp + g) * v_dim, v_dim), v_dim)] = (o_t / total).T.astype(o_ref.dtype)
            return 0

        lax.fori_loop(0, n_pair, pair_step, 0)

    for v in range(n_col):
        pl.when(col == v)(functools.partial(phase, 0, v + 1))
    for v in range(n_col):
        pl.when(col == v)(functools.partial(phase, 1, 2 * n_col - v))


def attend(q_t, lat, kpe, w_uk, w_uv, n_ctx, scale):
    heads, q_dim, q_count = q_t.shape
    keys, rank = lat.shape
    rope = kpe.shape[1]
    nope = q_dim - rope
    v_dim = w_uv.shape[1] // (2 * heads)
    n_pair = heads // 2
    bf16, f32 = jnp.bfloat16, jnp.float32
    vmem = pl.BlockSpec(memory_space=pltpu.VMEM)
    hbm = pl.BlockSpec(memory_space=pl.ANY)
    assert q_count == 2 * KEY_BLOCK and keys == n_ctx * KEY_BLOCK
    return pl.pallas_call(
        functools.partial(attend_kernel, n_ctx, scale),
        out_shape=jax.ShapeDtypeStruct((q_count, heads * v_dim), bf16),
        in_specs=[vmem, vmem, vmem, hbm, hbm],
        out_specs=vmem,
        scratch_shapes=[
            pltpu.VMEM((n_pair, rank, 2 * nope), bf16), pltpu.VMEM((n_pair, rank, 2 * v_dim), bf16), pltpu.VMEM((n_pair, 2 * v_dim, rank), bf16),
            pltpu.VMEM((rank, keys), bf16), pltpu.VMEM((2, keys, nope + rope), bf16), pltpu.VMEM((2 * v_dim, keys), bf16),
            pltpu.VMEM((2, keys, KEY_BLOCK), f32), pltpu.VMEM((2, keys, KEY_BLOCK), bf16),
            pltpu.SemaphoreType.DMA((2, n_pair)),
        ],
        compiler_params=pltpu.CompilerParams(vmem_limit_bytes=60 * 1024 * 1024),
        name='attend',
    )(q_t, lat, kpe, w_uk, w_uv)


def solution(mesh):
    tok_spec = P(('dp', 'ctx'), None)
    pos_spec = P(('dp', 'ctx'))
    full_mat = P(None, None)
    full_vec = P(None)
    col_spec = P(None, 'tp')
    row_spec = P('tp', None)

    def local_step(tok_x, tok_pos, w_dq, g_q, w_uq, w_qr, w_dkv, g_kv, w_kr, w_uk, w_uv, w_o):
        my_index = lax.axis_index('ctx')
        half_len = tok_x.shape[0] // 2
        rope_dim = w_kr.shape[1]
        heads_loc = w_qr.shape[1] // rope_dim
        nope_dim = w_uq.shape[1] // heads_loc
        value_dim = w_uv.shape[1] // heads_loc
        score_scale = (nope_dim + rope_dim) ** -0.5
        n_ctx = mesh.shape['ctx']
        heads_half = heads_loc // 2
        part = my_index % 2
        swap = [(i, i ^ 1) for i in range(n_ctx)]
        cos_t, sin_t = rope_tables(tok_pos, rope_dim)
        c_kv = rms_norm(jnp.dot(tok_x, w_dkv, preferred_element_type=jnp.float32), g_kv).astype(jnp.bfloat16)
        k_pe = apply_rope(jnp.dot(tok_x, w_kr, preferred_element_type=jnp.float32), cos_t, sin_t).astype(jnp.bfloat16)
        c_q = rms_norm(jnp.dot(tok_x, w_dq, preferred_element_type=jnp.float32), g_q).astype(jnp.bfloat16)

        def in_order(rows):
            rows = lax.all_gather(rows, 'ctx')
            halves = rows.reshape((n_ctx, 2, half_len) + rows.shape[2:])
            return jnp.concatenate([halves[:, 0], halves[::-1, 1]], axis=0).reshape((-1,) + rows.shape[2:])

        def pair_rows(own):
            other = lax.ppermute(own, 'ctx', swap)
            even = jnp.where(part == 0, own, other)
            odd = jnp.where(part == 0, other, own)
            return jnp.concatenate([even[:half_len], odd[:half_len], odd[half_len:], even[half_len:]], axis=0)

        lat_all = in_order(c_kv)
        kpe_all = in_order(k_pe)
        c_q2 = pair_rows(c_q)
        cos_2, sin_2 = rope_tables(pair_rows(tok_pos[:, None])[:, 0], rope_dim)
        w_uq_half = lax.dynamic_slice_in_dim(w_uq, part * heads_half * nope_dim, heads_half * nope_dim, axis=1)
        w_qr_half = lax.dynamic_slice_in_dim(w_qr, part * heads_half * rope_dim, heads_half * rope_dim, axis=1)
        q_nope = jnp.dot(c_q2, w_uq_half, preferred_element_type=jnp.float32).astype(jnp.bfloat16).reshape(-1, heads_half, nope_dim)
        q_rot = jnp.dot(c_q2, w_qr_half, preferred_element_type=jnp.float32).reshape(-1, heads_half, rope_dim)
        q_pe = apply_rope(q_rot, cos_2[:, None, :], sin_2[:, None, :]).astype(jnp.bfloat16)
        q_t = jnp.transpose(jnp.concatenate([q_nope, q_pe], axis=-1), (1, 2, 0))
        o_half = attend(q_t, lat_all, kpe_all, w_uk, w_uv, n_ctx, score_scale)
        quarter = [o_half[i * half_len:(i + 1) * half_len] for i in range(4)]
        o_even = jnp.concatenate([quarter[0], quarter[3]], axis=0)
        o_odd = jnp.concatenate([quarter[1], quarter[2]], axis=0)
        mine = jnp.where(part == 0, o_even, o_odd)
        theirs = lax.ppermute(jnp.where(part == 0, o_odd, o_even), 'ctx', swap)
        attn_out = jnp.concatenate([jnp.where(part == 0, mine, theirs), jnp.where(part == 0, theirs, mine)], axis=1)
        return project_out(attn_out, w_o, mesh.shape['tp'])

    return jax.shard_map(local_step, mesh=mesh,
                         in_specs=(tok_spec, pos_spec, full_mat, full_vec, col_spec, col_spec, full_mat, full_vec, full_mat, col_spec, col_spec, row_spec),
                         out_specs=tok_spec, check_vma=False)
```

```python
import functools

import jax
import jax.numpy as jnp
from jax import lax
from jax.experimental import pallas as pl
from jax.experimental.pallas import tpu as pltpu
from jax.sharding import PartitionSpec as P

ROPE_BASE = 10000.0
NORM_EPS = 1e-6


def rope_tables(pos_vals, rope_dim):
    half_dim = rope_dim // 2
    inv_freq = ROPE_BASE ** (-jnp.arange(half_dim, dtype=jnp.float32) * 2.0 / rope_dim)
    angles = pos_vals.astype(jnp.float32)[..., None] * inv_freq
    return jnp.cos(angles), jnp.sin(angles)


MESH = pl.DeviceIdType.MESH
OUT_BLOCK = 512
W_SLOTS = 3


def out_kernel(n_tp, n_blk, o_ref, w_hbm, out_hbm, o_all, wbuf, part, recv, ybuf, w_sem, rs_send, rs_recv, ag_send, ag_recv, out_sem, o_send, o_recv):
    me = lax.axis_index('tp')
    right = lax.rem(me + 1, n_tp)
    left = lax.rem(me + n_tp - 1, n_tp)
    peer = (right, left)
    step_of = (n_tp - 1, 1)
    blk = wbuf.shape[2]
    rows = part.shape[2]
    n_pair = n_blk // 2

    def w_copy(b):
        return pltpu.make_async_copy(w_hbm.at[:, pl.ds(pl.multiple_of(b * blk, blk), blk)], wbuf.at[lax.rem(b, W_SLOTS)], w_sem.at[lax.rem(b, W_SLOTS)])

    def chunk_at(way, hop):
        return lax.rem(me + (hop + 1) * step_of[way], n_tp)

    def rs_copy(b, way, hop):
        src = part.at[b, chunk_at(way, 0)] if hop == 0 else recv.at[b, hop - 1]
        return pltpu.make_async_remote_copy(src_ref=src, dst_ref=recv.at[b, hop], send_sem=rs_send.at[b, hop], recv_sem=rs_recv.at[b, hop],
                                            device_id={'tp': peer[way]}, device_id_type=MESH)

    def ag_copy(b, slot, way, chunk):
        return pltpu.make_async_remote_copy(src_ref=ybuf.at[chunk, b], dst_ref=ybuf.at[chunk, b], send_sem=ag_send.at[b, slot], recv_sem=ag_recv.at[b, slot],
                                            device_id={'tp': peer[way]}, device_id_type=MESH)

    def out_copy(b, chunk):
        return pltpu.make_async_copy(ybuf.at[chunk, b], out_hbm.at[pl.ds(pl.multiple_of(chunk * rows, rows), rows), pl.ds(pl.multiple_of(b * blk, blk), blk)],
                                     out_sem.at[chunk, b])

    for b in range(W_SLOTS):
        w_copy(b).start()
    ctx = lax.axis_index('ctx')
    half_id = lax.rem(ctx, 2)
    mate = ctx + 1 - 2 * half_id
    half = o_all.shape[1] // 2
    barrier = pltpu.get_barrier_semaphore()
    for neighbour in peer:
        pl.semaphore_signal(barrier, inc=1, device_id={'tp': neighbour}, device_id_type=MESH)
    pl.semaphore_signal(barrier, inc=1, device_id={'ctx': mate}, device_id_type=MESH)
    pl.semaphore_wait(barrier, 3)
    own_at = (half_id, 3 - half_id)
    mate_at = (1 - half_id, 2 + half_id)
    o_share = [pltpu.make_async_remote_copy(src_ref=o_ref.at[pl.ds(pl.multiple_of(mate_at[s] * half, half), half)], dst_ref=o_all.at[half_id, pl.ds(s * half, half)],
                                            send_sem=o_send.at[s], recv_sem=o_recv.at[s], device_id={'ctx': mate}, device_id_type=MESH) for s in range(2)]
    for s in range(2):
        o_share[s].start()
    for s in range(2):
        o_all[half_id, s * half:(s + 1) * half] = o_ref[pl.ds(pl.multiple_of(own_at[s] * half, half), half), :]
    for s in range(2):
        o_share[s].wait()

    def product(p, _):
        for way in range(2):
            b = 2 * p + way
            w_copy(b).wait()
            slot = lax.rem(b, W_SLOTS)
            depth = o_all.shape[2]
            res = jnp.dot(o_all[0], wbuf[slot, 0:depth], preferred_element_type=jnp.float32) + jnp.dot(o_all[1], wbuf[slot, depth:], preferred_element_type=jnp.float32)
            part[b] = res.reshape(n_tp, rows, blk)

            @pl.when(b + W_SLOTS < n_blk)
            def _():
                w_copy(b + W_SLOTS).start()

            rs_copy(b, way, 0).start()
        return 0

    lax.fori_loop(0, n_pair, product, 0)

    for hop in range(1, n_tp - 1):
        def forward(p, _):
            for way in range(2):
                b = 2 * p + way
                rs_copy(b, way, hop - 1).wait_recv()
                recv[b, hop - 1] = recv[b, hop - 1] + part[b, chunk_at(way, hop)]
            for way in range(2):
                rs_copy(2 * p + way, way, hop).start()
            return 0

        lax.fori_loop(0, n_pair, forward, 0)

    def relay(p):
        ag_copy(2 * p, 0, 0, left).wait_recv()
        ag_copy(2 * p, 2, 0, left).start()
        ag_copy(2 * p + 1, 1, 1, right).wait_recv()
        ag_copy(2 * p + 1, 2, 1, right).start()
        out_copy(2 * p, left).start()
        out_copy(2 * p + 1, right).start()

    def finish(p, _):
        for way in range(2):
            b = 2 * p + way
            rs_copy(b, way, n_tp - 2).wait_recv()
            ybuf[me, b] = (recv[b, n_tp - 2] + part[b, me]).astype(ybuf.dtype)
        for way in range(2):
            b = 2 * p + way
            ag_copy(b, 0, 0, me).start()
            ag_copy(b, 1, 1, me).start()
            out_copy(b, me).start()

        @pl.when(p > 0)
        def _():
            relay(p - 1)
        return 0

    lax.fori_loop(0, n_pair, finish, 0)
    relay(n_pair - 1)

    def drain(p, _):
        ag_copy(2 * p, 1, 1, right).wait_recv()
        out_copy(2 * p, right).start()
        ag_copy(2 * p + 1, 0, 0, left).wait_recv()
        out_copy(2 * p + 1, left).start()
        for way in range(2):
            b = 2 * p + way
            ag_copy(b, 2, way, lax.rem(me + 2, n_tp)).wait_recv()
            out_copy(b, lax.rem(me + 2, n_tp)).start()
        return 0

    lax.fori_loop(0, n_pair, drain, 0)

    def settle(p, _):
        for way in range(2):
            b = 2 * p + way
            for hop in range(n_tp - 1):
                rs_copy(b, way, hop).wait_send()
            ag_copy(b, 0, 0, me).wait_send()
            ag_copy(b, 1, 1, me).wait_send()
            ag_copy(b, 2, way, left if way == 0 else right).wait_send()
            for chunk in range(n_tp):
                out_copy(b, chunk).wait()
        return 0

    lax.fori_loop(0, n_pair, settle, 0)


def project_out(attn_out, w_o, n_tp):
    tok_count = attn_out.shape[0] // 2
    depth, width = w_o.shape
    n_blk = width // OUT_BLOCK
    assert n_tp == 4 and n_blk % 2 == 0 and width % OUT_BLOCK == 0
    rows = tok_count // n_tp
    dma = pltpu.SemaphoreType.DMA
    return pl.pallas_call(
        functools.partial(out_kernel, n_tp, n_blk),
        out_shape=jax.ShapeDtypeStruct((tok_count, width), jnp.bfloat16),
        in_specs=[pl.BlockSpec(memory_space=pltpu.VMEM), pl.BlockSpec(memory_space=pl.ANY)],
        out_specs=pl.BlockSpec(memory_space=pl.ANY),
        scratch_shapes=[
            pltpu.VMEM((2, tok_count, depth // 2), jnp.bfloat16),
            pltpu.VMEM((W_SLOTS, depth, OUT_BLOCK), jnp.bfloat16),
            pltpu.VMEM((n_blk, n_tp, rows, OUT_BLOCK), jnp.float32),
            pltpu.VMEM((n_blk, n_tp - 1, rows, OUT_BLOCK), jnp.float32),
            pltpu.VMEM((n_tp, n_blk, rows, OUT_BLOCK), jnp.bfloat16),
            dma((W_SLOTS,)), dma((n_blk, n_tp - 1)), dma((n_blk, n_tp - 1)), dma((n_blk, 3)), dma((n_blk, 3)), dma((n_tp, n_blk)), dma((2,)), dma((2,)),
        ],
        compiler_params=pltpu.CompilerParams(collective_id=1, has_side_effects=True, vmem_limit_bytes=60 * 1024 * 1024),
        name='out_proj',
    )(attn_out, w_o)


K_CHUNKS = 4
Q_BLOCK = 256
Q_SLOTS = 4


def latent_kernel(n_ctx, x_hbm, wdkv_hbm, wkr_hbm, wdq_hbm, wuq_hbm, wqr_hbm, gq_ref, gkv_ref, tab_ref, tabk_ref, lat_hbm, q_ref,
                  x_v, wdkv, wkr, wdq, wuq, wqr, kv_acc, kr_acc, cq_acc, cq_all, tab_all, lat,
                  x_sem, dkv_sem, kr_sem, dq_sem, uq_sem, qr_sem, ring_send, ring_recv, mate_send, mate_recv, cq_send, cq_recv, tab_send, tab_recv, lat_sem):
    me = lax.axis_index('ctx')
    part = lax.rem(me, 2)
    mate = me + 1 - 2 * part
    right = lax.rem(me + 2, n_ctx)
    left = lax.rem(me + n_ctx - 2, n_ctx)
    far = lax.rem(me + 4, n_ctx)
    f32 = jnp.float32
    rows, width = x_v.shape
    half = rows // 2
    rank = kv_acc.shape[1]
    rope = kr_acc.shape[1]
    rot = rope // 2
    kc = width // K_CHUNKS
    n_dq = cq_acc.shape[1] // Q_BLOCK
    n_uq, n_qr = wuq.shape[0], wqr.shape[0]
    nope = q_ref.shape[1] - rope

    def kcols(k):
        return pl.ds(k * kc, kc)

    x_copy = [pltpu.make_async_copy(x_hbm.at[:, kcols(k)], x_v.at[:, kcols(k)], x_sem.at[k]) for k in range(K_CHUNKS)]
    dkv_copy = [pltpu.make_async_copy(wdkv_hbm.at[kcols(k)], wdkv.at[kcols(k)], dkv_sem.at[k]) for k in range(K_CHUNKS)]
    kr_copy = [pltpu.make_async_copy(wkr_hbm.at[kcols(k)], wkr.at[kcols(k)], kr_sem.at[k]) for k in range(K_CHUNKS)]
    dq_copy = [pltpu.make_async_copy(wdq_hbm.at[:, pl.ds(b * Q_BLOCK, Q_BLOCK)], wdq.at[b % Q_SLOTS], dq_sem.at[b % Q_SLOTS]) for b in range(n_dq)]
    uq_copy = [pltpu.make_async_copy(wuq_hbm.at[:, pl.ds(pl.multiple_of((part * n_uq + b) * Q_BLOCK, Q_BLOCK), Q_BLOCK)], wuq.at[b], uq_sem.at[b]) for b in range(n_uq)]
    qr_copy = [pltpu.make_async_copy(wqr_hbm.at[:, pl.ds(pl.multiple_of((part * n_qr + b) * Q_BLOCK, Q_BLOCK), Q_BLOCK)], wqr.at[b], qr_sem.at[b]) for b in range(n_qr)]

    def piece(dev, sub):
        return dev if sub == 0 else 2 * n_ctx - 1 - dev

    def send(src, dst, send_sem, recv_sem, dev):
        return pltpu.make_async_remote_copy(src_ref=src, dst_ref=dst, send_sem=send_sem, recv_sem=recv_sem, device_id={'ctx': dev}, device_id_type=MESH)

    def ring(slot, src_dev, sub, dev):
        return send(lat.at[piece(src_dev, sub)], lat.at[piece(src_dev, sub)], ring_send.at[slot], ring_recv.at[slot], dev)

    def share(slot, src_dev, sub):
        return send(lat.at[piece(src_dev, sub)], lat.at[piece(src_dev, sub)], mate_send.at[slot], mate_recv.at[slot], mate)

    to_right = [ring(0, me, 0, right), ring(1, me, 1, right)]
    to_left = [ring(2, me, 0, left), ring(3, me, 1, left)]
    on_right = ring(4, left, 0, right)
    on_left = ring(5, right, 1, left)
    order = [(me, 0), (me, 1), (left, 0), (right, 1), (left, 1), (right, 0), (far, 0), (far, 1)]
    shares = [share(i, d, s) for i, (d, s) in enumerate(order)]
    slot_of = (part, 3 - part)
    cq_share = [send(cq_all.at[slot_of[s]], cq_all.at[slot_of[s]], cq_send.at[s], cq_recv.at[s], mate) for s in range(2)]

    def lanes(s):
        return pl.ds(pl.multiple_of(slot_of[s] * half, half), half)

    tab_share = [send(tab_all.at[:, lanes(s)], tab_all.at[:, lanes(s)], tab_send.at[s], tab_recv.at[s], mate) for s in range(2)]

    for k in range(K_CHUNKS):
        x_copy[k].start()
        dkv_copy[k].start()
        kr_copy[k].start()
    for b in range(Q_SLOTS):
        dq_copy[b].start()
    barrier = pltpu.get_barrier_semaphore()
    for dev in (mate, right, left):
        pl.semaphore_signal(barrier, inc=1, device_id={'ctx': dev}, device_id_type=MESH)
    for s in range(2):
        tab_all[:, lanes(s)] = tab_ref[:, s * half:(s + 1) * half]

    for k in range(K_CHUNKS):
        cols = slice(k * kc, (k + 1) * kc)
        x_copy[k].wait()
        dkv_copy[k].wait()
        kr_copy[k].wait()
        kv_new = jnp.dot(x_v[:, cols], wdkv[cols], preferred_element_type=f32)
        kr_new = jnp.dot(x_v[:, cols], wkr[cols], preferred_element_type=f32)
        if k == 0:
            kv_acc[...] = kv_new
            kr_acc[...] = kr_new
        else:
            kv_acc[...] += kv_new
            kr_acc[...] += kr_new
    kv = kv_acc[...]
    c_kv = (kv * lax.rsqrt(jnp.mean(kv * kv, axis=-1, keepdims=True) + NORM_EPS) * gkv_ref[...]).astype(jnp.bfloat16)
    kr = kr_acc[...]
    cos_k, sin_k = tabk_ref[:, :rot], tabk_ref[:, rot:]
    k_lo = (kr[:, :rot] * cos_k - kr[:, rot:] * sin_k).astype(jnp.bfloat16)
    k_hi = (kr[:, rot:] * cos_k + kr[:, :rot] * sin_k).astype(jnp.bfloat16)
    pad = jnp.zeros((half, lat.shape[2] - rank - rope), jnp.bfloat16)
    for s in range(2):
        own = slice(s * half, (s + 1) * half)
        lat[piece(me, s), :, 0:rank] = c_kv[own]
        lat[piece(me, s), :, rank:] = jnp.concatenate([k_lo[own], k_hi[own], pad], axis=1)

    pl.semaphore_wait(barrier, 3)
    for s in range(2):
        to_right[s].start()
        to_left[1 - s].start()
    for s in range(2):
        tab_share[s].start()
        shares[s].start()

    for b in range(n_dq):
        dq_copy[b].wait()
        cq_acc[:, b * Q_BLOCK:(b + 1) * Q_BLOCK] = jnp.dot(x_v[...], wdq[b % Q_SLOTS], preferred_element_type=f32)
        if b + Q_SLOTS < n_dq:
            dq_copy[b + Q_SLOTS].start()
        if b == 1:
            for c in qr_copy + uq_copy:
                c.start()
    for s in range(2):
        own = slice(s * half, (s + 1) * half)
        cq = cq_acc[own]
        cq_all[slot_of[s]] = (cq * lax.rsqrt(jnp.mean(cq * cq, axis=-1, keepdims=True) + NORM_EPS) * gq_ref[...]).astype(jnp.bfloat16)
        cq_share[s].start()

    to_right[0].wait_recv()
    on_right.start()
    to_left[1].wait_recv()
    on_left.start()
    shares[2].start()
    shares[3].start()
    for s in range(2):
        cq_share[s].wait_recv()
        tab_share[s].wait_recv()

    def rotary(b, _):
        pltpu.make_async_copy(wqr_hbm.at[:, pl.ds(0, Q_BLOCK)], wqr.at[b], qr_sem.at[b]).wait()
        res = jnp.dot(cq_all[...].reshape(2 * rows, cq_all.shape[2]), wqr[b], preferred_element_type=f32).T
        cos_q, sin_q = tab_all[0:rot], tab_all[rot:rope]
        for i in range(Q_BLOCK // rope):
            lo = res[i * rope:i * rope + rot]
            hi = res[i * rope + rot:(i + 1) * rope]
            h = b * (Q_BLOCK // rope) + i
            q_ref[h, nope:nope + rot, :] = (lo * cos_q - hi * sin_q).astype(jnp.bfloat16)
            q_ref[h, nope + rot:nope + rope, :] = (hi * cos_q + lo * sin_q).astype(jnp.bfloat16)
        return 0

    lax.fori_loop(0, n_qr, rotary, 0)
    to_right[1].wait_recv()
    to_left[0].wait_recv()
    shares[4].start()
    shares[5].start()

    def plain(b, _):
        pltpu.make_async_copy(wuq_hbm.at[:, pl.ds(0, Q_BLOCK)], wuq.at[b], uq_sem.at[b]).wait()
        res = jnp.dot(cq_all[...].reshape(2 * rows, cq_all.shape[2]), wuq[b], preferred_element_type=f32).astype(jnp.bfloat16).T
        for i in range(Q_BLOCK // nope):
            q_ref[b * (Q_BLOCK // nope) + i, 0:nope, :] = res[i * nope:(i + 1) * nope]
        return 0

    lax.fori_loop(0, n_uq // 2, plain, 0)
    on_right.wait_recv()
    on_left.wait_recv()
    shares[6].start()
    shares[7].start()
    lax.fori_loop(n_uq // 2, n_uq, plain, 0)
    for i in range(8):
        shares[i].wait_recv()
    out = pltpu.make_async_copy(lat, lat_hbm, lat_sem)
    out.start()
    for c in to_right + to_left + [on_right, on_left] + shares + cq_share + tab_share:
        c.wait_send()
    out.wait()


def latents(tok_x, w_dkv, w_kr, w_dq, w_uq, w_qr, g_q, g_kv, tab, n_ctx):
    rows, width = tok_x.shape
    rank, rope, q_rank = w_dkv.shape[1], w_kr.shape[1], w_dq.shape[1]
    heads = w_qr.shape[1] // rope // 2
    nope = w_uq.shape[1] // heads // 2
    bf16, f32 = jnp.bfloat16, jnp.float32
    vmem = pl.BlockSpec(memory_space=pltpu.VMEM)
    hbm = pl.BlockSpec(memory_space=pl.ANY)
    dma = pltpu.SemaphoreType.DMA
    n_uq, n_qr = heads * nope // Q_BLOCK, heads * rope // Q_BLOCK
    lat_width = rank + 128
    assert n_ctx == 8 and rope <= 128
    lat, q_t = pl.pallas_call(
        functools.partial(latent_kernel, n_ctx),
        out_shape=[jax.ShapeDtypeStruct((2 * n_ctx, rows // 2, lat_width), bf16), jax.ShapeDtypeStruct((heads, nope + rope, 2 * rows), bf16)],
        in_specs=[hbm] * 6 + [vmem] * 4,
        out_specs=[hbm, vmem],
        scratch_shapes=[
            pltpu.VMEM((rows, width), bf16), pltpu.VMEM((width, rank), bf16), pltpu.VMEM((width, rope), bf16), pltpu.VMEM((Q_SLOTS, width, Q_BLOCK), bf16),
            pltpu.VMEM((n_uq, q_rank, Q_BLOCK), bf16), pltpu.VMEM((n_qr, q_rank, Q_BLOCK), bf16),
            pltpu.VMEM((rows, rank), f32), pltpu.VMEM((rows, rope), f32), pltpu.VMEM((rows, q_rank), f32),
            pltpu.VMEM((4, rows // 2, q_rank), bf16), pltpu.VMEM((rope, 2 * rows), f32), pltpu.VMEM((2 * n_ctx, rows // 2, lat_width), bf16),
            dma((K_CHUNKS,)), dma((K_CHUNKS,)), dma((K_CHUNKS,)), dma((Q_SLOTS,)), dma((n_uq,)), dma((n_qr,)),
            dma((6,)), dma((6,)), dma((8,)), dma((8,)), dma((2,)), dma((2,)), dma((2,)), dma((2,)), dma,
        ],
        compiler_params=pltpu.CompilerParams(collective_id=2, has_side_effects=True, vmem_limit_bytes=62 * 1024 * 1024),
        name='latents',
    )(tok_x, w_dkv, w_kr, w_dq, w_uq, w_qr, g_q.astype(f32)[None], g_kv.astype(f32)[None], tab.T, tab)
    return lat.reshape(n_ctx * rows, lat_width), q_t


KEY_BLOCK = 256


def attend_kernel(n_ctx, scale, q_ref, lat_ref, wuk_hbm, wuv_hbm, o_ref, wuk, wuv, wuv_t, lat_t, kcat, v_t, s_buf, p_buf, w_sem):
    me = lax.axis_index('ctx')
    col = me // 2
    part = lax.rem(me, 2)
    n_col = n_ctx // 2
    heads = q_ref.shape[0]
    n_pair = heads // 2
    rank = wuk.shape[1]
    v_dim = v_t.shape[0] // 2
    nope = wuk.shape[2] // 2
    rope = q_ref.shape[1] - nope
    exp_scale = scale * 1.4426950408889634

    def w_copy(src, dst, which, hp):
        cols = dst.shape[2]
        return pltpu.make_async_copy(src.at[:, pl.ds(pl.multiple_of((part * n_pair + hp) * cols, cols), cols)], dst.at[hp], w_sem.at[which, hp])

    for hp in range(n_pair):
        w_copy(wuk_hbm, wuk, 0, hp).start()
        w_copy(wuv_hbm, wuv, 1, hp).start()
    for blk in range(lat_ref.shape[0] // KEY_BLOCK):
        lat_t[:, blk * KEY_BLOCK:(blk + 1) * KEY_BLOCK] = lat_ref[blk * KEY_BLOCK:(blk + 1) * KEY_BLOCK, 0:rank].T
        for g in range(2):
            kcat[g, blk * KEY_BLOCK:(blk + 1) * KEY_BLOCK, nope:nope + rope] = lat_ref[blk * KEY_BLOCK:(blk + 1) * KEY_BLOCK, rank:rank + rope]
    for hp in range(n_pair):
        w_copy(wuk_hbm, wuk, 0, hp).wait()
        w_copy(wuv_hbm, wuv, 1, hp).wait()
        wuv_t[hp] = wuv[hp].T

    def phase(sel, n_blk):
        q_cols = slice(sel * KEY_BLOCK, (sel + 1) * KEY_BLOCK)
        key_i = lax.broadcasted_iota(jnp.int32, (KEY_BLOCK, KEY_BLOCK), 0)
        q_i = lax.broadcasted_iota(jnp.int32, (KEY_BLOCK, KEY_BLOCK), 1)
        visible = key_i <= q_i

        def pair_step(hp, _):
            for blk in range(n_blk):
                rows = slice(blk * KEY_BLOCK, (blk + 1) * KEY_BLOCK)
                k2 = jnp.dot(lat_ref[rows, 0:rank], wuk[hp], preferred_element_type=jnp.float32).astype(jnp.bfloat16)
                kcat[0, rows, 0:nope] = k2[:, :nope]
                kcat[1, rows, 0:nope] = k2[:, nope:]
                v_t[:, rows] = jnp.dot(wuv_t[hp], lat_t[:, rows], preferred_element_type=jnp.float32).astype(jnp.bfloat16)
            top = []
            for g in range(2):
                q_t = q_ref[2 * hp + g, :, q_cols]
                top8 = None
                for blk in range(n_blk):
                    rows = slice(blk * KEY_BLOCK, (blk + 1) * KEY_BLOCK)
                    s = jnp.dot(kcat[g, rows, 0:nope + rope], q_t, preferred_element_type=jnp.float32)
                    if blk == n_blk - 1:
                        s = jnp.where(visible, s, -1e30)
                    s_buf[g, rows] = s
                    blk8 = jnp.max(s.reshape(KEY_BLOCK // 8, 8, KEY_BLOCK), axis=0)
                    top8 = blk8 if top8 is None else jnp.maximum(top8, blk8)
                top.append(jnp.max(top8, axis=0, keepdims=True) * exp_scale)
            for g in range(2):
                sum8 = None
                for blk in range(n_blk):
                    rows = slice(blk * KEY_BLOCK, (blk + 1) * KEY_BLOCK)
                    p = jnp.exp2(s_buf[g, rows] * exp_scale - top[g])
                    blk8 = jnp.sum(p.reshape(KEY_BLOCK // 8, 8, KEY_BLOCK), axis=0)
                    sum8 = blk8 if sum8 is None else sum8 + blk8
                    p_buf[g, rows] = p.astype(jnp.bfloat16)
                total = jnp.sum(sum8, axis=0, keepdims=True)
                o_t = jnp.dot(v_t[g * v_dim:(g + 1) * v_dim, 0:n_blk * KEY_BLOCK], p_buf[g, 0:n_blk * KEY_BLOCK], preferred_element_type=jnp.float32)
                o_ref[q_cols, pl.ds(pl.multiple_of((2 * hp + g) * v_dim, v_dim), v_dim)] = (o_t / total).T.astype(o_ref.dtype)
            return 0

        lax.fori_loop(0, n_pair, pair_step, 0)

    for v in range(n_col):
        pl.when(col == v)(functools.partial(phase, 0, v + 1))
    for v in range(n_col):
        pl.when(col == v)(functools.partial(phase, 1, 2 * n_col - v))


def attend(q_t, lat, w_uk, w_uv, n_ctx, scale):
    heads, q_dim, q_count = q_t.shape
    keys, rank = lat.shape[0], w_uk.shape[0]
    nope = w_uk.shape[1] // (2 * heads)
    rope = q_dim - nope
    v_dim = w_uv.shape[1] // (2 * heads)
    n_pair = heads // 2
    bf16, f32 = jnp.bfloat16, jnp.float32
    vmem = pl.BlockSpec(memory_space=pltpu.VMEM)
    hbm = pl.BlockSpec(memory_space=pl.ANY)
    assert q_count == 2 * KEY_BLOCK and keys == n_ctx * KEY_BLOCK
    return pl.pallas_call(
        functools.partial(attend_kernel, n_ctx, scale),
        out_shape=jax.ShapeDtypeStruct((q_count, heads * v_dim), bf16),
        in_specs=[vmem, vmem, hbm, hbm],
        out_specs=vmem,
        scratch_shapes=[
            pltpu.VMEM((n_pair, rank, 2 * nope), bf16), pltpu.VMEM((n_pair, rank, 2 * v_dim), bf16), pltpu.VMEM((n_pair, 2 * v_dim, rank), bf16),
            pltpu.VMEM((rank, keys), bf16), pltpu.VMEM((2, keys, nope + rope), bf16), pltpu.VMEM((2 * v_dim, keys), bf16),
            pltpu.VMEM((2, keys, KEY_BLOCK), f32), pltpu.VMEM((2, keys, KEY_BLOCK), bf16),
            pltpu.SemaphoreType.DMA((2, n_pair)),
        ],
        compiler_params=pltpu.CompilerParams(vmem_limit_bytes=60 * 1024 * 1024),
        name='attend',
    )(q_t, lat, w_uk, w_uv)


def solution(mesh):
    tok_spec = P(('dp', 'ctx'), None)
    pos_spec = P(('dp', 'ctx'))
    full_mat = P(None, None)
    full_vec = P(None)
    col_spec = P(None, 'tp')
    row_spec = P('tp', None)

    def local_step(tok_x, tok_pos, w_dq, g_q, w_uq, w_qr, w_dkv, g_kv, w_kr, w_uk, w_uv, w_o):
        rope_dim = w_kr.shape[1]
        heads_loc = w_qr.shape[1] // rope_dim
        nope_dim = w_uq.shape[1] // heads_loc
        score_scale = (nope_dim + rope_dim) ** -0.5
        n_ctx = mesh.shape['ctx']
        tab = jnp.concatenate(rope_tables(tok_pos, rope_dim), axis=-1)
        lat, q_t = latents(tok_x, w_dkv, w_kr, w_dq, w_uq, w_qr, g_q, g_kv, tab, n_ctx)
        o_half = attend(q_t, lat, w_uk, w_uv, n_ctx, score_scale)
        return project_out(o_half, w_o, mesh.shape['tp'])

    return jax.shard_map(local_step, mesh=mesh,
                         in_specs=(tok_spec, pos_spec, full_mat, full_vec, col_spec, col_spec, full_mat, full_vec, full_mat, col_spec, col_spec, row_spec),
                         out_specs=tok_spec, check_vma=False)
```

```python
import functools

import jax
import jax.numpy as jnp
from jax import lax
from jax.experimental import pallas as pl
from jax.experimental.pallas import tpu as pltpu
from jax.sharding import PartitionSpec as P

ROPE_BASE = 10000.0
NORM_EPS = 1e-6


def rope_tables(pos_vals, rope_dim):
    half_dim = rope_dim // 2
    inv_freq = ROPE_BASE ** (-jnp.arange(half_dim, dtype=jnp.float32) * 2.0 / rope_dim)
    angles = pos_vals.astype(jnp.float32)[..., None] * inv_freq
    return jnp.cos(angles), jnp.sin(angles)


MESH = pl.DeviceIdType.MESH
KEY_BLOCK = 256
OUT_BLOCK = 512
W_SLOTS = 3
LAG = 3


def mix_kernel(n_tp, n_ctx, n_blk, scale, q_ref, lat_ref, wuk_hbm, wuv_hbm, w_hbm, out_hbm,
               wuk, wuv, wuv_t, lat_t, kcat, v_t, s_buf, p_buf, o_buf, o_all, wbuf, part, recv, ybuf,
               up_sem, w_sem, o_send, o_recv, rs_send, rs_recv, ag_send, ag_recv, out_sem):
    f32, bf16 = jnp.float32, jnp.bfloat16
    ctx = lax.axis_index('ctx')
    col = ctx // 2
    core = lax.rem(ctx, 2)
    mate = ctx + 1 - 2 * core
    n_col = n_ctx // 2
    me = lax.axis_index('tp')
    right = lax.rem(me + 1, n_tp)
    left = lax.rem(me + n_tp - 1, n_tp)
    across = lax.rem(me + 2, n_tp)
    peer = (right, left)
    step_of = (n_tp - 1, 1)
    heads = q_ref.shape[0]
    n_hp = heads // 2
    rank = wuk.shape[1]
    v_dim = v_t.shape[0] // 2
    nope = wuk.shape[2] // 2
    rope = q_ref.shape[1] - nope
    exp_scale = scale * 1.4426950408889634
    blk = wbuf.shape[2]
    rows = part.shape[3]
    n_pair = n_blk // 2
    half = o_all.shape[2]

    def up_copy(src, dst, which, hp):
        cols = dst.shape[2]
        return pltpu.make_async_copy(src.at[:, pl.ds(pl.multiple_of((core * n_hp + hp) * cols, cols), cols)], dst.at[hp], up_sem.at[which, hp])

    def w_copy(i):
        b = lax.rem(i, n_blk)
        slot = lax.rem(i, W_SLOTS)
        return pltpu.make_async_copy(w_hbm.at[:, pl.ds(pl.multiple_of(b * blk, blk), blk)], wbuf.at[slot], w_sem.at[slot])

    def chunk_at(way, hop):
        return lax.rem(me + (hop + 1) * step_of[way], n_tp)

    def rs_first(sel, b, way):
        return pltpu.make_async_remote_copy(src_ref=part.at[sel, b, chunk_at(way, 0)], dst_ref=recv.at[sel, b, 0], send_sem=rs_send.at[sel, b, 0],
                                            recv_sem=rs_recv.at[sel, b, 0], device_id={'tp': peer[way]}, device_id_type=MESH)

    def rs_next(sel, b, way, hop):
        return pltpu.make_async_remote_copy(src_ref=recv.at[sel, b, hop - 1], dst_ref=recv.at[sel, b, hop], send_sem=rs_send.at[sel, b, hop],
                                            recv_sem=rs_recv.at[sel, b, hop], device_id={'tp': peer[way]}, device_id_type=MESH)

    def rs_arrived(sel, b, way, hop):
        pltpu.make_async_remote_copy(src_ref=recv.at[sel, b, hop], dst_ref=recv.at[sel, b, hop], send_sem=rs_send.at[sel, b, hop],
                                     recv_sem=rs_recv.at[sel, b, hop], device_id={'tp': peer[way]}, device_id_type=MESH).wait_recv()

    def ag_copy(sel, b, slot, way, chunk):
        return pltpu.make_async_remote_copy(src_ref=ybuf.at[sel, chunk, b], dst_ref=ybuf.at[sel, chunk, b], send_sem=ag_send.at[sel, b, slot],
                                            recv_sem=ag_recv.at[sel, b, slot], device_id={'tp': peer[way]}, device_id_type=MESH)

    def out_copy(sel, b, chunk):
        return pltpu.make_async_copy(ybuf.at[sel, chunk, b],
                                     out_hbm.at[pl.ds(pl.multiple_of(sel * half + chunk * rows, rows), rows), pl.ds(pl.multiple_of(b * blk, blk), blk)],
                                     out_sem.at[sel, chunk, b])

    own_at = (core, 3 - core)
    mate_at = (1 - core, 2 + core)

    def o_share(sel):
        return pltpu.make_async_remote_copy(src_ref=o_buf.at[pl.ds(pl.multiple_of(mate_at[sel] * half, half), half)], dst_ref=o_all.at[sel, core],
                                            send_sem=o_send.at[sel], recv_sem=o_recv.at[sel], device_id={'ctx': mate}, device_id_type=MESH)

    for hp in range(n_hp):
        up_copy(wuk_hbm, wuk, 0, hp).start()
        up_copy(wuv_hbm, wuv, 1, hp).start()
    for i in range(W_SLOTS):
        w_copy(i).start()
    barrier = pltpu.get_barrier_semaphore()
    for neighbour in peer:
        pl.semaphore_signal(barrier, inc=1, device_id={'tp': neighbour}, device_id_type=MESH)
    pl.semaphore_signal(barrier, inc=1, device_id={'ctx': mate}, device_id_type=MESH)
    for i in range(lat_ref.shape[0] // KEY_BLOCK):
        lat_t[:, i * KEY_BLOCK:(i + 1) * KEY_BLOCK] = lat_ref[i * KEY_BLOCK:(i + 1) * KEY_BLOCK, 0:rank].T
        for g in range(2):
            kcat[g, i * KEY_BLOCK:(i + 1) * KEY_BLOCK, nope:nope + rope] = lat_ref[i * KEY_BLOCK:(i + 1) * KEY_BLOCK, rank:rank + rope]
    for hp in range(n_hp):
        up_copy(wuk_hbm, wuk, 0, hp).wait()
        up_copy(wuv_hbm, wuv, 1, hp).wait()
        wuv_t[hp] = wuv[hp].T
    pl.semaphore_wait(barrier, 3)

    def attend(sel, n_key, serve):
        q_cols = slice(sel * KEY_BLOCK, (sel + 1) * KEY_BLOCK)
        key_i = lax.broadcasted_iota(jnp.int32, (KEY_BLOCK, KEY_BLOCK), 0)
        q_i = lax.broadcasted_iota(jnp.int32, (KEY_BLOCK, KEY_BLOCK), 1)
        visible = key_i <= q_i

        def pair_step(hp, _):
            for i in range(n_key):
                keys = slice(i * KEY_BLOCK, (i + 1) * KEY_BLOCK)
                k2 = jnp.dot(lat_ref[keys, 0:rank], wuk[hp], preferred_element_type=f32).astype(bf16)
                kcat[0, keys, 0:nope] = k2[:, :nope]
                kcat[1, keys, 0:nope] = k2[:, nope:]
                v_t[:, keys] = jnp.dot(wuv_t[hp], lat_t[:, keys], preferred_element_type=f32).astype(bf16)
            top = []
            for g in range(2):
                q_t = q_ref[2 * hp + g, :, q_cols]
                top8 = None
                for i in range(n_key):
                    keys = slice(i * KEY_BLOCK, (i + 1) * KEY_BLOCK)
                    s = jnp.dot(kcat[g, keys, 0:nope + rope], q_t, preferred_element_type=f32)
                    if i == n_key - 1:
                        s = jnp.where(visible, s, -1e30)
                    s_buf[g, keys] = s
                    blk8 = jnp.max(s.reshape(KEY_BLOCK // 8, 8, KEY_BLOCK), axis=0)
                    top8 = blk8 if top8 is None else jnp.maximum(top8, blk8)
                top.append(jnp.max(top8, axis=0, keepdims=True) * exp_scale)
            for g in range(2):
                sum8 = None
                for i in range(n_key):
                    keys = slice(i * KEY_BLOCK, (i + 1) * KEY_BLOCK)
                    p = jnp.exp2(s_buf[g, keys] * exp_scale - top[g])
                    blk8 = jnp.sum(p.reshape(KEY_BLOCK // 8, 8, KEY_BLOCK), axis=0)
                    sum8 = blk8 if sum8 is None else sum8 + blk8
                    p_buf[g, keys] = p.astype(bf16)
                total = jnp.sum(sum8, axis=0, keepdims=True)
                o_t = jnp.dot(v_t[g * v_dim:(g + 1) * v_dim, 0:n_key * KEY_BLOCK], p_buf[g, 0:n_key * KEY_BLOCK], preferred_element_type=f32)
                o_buf[q_cols, pl.ds(pl.multiple_of((2 * hp + g) * v_dim, v_dim), v_dim)] = (o_t / total).T.astype(bf16)
            if serve is not None:
                serve(hp)
            return 0

        lax.fori_loop(0, n_hp, pair_step, 0)

    def exchange(sel):
        o_share(sel).start()
        o_all[sel, core] = o_buf[pl.ds(pl.multiple_of(own_at[sel] * half, half), half), :]
        o_share(sel).wait()

    def product(sel, p):
        for way in range(2):
            b = 2 * p + way
            i = sel * n_blk + b
            slot = lax.rem(i, W_SLOTS)
            w_copy(i).wait()
            depth = o_all.shape[3]
            res = jnp.dot(o_all[sel, 0], wbuf[slot, 0:depth], preferred_element_type=f32) + jnp.dot(o_all[sel, 1], wbuf[slot, depth:], preferred_element_type=f32)
            part[sel, b] = res.reshape(n_tp, rows, blk)

            @pl.when(i + W_SLOTS < 2 * n_blk)
            def _():
                w_copy(i + W_SLOTS).start()

            rs_first(sel, b, way).start()

    def forward(sel, p, hop):
        for way in range(2):
            b = 2 * p + way
            rs_arrived(sel, b, way, hop - 1)
            recv[sel, b, hop - 1] = recv[sel, b, hop - 1] + part[sel, b, chunk_at(way, hop)]
        for way in range(2):
            rs_next(sel, 2 * p + way, way, hop).start()

    def finish(sel, p):
        for way in range(2):
            b = 2 * p + way
            rs_arrived(sel, b, way, n_tp - 2)
            ybuf[sel, me, b] = (recv[sel, b, n_tp - 2] + part[sel, b, me]).astype(ybuf.dtype)
        for way in range(2):
            b = 2 * p + way
            ag_copy(sel, b, 0, 0, me).start()
            ag_copy(sel, b, 1, 1, me).start()
            out_copy(sel, b, me).start()

    def relay(sel, p):
        ag_copy(sel, 2 * p, 0, 0, left).wait_recv()
        ag_copy(sel, 2 * p, 2, 0, left).start()
        ag_copy(sel, 2 * p + 1, 1, 1, right).wait_recv()
        ag_copy(sel, 2 * p + 1, 2, 1, right).start()
        out_copy(sel, 2 * p, left).start()
        out_copy(sel, 2 * p + 1, right).start()

    def drain(sel, p):
        ag_copy(sel, 2 * p, 1, 1, right).wait_recv()
        out_copy(sel, 2 * p, right).start()
        ag_copy(sel, 2 * p + 1, 0, 0, left).wait_recv()
        out_copy(sel, 2 * p + 1, left).start()
        for way in range(2):
            b = 2 * p + way
            ag_copy(sel, b, 2, way, across).wait_recv()
            out_copy(sel, b, across).start()

    def settle(sel, p):
        for way in range(2):
            b = 2 * p + way
            rs_first(sel, b, way).wait_send()
            for hop in range(1, n_tp - 1):
                rs_next(sel, b, way, hop).wait_send()
            ag_copy(sel, b, 0, 0, me).wait_send()
            ag_copy(sel, b, 1, 1, me).wait_send()
            ag_copy(sel, b, 2, way, left if way == 0 else right).wait_send()
            for chunk in range(n_tp):
                out_copy(sel, b, chunk).wait()

    def loop(start, stop, body):
        def step(p, _):
            body(p)
            return 0
        lax.fori_loop(start, stop, step, 0)

    for v in range(n_col):
        pl.when(col == v)(functools.partial(attend, 0, v + 1, None))
    exchange(0)

    def early(p):
        product(0, p)

        @pl.when(p >= LAG)
        def _():
            forward(0, p - LAG, 1)

    loop(0, n_pair, early)
    hop1_left = n_pair - LAG

    def serve(hp):
        for j in range(2):
            n = hop1_left + 2 * hp + j
            pl.when(n < n_pair)(lambda: forward(0, n, 1))
            pl.when((n >= n_pair) & (n < 2 * n_pair))(lambda: forward(0, n - n_pair, 2))
            pl.when((n >= 2 * n_pair) & (n < 3 * n_pair))(lambda: finish(0, n - 2 * n_pair))

    for v in range(n_col):
        pl.when(col == v)(functools.partial(attend, 1, 2 * n_col - v, serve))
    served = min(hop1_left + 2 * n_hp, 3 * n_pair) - 2 * n_pair
    exchange(1)

    def late(p):
        product(1, p)
        pl.when(p + served < n_pair)(lambda: finish(0, p + served))

        @pl.when(p >= LAG)
        def _():
            forward(1, p - LAG, 1)

        relay(0, p)

    loop(0, n_pair, late)
    loop(hop1_left, n_pair, lambda p: forward(1, p, 1))
    loop(0, n_pair, lambda p: forward(1, p, 2))

    def close(p):
        finish(1, p)
        pl.when(p > 0)(lambda: relay(1, p - 1))
        drain(0, p)

    loop(0, n_pair, close)
    relay(1, n_pair - 1)
    loop(0, n_pair, lambda p: drain(1, p))
    o_wait = n_pair
    loop(0, o_wait, lambda p: settle(0, p))
    loop(0, o_wait, lambda p: settle(1, p))


def mix(q_t, lat, w_uk, w_uv, w_o, n_tp, n_ctx, scale):
    heads, q_dim, q_count = q_t.shape
    keys, rank = lat.shape[0], w_uk.shape[0]
    nope = w_uk.shape[1] // (2 * heads)
    rope = q_dim - nope
    v_dim = w_uv.shape[1] // (2 * heads)
    n_hp = heads // 2
    depth, width = w_o.shape
    n_blk = width // OUT_BLOCK
    half = q_count // 4
    rows = half // n_tp
    assert n_tp == 4 and n_blk % 2 == 0 and width % OUT_BLOCK == 0
    assert q_count == 2 * KEY_BLOCK and keys == n_ctx * KEY_BLOCK
    bf16, f32 = jnp.bfloat16, jnp.float32
    vmem = pl.BlockSpec(memory_space=pltpu.VMEM)
    hbm = pl.BlockSpec(memory_space=pl.ANY)
    dma = pltpu.SemaphoreType.DMA
    return pl.pallas_call(
        functools.partial(mix_kernel, n_tp, n_ctx, n_blk, scale),
        out_shape=jax.ShapeDtypeStruct((2 * half, width), bf16),
        in_specs=[vmem, vmem, hbm, hbm, hbm],
        out_specs=hbm,
        scratch_shapes=[
            pltpu.VMEM((n_hp, rank, 2 * nope), bf16), pltpu.VMEM((n_hp, rank, 2 * v_dim), bf16), pltpu.VMEM((n_hp, 2 * v_dim, rank), bf16),
            pltpu.VMEM((rank, keys), bf16), pltpu.VMEM((2, keys, nope + rope), bf16), pltpu.VMEM((2 * v_dim, keys), bf16),
            pltpu.VMEM((2, keys, KEY_BLOCK), f32), pltpu.VMEM((2, keys, KEY_BLOCK), bf16),
            pltpu.VMEM((q_count, heads * v_dim), bf16), pltpu.VMEM((2, 2, half, depth // 2), bf16),
            pltpu.VMEM((W_SLOTS, depth, OUT_BLOCK), bf16),
            pltpu.VMEM((2, n_blk, n_tp, rows, OUT_BLOCK), f32),
            pltpu.VMEM((2, n_blk, n_tp - 1, rows, OUT_BLOCK), f32),
            pltpu.VMEM((2, n_tp, n_blk, rows, OUT_BLOCK), bf16),
            dma((2, n_hp)), dma((W_SLOTS,)), dma((2,)), dma((2,)), dma((2, n_blk, n_tp - 1)), dma((2, n_blk, n_tp - 1)),
            dma((2, n_blk, 3)), dma((2, n_blk, 3)), dma((2, n_tp, n_blk)),
        ],
        compiler_params=pltpu.CompilerParams(collective_id=1, has_side_effects=True, vmem_limit_bytes=63 * 1024 * 1024),
        name='mix',
    )(q_t, lat, w_uk, w_uv, w_o)


K_CHUNKS = 4
Q_BLOCK = 256
Q_SLOTS = 4


def latent_kernel(n_ctx, x_hbm, wdkv_hbm, wkr_hbm, wdq_hbm, wuq_hbm, wqr_hbm, gq_ref, gkv_ref, tab_ref, tabk_ref, lat_hbm, q_ref,
                  x_v, wdkv, wkr, wdq, wuq, wqr, kv_acc, kr_acc, cq_acc, cq_all, tab_all, lat,
                  x_sem, dkv_sem, kr_sem, dq_sem, uq_sem, qr_sem, ring_send, ring_recv, mate_send, mate_recv, cq_send, cq_recv, tab_send, tab_recv, lat_sem):
    me = lax.axis_index('ctx')
    part = lax.rem(me, 2)
    mate = me + 1 - 2 * part
    right = lax.rem(me + 2, n_ctx)
    left = lax.rem(me + n_ctx - 2, n_ctx)
    far = lax.rem(me + 4, n_ctx)
    f32 = jnp.float32
    rows, width = x_v.shape
    half = rows // 2
    rank = kv_acc.shape[1]
    rope = kr_acc.shape[1]
    rot = rope // 2
    kc = width // K_CHUNKS
    n_dq = cq_acc.shape[1] // Q_BLOCK
    n_uq, n_qr = wuq.shape[0], wqr.shape[0]
    nope = q_ref.shape[1] - rope

    def kcols(k):
        return pl.ds(k * kc, kc)

    x_copy = [pltpu.make_async_copy(x_hbm.at[:, kcols(k)], x_v.at[:, kcols(k)], x_sem.at[k]) for k in range(K_CHUNKS)]
    dkv_copy = [pltpu.make_async_copy(wdkv_hbm.at[kcols(k)], wdkv.at[kcols(k)], dkv_sem.at[k]) for k in range(K_CHUNKS)]
    kr_copy = [pltpu.make_async_copy(wkr_hbm.at[kcols(k)], wkr.at[kcols(k)], kr_sem.at[k]) for k in range(K_CHUNKS)]
    dq_copy = [pltpu.make_async_copy(wdq_hbm.at[:, pl.ds(b * Q_BLOCK, Q_BLOCK)], wdq.at[b % Q_SLOTS], dq_sem.at[b % Q_SLOTS]) for b in range(n_dq)]
    uq_copy = [pltpu.make_async_copy(wuq_hbm.at[:, pl.ds(pl.multiple_of((part * n_uq + b) * Q_BLOCK, Q_BLOCK), Q_BLOCK)], wuq.at[b], uq_sem.at[b]) for b in range(n_uq)]
    qr_copy = [pltpu.make_async_copy(wqr_hbm.at[:, pl.ds(pl.multiple_of((part * n_qr + b) * Q_BLOCK, Q_BLOCK), Q_BLOCK)], wqr.at[b], qr_sem.at[b]) for b in range(n_qr)]

    def piece(dev, sub):
        return dev if sub == 0 else 2 * n_ctx - 1 - dev

    def send(src, dst, send_sem, recv_sem, dev):
        return pltpu.make_async_remote_copy(src_ref=src, dst_ref=dst, send_sem=send_sem, recv_sem=recv_sem, device_id={'ctx': dev}, device_id_type=MESH)

    def ring(slot, src_dev, sub, dev):
        return send(lat.at[piece(src_dev, sub)], lat.at[piece(src_dev, sub)], ring_send.at[slot], ring_recv.at[slot], dev)

    def share(slot, src_dev, sub):
        return send(lat.at[piece(src_dev, sub)], lat.at[piece(src_dev, sub)], mate_send.at[slot], mate_recv.at[slot], mate)

    to_right = [ring(0, me, 0, right), ring(1, me, 1, right)]
    to_left = [ring(2, me, 0, left), ring(3, me, 1, left)]
    on_right = ring(4, left, 0, right)
    on_left = ring(5, right, 1, left)
    order = [(me, 0), (me, 1), (left, 0), (right, 1), (left, 1), (right, 0), (far, 0), (far, 1)]
    shares = [share(i, d, s) for i, (d, s) in enumerate(order)]
    slot_of = (part, 3 - part)
    cq_share = [send(cq_all.at[slot_of[s]], cq_all.at[slot_of[s]], cq_send.at[s], cq_recv.at[s], mate) for s in range(2)]

    def lanes(s):
        return pl.ds(pl.multiple_of(slot_of[s] * half, half), half)

    tab_share = [send(tab_all.at[:, lanes(s)], tab_all.at[:, lanes(s)], tab_send.at[s], tab_recv.at[s], mate) for s in range(2)]

    for k in range(K_CHUNKS):
        x_copy[k].start()
        dkv_copy[k].start()
        kr_copy[k].start()
    for b in range(Q_SLOTS):
        dq_copy[b].start()
    barrier = pltpu.get_barrier_semaphore()
    for dev in (mate, right, left):
        pl.semaphore_signal(barrier, inc=1, device_id={'ctx': dev}, device_id_type=MESH)
    for s in range(2):
        tab_all[:, lanes(s)] = tab_ref[:, s * half:(s + 1) * half]

    for k in range(K_CHUNKS):
        cols = slice(k * kc, (k + 1) * kc)
        x_copy[k].wait()
        dkv_copy[k].wait()
        kr_copy[k].wait()
        kv_new = jnp.dot(x_v[:, cols], wdkv[cols], preferred_element_type=f32)
        kr_new = jnp.dot(x_v[:, cols], wkr[cols], preferred_element_type=f32)
        if k == 0:
            kv_acc[...] = kv_new
            kr_acc[...] = kr_new
        else:
            kv_acc[...] += kv_new
            kr_acc[...] += kr_new
    kv = kv_acc[...]
    c_kv = (kv * lax.rsqrt(jnp.mean(kv * kv, axis=-1, keepdims=True) + NORM_EPS) * gkv_ref[...]).astype(jnp.bfloat16)
    kr = kr_acc[...]
    cos_k, sin_k = tabk_ref[:, :rot], tabk_ref[:, rot:]
    k_lo = (kr[:, :rot] * cos_k - kr[:, rot:] * sin_k).astype(jnp.bfloat16)
    k_hi = (kr[:, rot:] * cos_k + kr[:, :rot] * sin_k).astype(jnp.bfloat16)
    pad = jnp.zeros((half, lat.shape[2] - rank - rope), jnp.bfloat16)
    for s in range(2):
        own = slice(s * half, (s + 1) * half)
        lat[piece(me, s), :, 0:rank] = c_kv[own]
        lat[piece(me, s), :, rank:] = jnp.concatenate([k_lo[own], k_hi[own], pad], axis=1)

    pl.semaphore_wait(barrier, 3)
    for s in range(2):
        to_right[s].start()
        to_left[1 - s].start()
    for s in range(2):
        tab_share[s].start()
        shares[s].start()

    for b in range(n_dq):
        dq_copy[b].wait()
        cq_acc[:, b * Q_BLOCK:(b + 1) * Q_BLOCK] = jnp.dot(x_v[...], wdq[b % Q_SLOTS], preferred_element_type=f32)
        if b + Q_SLOTS < n_dq:
            dq_copy[b + Q_SLOTS].start()
        if b == 1:
            for c in qr_copy + uq_copy:
                c.start()
    for s in range(2):
        own = slice(s * half, (s + 1) * half)
        cq = cq_acc[own]
        cq_all[slot_of[s]] = (cq * lax.rsqrt(jnp.mean(cq * cq, axis=-1, keepdims=True) + NORM_EPS) * gq_ref[...]).astype(jnp.bfloat16)
        cq_share[s].start()

    to_right[0].wait_recv()
    on_right.start()
    to_left[1].wait_recv()
    on_left.start()
    shares[2].start()
    shares[3].start()
    for s in range(2):
        cq_share[s].wait_recv()
        tab_share[s].wait_recv()

    def rotary(b, _):
        pltpu.make_async_copy(wqr_hbm.at[:, pl.ds(0, Q_BLOCK)], wqr.at[b], qr_sem.at[b]).wait()
        res = jnp.dot(cq_all[...].reshape(2 * rows, cq_all.shape[2]), wqr[b], preferred_element_type=f32).T
        cos_q, sin_q = tab_all[0:rot], tab_all[rot:rope]
        for i in range(Q_BLOCK // rope):
            lo = res[i * rope:i * rope + rot]
            hi = res[i * rope + rot:(i + 1) * rope]
            h = b * (Q_BLOCK // rope) + i
            q_ref[h, nope:nope + rot, :] = (lo * cos_q - hi * sin_q).astype(jnp.bfloat16)
            q_ref[h, nope + rot:nope + rope, :] = (hi * cos_q + lo * sin_q).astype(jnp.bfloat16)
        return 0

    lax.fori_loop(0, n_qr, rotary, 0)
    to_right[1].wait_recv()
    to_left[0].wait_recv()
    shares[4].start()
    shares[5].start()

    def plain(b, _):
        pltpu.make_async_copy(wuq_hbm.at[:, pl.ds(0, Q_BLOCK)], wuq.at[b], uq_sem.at[b]).wait()
        res = jnp.dot(cq_all[...].reshape(2 * rows, cq_all.shape[2]), wuq[b], preferred_element_type=f32).astype(jnp.bfloat16).T
        for i in range(Q_BLOCK // nope):
            q_ref[b * (Q_BLOCK // nope) + i, 0:nope, :] = res[i * nope:(i + 1) * nope]
        return 0

    lax.fori_loop(0, n_uq // 2, plain, 0)
    on_right.wait_recv()
    on_left.wait_recv()
    shares[6].start()
    shares[7].start()
    lax.fori_loop(n_uq // 2, n_uq, plain, 0)
    for i in range(8):
        shares[i].wait_recv()
    out = pltpu.make_async_copy(lat, lat_hbm, lat_sem)
    out.start()
    for c in to_right + to_left + [on_right, on_left] + shares + cq_share + tab_share:
        c.wait_send()
    out.wait()


def latents(tok_x, w_dkv, w_kr, w_dq, w_uq, w_qr, g_q, g_kv, tab, n_ctx):
    rows, width = tok_x.shape
    rank, rope, q_rank = w_dkv.shape[1], w_kr.shape[1], w_dq.shape[1]
    heads = w_qr.shape[1] // rope // 2
    nope = w_uq.shape[1] // heads // 2
    bf16, f32 = jnp.bfloat16, jnp.float32
    vmem = pl.BlockSpec(memory_space=pltpu.VMEM)
    hbm = pl.BlockSpec(memory_space=pl.ANY)
    dma = pltpu.SemaphoreType.DMA
    n_uq, n_qr = heads * nope // Q_BLOCK, heads * rope // Q_BLOCK
    lat_width = rank + 128
    assert n_ctx == 8 and rope <= 128
    lat, q_t = pl.pallas_call(
        functools.partial(latent_kernel, n_ctx),
        out_shape=[jax.ShapeDtypeStruct((2 * n_ctx, rows // 2, lat_width), bf16), jax.ShapeDtypeStruct((heads, nope + rope, 2 * rows), bf16)],
        in_specs=[hbm] * 6 + [vmem] * 4,
        out_specs=[hbm, vmem],
        scratch_shapes=[
            pltpu.VMEM((rows, width), bf16), pltpu.VMEM((width, rank), bf16), pltpu.VMEM((width, rope), bf16), pltpu.VMEM((Q_SLOTS, width, Q_BLOCK), bf16),
            pltpu.VMEM((n_uq, q_rank, Q_BLOCK), bf16), pltpu.VMEM((n_qr, q_rank, Q_BLOCK), bf16),
            pltpu.VMEM((rows, rank), f32), pltpu.VMEM((rows, rope), f32), pltpu.VMEM((rows, q_rank), f32),
            pltpu.VMEM((4, rows // 2, q_rank), bf16), pltpu.VMEM((rope, 2 * rows), f32), pltpu.VMEM((2 * n_ctx, rows // 2, lat_width), bf16),
            dma((K_CHUNKS,)), dma((K_CHUNKS,)), dma((K_CHUNKS,)), dma((Q_SLOTS,)), dma((n_uq,)), dma((n_qr,)),
            dma((6,)), dma((6,)), dma((8,)), dma((8,)), dma((2,)), dma((2,)), dma((2,)), dma((2,)), dma,
        ],
        compiler_params=pltpu.CompilerParams(collective_id=2, has_side_effects=True, vmem_limit_bytes=62 * 1024 * 1024),
        name='latents',
    )(tok_x, w_dkv, w_kr, w_dq, w_uq, w_qr, g_q.astype(f32)[None], g_kv.astype(f32)[None], tab.T, tab)
    return lat.reshape(n_ctx * rows, lat_width), q_t


def solution(mesh):
    tok_spec = P(('dp', 'ctx'), None)
    pos_spec = P(('dp', 'ctx'))
    full_mat = P(None, None)
    full_vec = P(None)
    col_spec = P(None, 'tp')
    row_spec = P('tp', None)

    def local_step(tok_x, tok_pos, w_dq, g_q, w_uq, w_qr, w_dkv, g_kv, w_kr, w_uk, w_uv, w_o):
        rope_dim = w_kr.shape[1]
        heads_loc = w_qr.shape[1] // rope_dim
        nope_dim = w_uq.shape[1] // heads_loc
        score_scale = (nope_dim + rope_dim) ** -0.5
        n_ctx = mesh.shape['ctx']
        tab = jnp.concatenate(rope_tables(tok_pos, rope_dim), axis=-1)
        lat, q_t = latents(tok_x, w_dkv, w_kr, w_dq, w_uq, w_qr, g_q, g_kv, tab, n_ctx)
        return mix(q_t, lat, w_uk, w_uv, w_o, mesh.shape['tp'], n_ctx, score_scale)

    return jax.shard_map(local_step, mesh=mesh,
                         in_specs=(tok_spec, pos_spec, full_mat, full_vec, col_spec, col_spec, full_mat, full_vec, full_mat, col_spec, col_spec, row_spec),
                         out_specs=tok_spec, check_vma=False)
```

```python
import functools

import jax
import jax.numpy as jnp
from jax import lax
from jax.experimental import pallas as pl
from jax.experimental.pallas import tpu as pltpu
from jax.sharding import PartitionSpec as P

ROPE_BASE = 10000.0
NORM_EPS = 1e-6


def rope_table(pos_vals, rope_dim):
    half_dim = rope_dim // 2
    lane = lax.broadcasted_iota(jnp.int32, (1, 128), 1)
    inv_freq = ROPE_BASE ** (-(lane % half_dim).astype(jnp.float32) * 2.0 / rope_dim)
    angles = pos_vals.astype(jnp.float32)[:, None] * inv_freq
    return jnp.where(lane % rope_dim < half_dim, jnp.cos(angles), jnp.sin(angles))


MESH = pl.DeviceIdType.MESH
KEY_BLOCK = 256
OUT_BLOCK = 512
W_SLOTS = 3
LAG = 3


def mix_kernel(n_tp, n_ctx, n_blk, scale, q_ref, lat_ref, wuk_hbm, wuv_hbm, w_hbm, out_hbm,
               wuk, wuv, wuv_t, lat_t, kcat, v_t, s_buf, p_buf, o_buf, o_all, wbuf, part, recv, ybuf,
               up_sem, w_sem, o_send, o_recv, rs_send, rs_recv, ag_send, ag_recv, out_sem):
    f32, bf16 = jnp.float32, jnp.bfloat16
    ctx = lax.axis_index('ctx')
    col = ctx // 2
    core = lax.rem(ctx, 2)
    mate = ctx + 1 - 2 * core
    n_col = n_ctx // 2
    me = lax.axis_index('tp')
    right = lax.rem(me + 1, n_tp)
    left = lax.rem(me + n_tp - 1, n_tp)
    across = lax.rem(me + 2, n_tp)
    peer = (right, left)
    step_of = (n_tp - 1, 1)
    heads = q_ref.shape[0]
    n_hp = heads // 2
    rank = wuk.shape[1]
    v_dim = v_t.shape[0] // 2
    nope = wuk.shape[2] // 2
    rope = q_ref.shape[1] - nope
    exp_scale = scale * 1.4426950408889634
    blk = wbuf.shape[2]
    rows = part.shape[3]
    n_pair = n_blk // 2
    half = o_all.shape[2]

    def up_copy(src, dst, which, hp):
        cols = dst.shape[2]
        return pltpu.make_async_copy(src.at[:, pl.ds(pl.multiple_of((core * n_hp + hp) * cols, cols), cols)], dst.at[hp], up_sem.at[which, hp])

    def w_copy(i):
        b = lax.rem(i, n_blk)
        slot = lax.rem(i, W_SLOTS)
        return pltpu.make_async_copy(w_hbm.at[:, pl.ds(pl.multiple_of(b * blk, blk), blk)], wbuf.at[slot], w_sem.at[slot])

    def chunk_at(way, hop):
        return lax.rem(me + (hop + 1) * step_of[way], n_tp)

    def rs_first(sel, b, way):
        return pltpu.make_async_remote_copy(src_ref=part.at[sel, b, chunk_at(way, 0)], dst_ref=recv.at[sel, b, 0], send_sem=rs_send.at[sel, b, 0],
                                            recv_sem=rs_recv.at[sel, b, 0], device_id={'tp': peer[way]}, device_id_type=MESH)

    def rs_next(sel, b, way, hop):
        return pltpu.make_async_remote_copy(src_ref=recv.at[sel, b, hop - 1], dst_ref=recv.at[sel, b, hop], send_sem=rs_send.at[sel, b, hop],
                                            recv_sem=rs_recv.at[sel, b, hop], device_id={'tp': peer[way]}, device_id_type=MESH)

    def rs_arrived(sel, b, way, hop):
        pltpu.make_async_remote_copy(src_ref=recv.at[sel, b, hop], dst_ref=recv.at[sel, b, hop], send_sem=rs_send.at[sel, b, hop],
                                     recv_sem=rs_recv.at[sel, b, hop], device_id={'tp': peer[way]}, device_id_type=MESH).wait_recv()

    def ag_copy(sel, b, slot, way, chunk):
        return pltpu.make_async_remote_copy(src_ref=ybuf.at[sel, chunk, b], dst_ref=ybuf.at[sel, chunk, b], send_sem=ag_send.at[sel, b, slot],
                                            recv_sem=ag_recv.at[sel, b, slot], device_id={'tp': peer[way]}, device_id_type=MESH)

    def out_copy(sel, b, chunk):
        return pltpu.make_async_copy(ybuf.at[sel, chunk, b],
                                     out_hbm.at[pl.ds(pl.multiple_of(sel * half + chunk * rows, rows), rows), pl.ds(pl.multiple_of(b * blk, blk), blk)],
                                     out_sem.at[sel, chunk, b])

    own_at = (core, 3 - core)
    mate_at = (1 - core, 2 + core)

    def o_share(sel):
        return pltpu.make_async_remote_copy(src_ref=o_buf.at[pl.ds(pl.multiple_of(mate_at[sel] * half, half), half)], dst_ref=o_all.at[sel, core],
                                            send_sem=o_send.at[sel], recv_sem=o_recv.at[sel], device_id={'ctx': mate}, device_id_type=MESH)

    for hp in range(n_hp):
        up_copy(wuk_hbm, wuk, 0, hp).start()
        up_copy(wuv_hbm, wuv, 1, hp).start()
    for i in range(W_SLOTS):
        w_copy(i).start()
    barrier = pltpu.get_barrier_semaphore()
    for neighbour in peer:
        pl.semaphore_signal(barrier, inc=1, device_id={'tp': neighbour}, device_id_type=MESH)
    pl.semaphore_signal(barrier, inc=1, device_id={'ctx': mate}, device_id_type=MESH)
    for i in range(lat_ref.shape[0] // KEY_BLOCK):
        lat_t[:, i * KEY_BLOCK:(i + 1) * KEY_BLOCK] = lat_ref[i * KEY_BLOCK:(i + 1) * KEY_BLOCK, 0:rank].T
        for g in range(2):
            kcat[g, i * KEY_BLOCK:(i + 1) * KEY_BLOCK, nope:nope + rope] = lat_ref[i * KEY_BLOCK:(i + 1) * KEY_BLOCK, rank:rank + rope]
    for hp in range(n_hp):
        up_copy(wuk_hbm, wuk, 0, hp).wait()
        up_copy(wuv_hbm, wuv, 1, hp).wait()
        wuv_t[hp] = wuv[hp].T
    pl.semaphore_wait(barrier, 3)

    def attend(sel, n_key, serve):
        q_cols = slice(sel * KEY_BLOCK, (sel + 1) * KEY_BLOCK)
        key_i = lax.broadcasted_iota(jnp.int32, (KEY_BLOCK, KEY_BLOCK), 0)
        q_i = lax.broadcasted_iota(jnp.int32, (KEY_BLOCK, KEY_BLOCK), 1)
        visible = key_i <= q_i

        def pair_step(hp, _):
            span = n_key * KEY_BLOCK
            k2 = jnp.dot(lat_ref[0:span, 0:rank], wuk[hp], preferred_element_type=f32).astype(bf16)
            kcat[0, 0:span, 0:nope] = k2[:, :nope]
            kcat[1, 0:span, 0:nope] = k2[:, nope:]
            v_t[:, 0:span] = jnp.dot(wuv_t[hp], lat_t[:, 0:span], preferred_element_type=f32).astype(bf16)
            for g in range(2):
                s_buf[g, 0:span] = jnp.dot(kcat[g, 0:span, 0:nope + rope], q_ref[2 * hp + g, :, q_cols], preferred_element_type=f32)
            total = []
            for g in range(2):
                top8 = None
                for i in range(n_key):
                    s = s_buf[g, i * KEY_BLOCK:(i + 1) * KEY_BLOCK]
                    if i == n_key - 1:
                        s = jnp.where(visible, s, -1e30)
                    blk8 = jnp.max(s.reshape(KEY_BLOCK // 8, 8, KEY_BLOCK), axis=0)
                    top8 = blk8 if top8 is None else jnp.maximum(top8, blk8)
                top = jnp.max(top8, axis=0, keepdims=True) * exp_scale
                sum8 = None
                for i in range(n_key):
                    keys = slice(i * KEY_BLOCK, (i + 1) * KEY_BLOCK)
                    s = s_buf[g, keys]
                    if i == n_key - 1:
                        s = jnp.where(visible, s, -1e30)
                    p = jnp.exp2(s * exp_scale - top)
                    blk8 = jnp.sum(p.reshape(KEY_BLOCK // 8, 8, KEY_BLOCK), axis=0)
                    sum8 = blk8 if sum8 is None else sum8 + blk8
                    p_buf[keys, g * KEY_BLOCK:(g + 1) * KEY_BLOCK] = p.astype(bf16)
                total.append(jnp.sum(sum8, axis=0, keepdims=True))
            o_t = jnp.dot(v_t[:, 0:span], p_buf[0:span], preferred_element_type=f32)
            for g in range(2):
                o_g = o_t[g * v_dim:(g + 1) * v_dim, g * KEY_BLOCK:(g + 1) * KEY_BLOCK] / total[g]
                o_buf[q_cols, pl.ds(pl.multiple_of((2 * hp + g) * v_dim, v_dim), v_dim)] = o_g.T.astype(bf16)
            if serve is not None:
                serve(hp)
            return 0

        lax.fori_loop(0, n_hp, pair_step, 0)

    def exchange(sel):
        o_share(sel).start()
        o_all[sel, core] = o_buf[pl.ds(pl.multiple_of(own_at[sel] * half, half), half), :]
        o_share(sel).wait()

    def product(sel, p):
        for way in range(2):
            b = 2 * p + way
            i = sel * n_blk + b
            slot = lax.rem(i, W_SLOTS)
            w_copy(i).wait()
            depth = o_all.shape[3]
            res = jnp.dot(o_all[sel, 0], wbuf[slot, 0:depth], preferred_element_type=f32) + jnp.dot(o_all[sel, 1], wbuf[slot, depth:], preferred_element_type=f32)
            part[sel, b] = res.reshape(n_tp, rows, blk)

            @pl.when(i + W_SLOTS < 2 * n_blk)
            def _():
                w_copy(i + W_SLOTS).start()

            rs_first(sel, b, way).start()

    def forward(sel, p, hop):
        for way in range(2):
            b = 2 * p + way
            rs_arrived(sel, b, way, hop - 1)
            recv[sel, b, hop - 1] = recv[sel, b, hop - 1] + part[sel, b, chunk_at(way, hop)]
        for way in range(2):
            rs_next(sel, 2 * p + way, way, hop).start()

    def finish(sel, p):
        for way in range(2):
            b = 2 * p + way
            rs_arrived(sel, b, way, n_tp - 2)
            ybuf[sel, me, b] = (recv[sel, b, n_tp - 2] + part[sel, b, me]).astype(ybuf.dtype)
        for way in range(2):
            b = 2 * p + way
            ag_copy(sel, b, 0, 0, me).start()
            ag_copy(sel, b, 1, 1, me).start()
            out_copy(sel, b, me).start()

    def relay(sel, p):
        ag_copy(sel, 2 * p, 0, 0, left).wait_recv()
        ag_copy(sel, 2 * p, 2, 0, left).start()
        ag_copy(sel, 2 * p + 1, 1, 1, right).wait_recv()
        ag_copy(sel, 2 * p + 1, 2, 1, right).start()
        out_copy(sel, 2 * p, left).start()
        out_copy(sel, 2 * p + 1, right).start()

    def drain(sel, p):
        ag_copy(sel, 2 * p, 1, 1, right).wait_recv()
        out_copy(sel, 2 * p, right).start()
        ag_copy(sel, 2 * p + 1, 0, 0, left).wait_recv()
        out_copy(sel, 2 * p + 1, left).start()
        for way in range(2):
            b = 2 * p + way
            ag_copy(sel, b, 2, way, across).wait_recv()
            out_copy(sel, b, across).start()

    def settle(sel, p):
        for way in range(2):
            b = 2 * p + way
            rs_first(sel, b, way).wait_send()
            for hop in range(1, n_tp - 1):
                rs_next(sel, b, way, hop).wait_send()
            ag_copy(sel, b, 0, 0, me).wait_send()
            ag_copy(sel, b, 1, 1, me).wait_send()
            ag_copy(sel, b, 2, way, left if way == 0 else right).wait_send()
            for chunk in range(n_tp):
                out_copy(sel, b, chunk).wait()

    def loop(start, stop, body):
        def step(p, _):
            body(p)
            return 0
        lax.fori_loop(start, stop, step, 0)

    for v in range(n_col):
        pl.when(col == v)(functools.partial(attend, 0, v + 1, None))
    exchange(0)

    def early(p):
        product(0, p)

        @pl.when(p >= LAG)
        def _():
            forward(0, p - LAG, 1)

    loop(0, n_pair, early)
    hop1_left = n_pair - LAG

    def serve(hp):
        for j in range(2):
            n = hop1_left + 2 * hp + j
            pl.when(n < n_pair)(lambda: forward(0, n, 1))
            pl.when((n >= n_pair) & (n < 2 * n_pair))(lambda: forward(0, n - n_pair, 2))
            pl.when((n >= 2 * n_pair) & (n < 3 * n_pair))(lambda: finish(0, n - 2 * n_pair))

    for v in range(n_col):
        pl.when(col == v)(functools.partial(attend, 1, 2 * n_col - v, serve))
    served = min(hop1_left + 2 * n_hp, 3 * n_pair) - 2 * n_pair
    exchange(1)

    def late(p):
        product(1, p)
        pl.when(p + served < n_pair)(lambda: finish(0, p + served))

        @pl.when(p >= LAG)
        def _():
            forward(1, p - LAG, 1)

        relay(0, p)

    loop(0, n_pair, late)
    loop(hop1_left, n_pair, lambda p: forward(1, p, 1))
    loop(0, n_pair, lambda p: forward(1, p, 2))

    def close(p):
        finish(1, p)
        pl.when(p > 0)(lambda: relay(1, p - 1))
        drain(0, p)

    loop(0, n_pair, close)
    relay(1, n_pair - 1)
    loop(0, n_pair, lambda p: drain(1, p))
    o_wait = n_pair
    loop(0, o_wait, lambda p: settle(0, p))
    loop(0, o_wait, lambda p: settle(1, p))


def mix(q_t, lat, w_uk, w_uv, w_o, n_tp, n_ctx, scale):
    heads, q_dim, q_count = q_t.shape
    keys, rank = lat.shape[0], w_uk.shape[0]
    nope = w_uk.shape[1] // (2 * heads)
    rope = q_dim - nope
    v_dim = w_uv.shape[1] // (2 * heads)
    n_hp = heads // 2
    depth, width = w_o.shape
    n_blk = width // OUT_BLOCK
    half = q_count // 4
    rows = half // n_tp
    assert n_tp == 4 and n_blk % 2 == 0 and width % OUT_BLOCK == 0
    assert q_count == 2 * KEY_BLOCK and keys == n_ctx * KEY_BLOCK
    bf16, f32 = jnp.bfloat16, jnp.float32
    vmem = pl.BlockSpec(memory_space=pltpu.VMEM)
    hbm = pl.BlockSpec(memory_space=pl.ANY)
    dma = pltpu.SemaphoreType.DMA
    return pl.pallas_call(
        functools.partial(mix_kernel, n_tp, n_ctx, n_blk, scale),
        out_shape=jax.ShapeDtypeStruct((2 * half, width), bf16),
        in_specs=[vmem, vmem, hbm, hbm, hbm],
        out_specs=hbm,
        scratch_shapes=[
            pltpu.VMEM((n_hp, rank, 2 * nope), bf16), pltpu.VMEM((n_hp, rank, 2 * v_dim), bf16), pltpu.VMEM((n_hp, 2 * v_dim, rank), bf16),
            pltpu.VMEM((rank, keys), bf16), pltpu.VMEM((2, keys, nope + rope), bf16), pltpu.VMEM((2 * v_dim, keys), bf16),
            pltpu.VMEM((2, keys, KEY_BLOCK), f32), pltpu.VMEM((keys, 2 * KEY_BLOCK), bf16),
            pltpu.VMEM((q_count, heads * v_dim), bf16), pltpu.VMEM((2, 2, half, depth // 2), bf16),
            pltpu.VMEM((W_SLOTS, depth, OUT_BLOCK), bf16),
            pltpu.VMEM((2, n_blk, n_tp, rows, OUT_BLOCK), f32),
            pltpu.VMEM((2, n_blk, n_tp - 1, rows, OUT_BLOCK), f32),
            pltpu.VMEM((2, n_tp, n_blk, rows, OUT_BLOCK), bf16),
            dma((2, n_hp)), dma((W_SLOTS,)), dma((2,)), dma((2,)), dma((2, n_blk, n_tp - 1)), dma((2, n_blk, n_tp - 1)),
            dma((2, n_blk, 3)), dma((2, n_blk, 3)), dma((2, n_tp, n_blk)),
        ],
        compiler_params=pltpu.CompilerParams(collective_id=1, has_side_effects=True, vmem_limit_bytes=63 * 1024 * 1024),
        name='mix',
    )(q_t, lat, w_uk, w_uv, w_o)


K_CHUNKS = 4
Q_BLOCK = 256


def latent_kernel(n_ctx, x_hbm, wdkv_hbm, wkr_hbm, wdq_hbm, wuq_hbm, wqr_hbm, gain_ref, tab_ref, lat_hbm, q_ref,
                  x_v, wdkv, wkr, wdq, wuq, wqr, kv_acc, kr_acc, cq_acc, cq_all, tab_all, lat,
                  x_sem, dkv_sem, kr_sem, dq_sem, uq_sem, qr_sem, ring_send, ring_recv, mate_send, mate_recv, cq_send, cq_recv, tab_send, tab_recv, lat_sem):
    me = lax.axis_index('ctx')
    part = lax.rem(me, 2)
    mate = me + 1 - 2 * part
    right = lax.rem(me + 2, n_ctx)
    left = lax.rem(me + n_ctx - 2, n_ctx)
    far = lax.rem(me + 4, n_ctx)
    f32 = jnp.float32
    rows, width = x_v.shape
    half = rows // 2
    rank = kv_acc.shape[1]
    rope = kr_acc.shape[1]
    rot = rope // 2
    kc = width // K_CHUNKS
    n_uq, n_qr = wuq.shape[0], wqr.shape[0]
    nope = q_ref.shape[1] - rope

    def kcols(k):
        return pl.ds(k * kc, kc)

    x_copy = [pltpu.make_async_copy(x_hbm.at[:, kcols(k)], x_v.at[:, kcols(k)], x_sem.at[k]) for k in range(K_CHUNKS)]
    dkv_copy = [pltpu.make_async_copy(wdkv_hbm.at[kcols(k)], wdkv.at[kcols(k)], dkv_sem.at[k]) for k in range(K_CHUNKS)]
    kr_copy = [pltpu.make_async_copy(wkr_hbm.at[:, kcols(k)], wkr.at[:, kcols(k)], kr_sem.at[k]) for k in range(K_CHUNKS)]
    dq_copy = [pltpu.make_async_copy(wdq_hbm.at[kcols(k)], wdq.at[kcols(k)], dq_sem.at[k]) for k in range(K_CHUNKS)]
    uq_copy = [pltpu.make_async_copy(wuq_hbm.at[:, pl.ds(pl.multiple_of((part * n_uq + b) * Q_BLOCK, Q_BLOCK), Q_BLOCK)], wuq.at[b], uq_sem.at[b]) for b in range(n_uq)]
    qr_copy = [pltpu.make_async_copy(wqr_hbm.at[:, pl.ds(pl.multiple_of((part * n_qr + b) * Q_BLOCK, Q_BLOCK), Q_BLOCK)], wqr.at[b], qr_sem.at[b]) for b in range(n_qr)]

    def piece(dev, sub):
        return dev if sub == 0 else 2 * n_ctx - 1 - dev

    def send(src, dst, send_sem, recv_sem, dev):
        return pltpu.make_async_remote_copy(src_ref=src, dst_ref=dst, send_sem=send_sem, recv_sem=recv_sem, device_id={'ctx': dev}, device_id_type=MESH)

    def ring(slot, src_dev, sub, dev):
        return send(lat.at[piece(src_dev, sub)], lat.at[piece(src_dev, sub)], ring_send.at[slot], ring_recv.at[slot], dev)

    def share(slot, src_dev, sub):
        return send(lat.at[piece(src_dev, sub)], lat.at[piece(src_dev, sub)], mate_send.at[slot], mate_recv.at[slot], mate)

    to_right = [ring(0, me, 0, right), ring(1, me, 1, right)]
    to_left = [ring(2, me, 0, left), ring(3, me, 1, left)]
    on_right = ring(4, left, 0, right)
    on_left = ring(5, right, 1, left)
    order = [(me, 0), (me, 1), (left, 0), (right, 1), (left, 1), (right, 0), (far, 0), (far, 1)]
    shares = [share(i, d, s) for i, (d, s) in enumerate(order)]
    slot_of = (part, 3 - part)
    cq_share = [send(cq_all.at[slot_of[s]], cq_all.at[slot_of[s]], cq_send.at[s], cq_recv.at[s], mate) for s in range(2)]

    def lanes(s):
        return pl.ds(pl.multiple_of(slot_of[s] * half, half), half)

    tab_share = [send(tab_all.at[:, lanes(s)], tab_all.at[:, lanes(s)], tab_send.at[s], tab_recv.at[s], mate) for s in range(2)]

    for k in range(K_CHUNKS):
        x_copy[k].start()
        dkv_copy[k].start()
        kr_copy[k].start()
    for k in range(K_CHUNKS):
        dq_copy[k].start()
    barrier = pltpu.get_barrier_semaphore()
    for dev in (mate, right, left):
        pl.semaphore_signal(barrier, inc=1, device_id={'ctx': dev}, device_id_type=MESH)
    for s in range(2):
        tab_all[:, lanes(s)] = tab_ref[s * half:(s + 1) * half].T[0:rope]

    for k in range(K_CHUNKS):
        cols = slice(k * kc, (k + 1) * kc)
        x_copy[k].wait()
        dkv_copy[k].wait()
        kr_copy[k].wait()
        kv_new = jnp.dot(x_v[:, cols], wdkv[cols], preferred_element_type=f32)
        kr_new = lax.dot_general(x_v[:, cols], wkr[:, cols], (((1,), (1,)), ((), ())), preferred_element_type=f32)
        if k == 0:
            kv_acc[...] = kv_new
            kr_acc[...] = kr_new
        else:
            kv_acc[...] += kv_new
            kr_acc[...] += kr_new
    kv = kv_acc[...]
    c_kv = (kv * lax.rsqrt(jnp.mean(kv * kv, axis=-1, keepdims=True) + NORM_EPS) * gain_ref[0:1, 0:rank]).astype(jnp.bfloat16)
    kr = kr_acc[...]
    cos_k, sin_k = tab_ref[:, :rot], tab_ref[:, rot:rope]
    k_lo = (kr[:, :rot] * cos_k - kr[:, rot:] * sin_k).astype(jnp.bfloat16)
    k_hi = (kr[:, rot:] * cos_k + kr[:, :rot] * sin_k).astype(jnp.bfloat16)
    pad = jnp.zeros((half, lat.shape[2] - rank - rope), jnp.bfloat16)
    for s in range(2):
        own = slice(s * half, (s + 1) * half)
        lat[piece(me, s), :, 0:rank] = c_kv[own]
        lat[piece(me, s), :, rank:] = jnp.concatenate([k_lo[own], k_hi[own], pad], axis=1)

    pl.semaphore_wait(barrier, 3)
    for s in range(2):
        to_right[s].start()
        to_left[1 - s].start()
    for s in range(2):
        tab_share[s].start()
        shares[s].start()

    for k in range(K_CHUNKS):
        cols = slice(k * kc, (k + 1) * kc)
        dq_copy[k].wait()
        cq_new = jnp.dot(x_v[:, cols], wdq[cols], preferred_element_type=f32)
        if k == 0:
            cq_acc[...] = cq_new
            for c in qr_copy + uq_copy:
                c.start()
        else:
            cq_acc[...] += cq_new
    for s in range(2):
        own = slice(s * half, (s + 1) * half)
        cq = cq_acc[own]
        cq_all[slot_of[s]] = (cq * lax.rsqrt(jnp.mean(cq * cq, axis=-1, keepdims=True) + NORM_EPS) * gain_ref[0:1, rank:]).astype(jnp.bfloat16)
        cq_share[s].start()

    to_right[0].wait_recv()
    on_right.start()
    to_left[1].wait_recv()
    on_left.start()
    shares[2].start()
    shares[3].start()
    for s in range(2):
        cq_share[s].wait_recv()
        tab_share[s].wait_recv()

    def rotary(b, _):
        pltpu.make_async_copy(wqr_hbm.at[:, pl.ds(0, Q_BLOCK)], wqr.at[b], qr_sem.at[b]).wait()
        res = jnp.dot(cq_all[...].reshape(2 * rows, cq_all.shape[2]), wqr[b], preferred_element_type=f32).T
        cos_q, sin_q = tab_all[0:rot], tab_all[rot:rope]
        for i in range(Q_BLOCK // rope):
            lo = res[i * rope:i * rope + rot]
            hi = res[i * rope + rot:(i + 1) * rope]
            h = b * (Q_BLOCK // rope) + i
            q_ref[h, nope:nope + rot, :] = (lo * cos_q - hi * sin_q).astype(jnp.bfloat16)
            q_ref[h, nope + rot:nope + rope, :] = (hi * cos_q + lo * sin_q).astype(jnp.bfloat16)
        return 0

    lax.fori_loop(0, n_qr, rotary, 0)
    to_right[1].wait_recv()
    to_left[0].wait_recv()
    shares[4].start()
    shares[5].start()

    def plain(b, _):
        pltpu.make_async_copy(wuq_hbm.at[:, pl.ds(0, Q_BLOCK)], wuq.at[b], uq_sem.at[b]).wait()
        res = jnp.dot(cq_all[...].reshape(2 * rows, cq_all.shape[2]), wuq[b], preferred_element_type=f32).astype(jnp.bfloat16).T
        for i in range(Q_BLOCK // nope):
            q_ref[b * (Q_BLOCK // nope) + i, 0:nope, :] = res[i * nope:(i + 1) * nope]
        return 0

    lax.fori_loop(0, n_uq // 2, plain, 0)
    on_right.wait_recv()
    on_left.wait_recv()
    shares[6].start()
    shares[7].start()
    lax.fori_loop(n_uq // 2, n_uq, plain, 0)
    for i in range(8):
        shares[i].wait_recv()
    out = pltpu.make_async_copy(lat, lat_hbm, lat_sem)
    out.start()
    for c in to_right + to_left + [on_right, on_left] + shares + cq_share + tab_share:
        c.wait_send()
    out.wait()


def latents(tok_x, w_dkv, w_kr, w_dq, w_uq, w_qr, g_q, g_kv, tab, n_ctx):
    rows, width = tok_x.shape
    rank, rope, q_rank = w_dkv.shape[1], w_kr.shape[1], w_dq.shape[1]
    heads = w_qr.shape[1] // rope // 2
    nope = w_uq.shape[1] // heads // 2
    bf16, f32 = jnp.bfloat16, jnp.float32
    vmem = pl.BlockSpec(memory_space=pltpu.VMEM)
    hbm = pl.BlockSpec(memory_space=pl.ANY)
    dma = pltpu.SemaphoreType.DMA
    n_uq, n_qr = heads * nope // Q_BLOCK, heads * rope // Q_BLOCK
    lat_width = rank + 128
    assert n_ctx == 8 and rope <= 128
    gain = jnp.broadcast_to(jnp.concatenate([g_kv, g_q]).astype(f32)[None], (8, rank + q_rank))
    lat, q_t = pl.pallas_call(
        functools.partial(latent_kernel, n_ctx),
        out_shape=[jax.ShapeDtypeStruct((2 * n_ctx, rows // 2, lat_width), bf16), jax.ShapeDtypeStruct((heads, nope + rope, 2 * rows), bf16)],
        in_specs=[hbm] * 6 + [vmem] * 2,
        out_specs=[hbm, vmem],
        scratch_shapes=[
            pltpu.VMEM((rows, width), bf16), pltpu.VMEM((width, rank), bf16), pltpu.VMEM((rope, width), bf16), pltpu.VMEM((width, q_rank), bf16),
            pltpu.VMEM((n_uq, q_rank, Q_BLOCK), bf16), pltpu.VMEM((n_qr, q_rank, Q_BLOCK), bf16),
            pltpu.VMEM((rows, rank), f32), pltpu.VMEM((rows, rope), f32), pltpu.VMEM((rows, q_rank), f32),
            pltpu.VMEM((4, rows // 2, q_rank), bf16), pltpu.VMEM((rope, 2 * rows), f32), pltpu.VMEM((2 * n_ctx, rows // 2, lat_width), bf16),
            dma((K_CHUNKS,)), dma((K_CHUNKS,)), dma((K_CHUNKS,)), dma((K_CHUNKS,)), dma((n_uq,)), dma((n_qr,)),
            dma((6,)), dma((6,)), dma((8,)), dma((8,)), dma((2,)), dma((2,)), dma((2,)), dma((2,)), dma,
        ],
        compiler_params=pltpu.CompilerParams(collective_id=2, has_side_effects=True, vmem_limit_bytes=62 * 1024 * 1024),
        name='latents',
    )(tok_x, w_dkv, w_kr.T, w_dq, w_uq, w_qr, gain, tab)
    return lat.reshape(n_ctx * rows, lat_width), q_t


def solution(mesh):
    tok_spec = P(('dp', 'ctx'), None)
    pos_spec = P(('dp', 'ctx'))
    full_mat = P(None, None)
    full_vec = P(None)
    col_spec = P(None, 'tp')
    row_spec = P('tp', None)

    def local_step(tok_x, tok_pos, w_dq, g_q, w_uq, w_qr, w_dkv, g_kv, w_kr, w_uk, w_uv, w_o):
        rope_dim = w_kr.shape[1]
        heads_loc = w_qr.shape[1] // rope_dim
        nope_dim = w_uq.shape[1] // heads_loc
        score_scale = (nope_dim + rope_dim) ** -0.5
        n_ctx = mesh.shape['ctx']
        tab = rope_table(tok_pos, rope_dim)
        lat, q_t = latents(tok_x, w_dkv, w_kr, w_dq, w_uq, w_qr, g_q, g_kv, tab, n_ctx)
        return mix(q_t, lat, w_uk, w_uv, w_o, mesh.shape['tp'], n_ctx, score_scale)

    return jax.shard_map(local_step, mesh=mesh,
                         in_specs=(tok_spec, pos_spec, full_mat, full_vec, col_spec, col_spec, full_mat, full_vec, full_mat, col_spec, col_spec, row_spec),
                         out_specs=tok_spec, check_vma=False)
```

```python
import functools

import jax
import jax.numpy as jnp
from jax import lax
from jax.experimental import pallas as pl
from jax.experimental.pallas import tpu as pltpu
from jax.sharding import PartitionSpec as P

ROPE_BASE = 10000.0
NORM_EPS = 1e-6


def rope_table(pos_vals, rope_dim):
    half_dim = rope_dim // 2
    lane = lax.broadcasted_iota(jnp.int32, (1, 128), 1)
    inv_freq = ROPE_BASE ** (-(lane % half_dim).astype(jnp.float32) * 2.0 / rope_dim)
    angles = pos_vals.astype(jnp.float32)[:, None] * inv_freq
    return jnp.where(lane % rope_dim < half_dim, jnp.cos(angles), jnp.sin(angles))


MESH = pl.DeviceIdType.MESH
KEY_BLOCK = 256
OUT_BLOCK = 512
W_SLOTS = 3
LAG = 3


def mix_kernel(n_tp, n_ctx, n_blk, scale, q_ref, lat_ref, wuk_hbm, wuv_hbm, w_hbm, out_hbm,
               wuk, wuv, wuv_t, lat_t, kcat, v_t, s_buf, top_buf, p_buf, o_buf, o_all, wbuf, part, recv, ybuf,
               up_sem, w_sem, o_send, o_recv, rs_send, rs_recv, ag_send, ag_recv, out_sem):
    f32, bf16 = jnp.float32, jnp.bfloat16
    ctx = lax.axis_index('ctx')
    col = ctx // 2
    core = lax.rem(ctx, 2)
    mate = ctx + 1 - 2 * core
    n_col = n_ctx // 2
    me = lax.axis_index('tp')
    right = lax.rem(me + 1, n_tp)
    left = lax.rem(me + n_tp - 1, n_tp)
    across = lax.rem(me + 2, n_tp)
    peer = (right, left)
    step_of = (n_tp - 1, 1)
    heads = q_ref.shape[0]
    n_hp = heads // 2
    rank = wuk.shape[1]
    v_dim = v_t.shape[1] // 2
    nope = wuk.shape[2] // 2
    rope = q_ref.shape[1] - nope
    exp_scale = scale * 1.4426950408889634
    blk = wbuf.shape[2]
    rows = part.shape[3]
    n_pair = n_blk // 2
    half = o_all.shape[2]

    def up_copy(src, dst, which, hp):
        cols = dst.shape[2]
        return pltpu.make_async_copy(src.at[:, pl.ds(pl.multiple_of((core * n_hp + hp) * cols, cols), cols)], dst.at[hp], up_sem.at[which, hp])

    def w_copy(i):
        b = lax.rem(i, n_blk)
        slot = lax.rem(i, W_SLOTS)
        return pltpu.make_async_copy(w_hbm.at[:, pl.ds(pl.multiple_of(b * blk, blk), blk)], wbuf.at[slot], w_sem.at[slot])

    def chunk_at(way, hop):
        return lax.rem(me + (hop + 1) * step_of[way], n_tp)

    def rs_first(sel, b, way):
        return pltpu.make_async_remote_copy(src_ref=part.at[sel, b, chunk_at(way, 0)], dst_ref=recv.at[sel, b, 0], send_sem=rs_send.at[sel, b, 0],
                                            recv_sem=rs_recv.at[sel, b, 0], device_id={'tp': peer[way]}, device_id_type=MESH)

    def rs_next(sel, b, way, hop):
        return pltpu.make_async_remote_copy(src_ref=recv.at[sel, b, hop - 1], dst_ref=recv.at[sel, b, hop], send_sem=rs_send.at[sel, b, hop],
                                            recv_sem=rs_recv.at[sel, b, hop], device_id={'tp': peer[way]}, device_id_type=MESH)

    def rs_arrived(sel, b, way, hop):
        pltpu.make_async_remote_copy(src_ref=recv.at[sel, b, hop], dst_ref=recv.at[sel, b, hop], send_sem=rs_send.at[sel, b, hop],
                                     recv_sem=rs_recv.at[sel, b, hop], device_id={'tp': peer[way]}, device_id_type=MESH).wait_recv()

    def ag_copy(sel, b, slot, way, chunk):
        return pltpu.make_async_remote_copy(src_ref=ybuf.at[sel, chunk, b], dst_ref=ybuf.at[sel, chunk, b], send_sem=ag_send.at[sel, b, slot],
                                            recv_sem=ag_recv.at[sel, b, slot], device_id={'tp': peer[way]}, device_id_type=MESH)

    def out_copy(sel, b, chunk):
        return pltpu.make_async_copy(ybuf.at[sel, chunk, b],
                                     out_hbm.at[pl.ds(pl.multiple_of(sel * half + chunk * rows, rows), rows), pl.ds(pl.multiple_of(b * blk, blk), blk)],
                                     out_sem.at[sel, chunk, b])

    own_at = (core, 3 - core)
    mate_at = (1 - core, 2 + core)

    def o_share(sel):
        return pltpu.make_async_remote_copy(src_ref=o_buf.at[pl.ds(pl.multiple_of(mate_at[sel] * half, half), half)], dst_ref=o_all.at[sel, core],
                                            send_sem=o_send.at[sel], recv_sem=o_recv.at[sel], device_id={'ctx': mate}, device_id_type=MESH)

    for hp in range(n_hp):
        up_copy(wuk_hbm, wuk, 0, hp).start()
        up_copy(wuv_hbm, wuv, 1, hp).start()
    for i in range(W_SLOTS):
        w_copy(i).start()
    barrier = pltpu.get_barrier_semaphore()
    for neighbour in peer:
        pl.semaphore_signal(barrier, inc=1, device_id={'tp': neighbour}, device_id_type=MESH)
    pl.semaphore_signal(barrier, inc=1, device_id={'ctx': mate}, device_id_type=MESH)
    for i in range(lat_ref.shape[0] // KEY_BLOCK):
        lat_t[:, i * KEY_BLOCK:(i + 1) * KEY_BLOCK] = lat_ref[i * KEY_BLOCK:(i + 1) * KEY_BLOCK, 0:rank].T
        for g in range(2):
            kcat[g, i * KEY_BLOCK:(i + 1) * KEY_BLOCK, nope:nope + rope] = lat_ref[i * KEY_BLOCK:(i + 1) * KEY_BLOCK, rank:rank + rope]
    for hp in range(n_hp):
        up_copy(wuk_hbm, wuk, 0, hp).wait()
        up_copy(wuv_hbm, wuv, 1, hp).wait()
        wuv_t[hp] = wuv[hp].T
    pl.semaphore_wait(barrier, 3)

    def attend(sel, n_key, serve):
        q_cols = slice(sel * KEY_BLOCK, (sel + 1) * KEY_BLOCK)
        key_i = lax.broadcasted_iota(jnp.int32, (KEY_BLOCK, KEY_BLOCK), 0)
        q_i = lax.broadcasted_iota(jnp.int32, (KEY_BLOCK, KEY_BLOCK), 1)
        visible = key_i <= q_i

        span = n_key * KEY_BLOCK

        def overlap(nxt, now):
            top8 = [None, None]
            sum8 = [None, None]
            top = None if now is None else [top_buf[g] for g in range(2)]
            for i in range(n_key):
                keys = slice(i * KEY_BLOCK, (i + 1) * KEY_BLOCK)
                if now is not None:
                    for g in range(2):
                        p = jnp.exp2(s_buf[g, keys] * exp_scale - top[g])
                        blk8 = jnp.sum(p.reshape(KEY_BLOCK // 8, 8, KEY_BLOCK), axis=0)
                        sum8[g] = blk8 if sum8[g] is None else sum8[g] + blk8
                        p_buf[keys, g * KEY_BLOCK:(g + 1) * KEY_BLOCK] = p.astype(bf16)
                k2 = jnp.dot(lat_ref[keys, 0:rank], wuk[nxt], preferred_element_type=f32).astype(bf16)
                kcat[0, keys, 0:nope] = k2[:, :nope]
                kcat[1, keys, 0:nope] = k2[:, nope:]
                v_t[lax.rem(nxt, 2), :, keys] = jnp.dot(wuv_t[nxt], lat_t[:, keys], preferred_element_type=f32).astype(bf16)
                for g in range(2):
                    sc = jnp.dot(kcat[g, keys, 0:nope + rope], q_ref[2 * nxt + g, :, q_cols], preferred_element_type=f32)
                    if i == n_key - 1:
                        sc = jnp.where(visible, sc, -1e30)
                    s_buf[g, keys] = sc
                    blk8 = jnp.max(sc.reshape(KEY_BLOCK // 8, 8, KEY_BLOCK), axis=0)
                    top8[g] = blk8 if top8[g] is None else jnp.maximum(top8[g], blk8)
            for g in range(2):
                top_buf[g] = jnp.max(top8[g], axis=0, keepdims=True) * exp_scale
            if now is not None:
                o_t = jnp.dot(v_t[lax.rem(now, 2), :, 0:span], p_buf[0:span], preferred_element_type=f32)
                for g in range(2):
                    o_g = o_t[g * v_dim:(g + 1) * v_dim, g * KEY_BLOCK:(g + 1) * KEY_BLOCK] / jnp.sum(sum8[g], axis=0, keepdims=True)
                    o_buf[q_cols, pl.ds(pl.multiple_of((2 * now + g) * v_dim, v_dim), v_dim)] = o_g.T.astype(bf16)

        overlap(0, None)

        def pair_step(hp, _):
            overlap(jnp.where(hp + 1 < n_hp, hp + 1, n_hp - 2), hp)
            if serve is not None:
                serve(hp)
            return 0

        lax.fori_loop(0, n_hp, pair_step, 0)

    def exchange(sel):
        o_share(sel).start()
        o_all[sel, core] = o_buf[pl.ds(pl.multiple_of(own_at[sel] * half, half), half), :]
        o_share(sel).wait()

    def product(sel, p):
        for way in range(2):
            b = 2 * p + way
            i = sel * n_blk + b
            slot = lax.rem(i, W_SLOTS)
            w_copy(i).wait()
            depth = o_all.shape[3]
            res = jnp.dot(o_all[sel, 0], wbuf[slot, 0:depth], preferred_element_type=f32) + jnp.dot(o_all[sel, 1], wbuf[slot, depth:], preferred_element_type=f32)
            part[sel, b] = res.reshape(n_tp, rows, blk)

            @pl.when(i + W_SLOTS < 2 * n_blk)
            def _():
                w_copy(i + W_SLOTS).start()

            rs_first(sel, b, way).start()

    def forward(sel, p, hop):
        for way in range(2):
            b = 2 * p + way
            rs_arrived(sel, b, way, hop - 1)
            recv[sel, b, hop - 1] = recv[sel, b, hop - 1] + part[sel, b, chunk_at(way, hop)]
        for way in range(2):
            rs_next(sel, 2 * p + way, way, hop).start()

    def finish(sel, p):
        for way in range(2):
            b = 2 * p + way
            rs_arrived(sel, b, way, n_tp - 2)
            ybuf[sel, me, b] = (recv[sel, b, n_tp - 2] + part[sel, b, me]).astype(ybuf.dtype)
        for way in range(2):
            b = 2 * p + way
            ag_copy(sel, b, 0, 0, me).start()
            ag_copy(sel, b, 1, 1, me).start()
            out_copy(sel, b, me).start()

    def relay(sel, p):
        ag_copy(sel, 2 * p, 0, 0, left).wait_recv()
        ag_copy(sel, 2 * p, 2, 0, left).start()
        ag_copy(sel, 2 * p + 1, 1, 1, right).wait_recv()
        ag_copy(sel, 2 * p + 1, 2, 1, right).start()
        out_copy(sel, 2 * p, left).start()
        out_copy(sel, 2 * p + 1, right).start()

    def drain(sel, p):
        ag_copy(sel, 2 * p, 1, 1, right).wait_recv()
        out_copy(sel, 2 * p, right).start()
        ag_copy(sel, 2 * p + 1, 0, 0, left).wait_recv()
        out_copy(sel, 2 * p + 1, left).start()
        for way in range(2):
            b = 2 * p + way
            ag_copy(sel, b, 2, way, across).wait_recv()
            out_copy(sel, b, across).start()

    def settle(sel, p):
        for way in range(2):
            b = 2 * p + way
            rs_first(sel, b, way).wait_send()
            for hop in range(1, n_tp - 1):
                rs_next(sel, b, way, hop).wait_send()
            ag_copy(sel, b, 0, 0, me).wait_send()
            ag_copy(sel, b, 1, 1, me).wait_send()
            ag_copy(sel, b, 2, way, left if way == 0 else right).wait_send()
            for chunk in range(n_tp):
                out_copy(sel, b, chunk).wait()

    def loop(start, stop, body):
        def step(p, _):
            body(p)
            return 0
        lax.fori_loop(start, stop, step, 0)

    for v in range(n_col):
        pl.when(col == v)(functools.partial(attend, 0, v + 1, None))
    exchange(0)

    def early(p):
        product(0, p)

        @pl.when(p >= LAG)
        def _():
            forward(0, p - LAG, 1)

    loop(0, n_pair, early)
    hop1_left = n_pair - LAG

    def serve(hp):
        for j in range(2):
            n = hop1_left + 2 * hp + j
            pl.when(n < n_pair)(lambda: forward(0, n, 1))
            pl.when((n >= n_pair) & (n < 2 * n_pair))(lambda: forward(0, n - n_pair, 2))
            pl.when((n >= 2 * n_pair) & (n < 3 * n_pair))(lambda: finish(0, n - 2 * n_pair))

    for v in range(n_col):
        pl.when(col == v)(functools.partial(attend, 1, 2 * n_col - v, serve))
    served = min(hop1_left + 2 * n_hp, 3 * n_pair) - 2 * n_pair
    exchange(1)

    def late(p):
        product(1, p)
        pl.when(p + served < n_pair)(lambda: finish(0, p + served))

        @pl.when(p >= LAG)
        def _():
            forward(1, p - LAG, 1)

        relay(0, p)

    loop(0, n_pair, late)
    loop(hop1_left, n_pair, lambda p: forward(1, p, 1))
    loop(0, n_pair, lambda p: forward(1, p, 2))

    def close(p):
        finish(1, p)
        pl.when(p > 0)(lambda: relay(1, p - 1))
        drain(0, p)

    loop(0, n_pair, close)
    relay(1, n_pair - 1)
    loop(0, n_pair, lambda p: drain(1, p))
    o_wait = n_pair
    loop(0, o_wait, lambda p: settle(0, p))
    loop(0, o_wait, lambda p: settle(1, p))


def mix(q_t, lat, w_uk, w_uv, w_o, n_tp, n_ctx, scale):
    heads, q_dim, q_count = q_t.shape
    keys, rank = lat.shape[0], w_uk.shape[0]
    nope = w_uk.shape[1] // (2 * heads)
    rope = q_dim - nope
    v_dim = w_uv.shape[1] // (2 * heads)
    n_hp = heads // 2
    depth, width = w_o.shape
    n_blk = width // OUT_BLOCK
    half = q_count // 4
    rows = half // n_tp
    assert n_tp == 4 and n_blk % 2 == 0 and width % OUT_BLOCK == 0
    assert q_count == 2 * KEY_BLOCK and keys == n_ctx * KEY_BLOCK
    bf16, f32 = jnp.bfloat16, jnp.float32
    vmem = pl.BlockSpec(memory_space=pltpu.VMEM)
    hbm = pl.BlockSpec(memory_space=pl.ANY)
    dma = pltpu.SemaphoreType.DMA
    return pl.pallas_call(
        functools.partial(mix_kernel, n_tp, n_ctx, n_blk, scale),
        out_shape=jax.ShapeDtypeStruct((2 * half, width), bf16),
        in_specs=[vmem, vmem, hbm, hbm, hbm],
        out_specs=hbm,
        scratch_shapes=[
            pltpu.VMEM((n_hp, rank, 2 * nope), bf16), pltpu.VMEM((n_hp, rank, 2 * v_dim), bf16), pltpu.VMEM((n_hp, 2 * v_dim, rank), bf16),
            pltpu.VMEM((rank, keys), bf16), pltpu.VMEM((2, keys, nope + rope), bf16), pltpu.VMEM((2, 2 * v_dim, keys), bf16),
            pltpu.VMEM((2, keys, KEY_BLOCK), f32), pltpu.VMEM((2, 1, KEY_BLOCK), f32), pltpu.VMEM((keys, 2 * KEY_BLOCK), bf16),
            pltpu.VMEM((q_count, heads * v_dim), bf16), pltpu.VMEM((2, 2, half, depth // 2), bf16),
            pltpu.VMEM((W_SLOTS, depth, OUT_BLOCK), bf16),
            pltpu.VMEM((2, n_blk, n_tp, rows, OUT_BLOCK), f32),
            pltpu.VMEM((2, n_blk, n_tp - 1, rows, OUT_BLOCK), f32),
            pltpu.VMEM((2, n_tp, n_blk, rows, OUT_BLOCK), bf16),
            dma((2, n_hp)), dma((W_SLOTS,)), dma((2,)), dma((2,)), dma((2, n_blk, n_tp - 1)), dma((2, n_blk, n_tp - 1)),
            dma((2, n_blk, 3)), dma((2, n_blk, 3)), dma((2, n_tp, n_blk)),
        ],
        compiler_params=pltpu.CompilerParams(collective_id=1, has_side_effects=True, vmem_limit_bytes=63 * 1024 * 1024),
        name='mix',
    )(q_t, lat, w_uk, w_uv, w_o)


K_CHUNKS = 4
Q_BLOCK = 256


def latent_kernel(n_ctx, x_hbm, wdkv_hbm, wkr_hbm, wdq_hbm, wuq_hbm, wqr_hbm, gain_ref, tab_ref, lat_hbm, q_ref,
                  x_v, wdkv, wkr, wdq, wuq, wqr, kv_acc, kr_acc, cq_acc, cq_all, tab_all, lat,
                  x_sem, dkv_sem, kr_sem, dq_sem, uq_sem, qr_sem, ring_send, ring_recv, mate_send, mate_recv, cq_send, cq_recv, tab_send, tab_recv, lat_sem):
    me = lax.axis_index('ctx')
    part = lax.rem(me, 2)
    mate = me + 1 - 2 * part
    right = lax.rem(me + 2, n_ctx)
    left = lax.rem(me + n_ctx - 2, n_ctx)
    far = lax.rem(me + 4, n_ctx)
    f32 = jnp.float32
    rows, width = x_v.shape
    half = rows // 2
    rank = kv_acc.shape[1]
    rope = kr_acc.shape[1]
    rot = rope // 2
    kc = width // K_CHUNKS
    n_uq, n_qr = wuq.shape[0], wqr.shape[0]
    nope = q_ref.shape[1] - rope

    def kcols(k):
        return pl.ds(k * kc, kc)

    x_copy = [pltpu.make_async_copy(x_hbm.at[:, kcols(k)], x_v.at[:, kcols(k)], x_sem.at[k]) for k in range(K_CHUNKS)]
    dkv_copy = [pltpu.make_async_copy(wdkv_hbm.at[kcols(k)], wdkv.at[kcols(k)], dkv_sem.at[k]) for k in range(K_CHUNKS)]
    kr_copy = [pltpu.make_async_copy(wkr_hbm.at[:, kcols(k)], wkr.at[:, kcols(k)], kr_sem.at[k]) for k in range(K_CHUNKS)]
    dq_copy = [pltpu.make_async_copy(wdq_hbm.at[kcols(k)], wdq.at[kcols(k)], dq_sem.at[k]) for k in range(K_CHUNKS)]
    uq_copy = [pltpu.make_async_copy(wuq_hbm.at[:, pl.ds(pl.multiple_of((part * n_uq + b) * Q_BLOCK, Q_BLOCK), Q_BLOCK)], wuq.at[b], uq_sem.at[b]) for b in range(n_uq)]
    qr_copy = [pltpu.make_async_copy(wqr_hbm.at[:, pl.ds(pl.multiple_of((part * n_qr + b) * Q_BLOCK, Q_BLOCK), Q_BLOCK)], wqr.at[b], qr_sem.at[b]) for b in range(n_qr)]

    def piece(dev, sub):
        return dev if sub == 0 else 2 * n_ctx - 1 - dev

    def send(src, dst, send_sem, recv_sem, dev):
        return pltpu.make_async_remote_copy(src_ref=src, dst_ref=dst, send_sem=send_sem, recv_sem=recv_sem, device_id={'ctx': dev}, device_id_type=MESH)

    def ring(slot, src_dev, sub, dev):
        return send(lat.at[piece(src_dev, sub)], lat.at[piece(src_dev, sub)], ring_send.at[slot], ring_recv.at[slot], dev)

    def share(slot, src_dev, sub):
        return send(lat.at[piece(src_dev, sub)], lat.at[piece(src_dev, sub)], mate_send.at[slot], mate_recv.at[slot], mate)

    to_right = [ring(0, me, 0, right), ring(1, me, 1, right)]
    to_left = [ring(2, me, 0, left), ring(3, me, 1, left)]
    on_right = ring(4, left, 0, right)
    on_left = ring(5, right, 1, left)
    order = [(me, 0), (me, 1), (left, 0), (right, 1), (left, 1), (right, 0), (far, 0), (far, 1)]
    shares = [share(i, d, s) for i, (d, s) in enumerate(order)]
    slot_of = (part, 3 - part)
    cq_share = [send(cq_all.at[slot_of[s]], cq_all.at[slot_of[s]], cq_send.at[s], cq_recv.at[s], mate) for s in range(2)]

    def lanes(s):
        return pl.ds(pl.multiple_of(slot_of[s] * half, half), half)

    tab_share = [send(tab_all.at[:, lanes(s)], tab_all.at[:, lanes(s)], tab_send.at[s], tab_recv.at[s], mate) for s in range(2)]

    for k in range(K_CHUNKS):
        x_copy[k].start()
        dkv_copy[k].start()
        kr_copy[k].start()
    for k in range(K_CHUNKS):
        dq_copy[k].start()
    barrier = pltpu.get_barrier_semaphore()
    for dev in (mate, right, left):
        pl.semaphore_signal(barrier, inc=1, device_id={'ctx': dev}, device_id_type=MESH)
    for s in range(2):
        tab_all[:, lanes(s)] = tab_ref[s * half:(s + 1) * half].T[0:rope]

    for k in range(K_CHUNKS):
        cols = slice(k * kc, (k + 1) * kc)
        x_copy[k].wait()
        dkv_copy[k].wait()
        kr_copy[k].wait()
        kv_new = jnp.dot(x_v[:, cols], wdkv[cols], preferred_element_type=f32)
        kr_new = lax.dot_general(x_v[:, cols], wkr[:, cols], (((1,), (1,)), ((), ())), preferred_element_type=f32)
        if k == 0:
            kv_acc[...] = kv_new
            kr_acc[...] = kr_new
        else:
            kv_acc[...] += kv_new
            kr_acc[...] += kr_new
    kv = kv_acc[...]
    c_kv = (kv * lax.rsqrt(jnp.mean(kv * kv, axis=-1, keepdims=True) + NORM_EPS) * gain_ref[0:1, 0:rank]).astype(jnp.bfloat16)
    kr = kr_acc[...]
    cos_k, sin_k = tab_ref[:, :rot], tab_ref[:, rot:rope]
    k_lo = (kr[:, :rot] * cos_k - kr[:, rot:] * sin_k).astype(jnp.bfloat16)
    k_hi = (kr[:, rot:] * cos_k + kr[:, :rot] * sin_k).astype(jnp.bfloat16)
    pad = jnp.zeros((half, lat.shape[2] - rank - rope), jnp.bfloat16)
    for s in range(2):
        own = slice(s * half, (s + 1) * half)
        lat[piece(me, s), :, 0:rank] = c_kv[own]
        lat[piece(me, s), :, rank:] = jnp.concatenate([k_lo[own], k_hi[own], pad], axis=1)

    pl.semaphore_wait(barrier, 3)
    for s in range(2):
        to_right[s].start()
        to_left[1 - s].start()
    for s in range(2):
        tab_share[s].start()
        shares[s].start()

    for c in qr_copy + uq_copy:
        c.start()
    cq_acc[...] = jnp.zeros_like(cq_acc)

    def contract(k, _):
        cols = pl.ds(pl.multiple_of(k * kc, kc), kc)
        pltpu.make_async_copy(wdq_hbm.at[cols], wdq.at[cols], dq_sem.at[k]).wait()
        cq_acc[...] += jnp.dot(x_v[:, cols], wdq[cols], preferred_element_type=f32)
        return 0

    lax.fori_loop(0, K_CHUNKS, contract, 0)
    for s in range(2):
        own = slice(s * half, (s + 1) * half)
        cq = cq_acc[own]
        cq_all[slot_of[s]] = (cq * lax.rsqrt(jnp.mean(cq * cq, axis=-1, keepdims=True) + NORM_EPS) * gain_ref[0:1, rank:]).astype(jnp.bfloat16)
        cq_share[s].start()

    to_right[0].wait_recv()
    on_right.start()
    to_left[1].wait_recv()
    on_left.start()
    shares[2].start()
    shares[3].start()
    for s in range(2):
        cq_share[s].wait_recv()
        tab_share[s].wait_recv()

    def rotary(b, _):
        pltpu.make_async_copy(wqr_hbm.at[:, pl.ds(0, Q_BLOCK)], wqr.at[b], qr_sem.at[b]).wait()
        res = jnp.dot(cq_all[...].reshape(2 * rows, cq_all.shape[2]), wqr[b], preferred_element_type=f32).T
        cos_q, sin_q = tab_all[0:rot], tab_all[rot:rope]
        for i in range(Q_BLOCK // rope):
            lo = res[i * rope:i * rope + rot]
            hi = res[i * rope + rot:(i + 1) * rope]
            h = b * (Q_BLOCK // rope) + i
            q_ref[h, nope:nope + rot, :] = (lo * cos_q - hi * sin_q).astype(jnp.bfloat16)
            q_ref[h, nope + rot:nope + rope, :] = (hi * cos_q + lo * sin_q).astype(jnp.bfloat16)
        return 0

    lax.fori_loop(0, n_qr, rotary, 0)
    to_right[1].wait_recv()
    to_left[0].wait_recv()
    shares[4].start()
    shares[5].start()

    def plain(b, _):
        pltpu.make_async_copy(wuq_hbm.at[:, pl.ds(0, Q_BLOCK)], wuq.at[b], uq_sem.at[b]).wait()
        res = jnp.dot(cq_all[...].reshape(2 * rows, cq_all.shape[2]), wuq[b], preferred_element_type=f32).astype(jnp.bfloat16).T
        for i in range(Q_BLOCK // nope):
            q_ref[b * (Q_BLOCK // nope) + i, 0:nope, :] = res[i * nope:(i + 1) * nope]
        return 0

    lax.fori_loop(0, n_uq // 2, plain, 0)
    on_right.wait_recv()
    on_left.wait_recv()
    shares[6].start()
    shares[7].start()
    lax.fori_loop(n_uq // 2, n_uq, plain, 0)
    for i in range(8):
        shares[i].wait_recv()
    out = pltpu.make_async_copy(lat, lat_hbm, lat_sem)
    out.start()
    for c in to_right + to_left + [on_right, on_left] + shares + cq_share + tab_share:
        c.wait_send()
    out.wait()


def latents(tok_x, w_dkv, w_kr, w_dq, w_uq, w_qr, g_q, g_kv, tab, n_ctx):
    rows, width = tok_x.shape
    rank, rope, q_rank = w_dkv.shape[1], w_kr.shape[1], w_dq.shape[1]
    heads = w_qr.shape[1] // rope // 2
    nope = w_uq.shape[1] // heads // 2
    bf16, f32 = jnp.bfloat16, jnp.float32
    vmem = pl.BlockSpec(memory_space=pltpu.VMEM)
    hbm = pl.BlockSpec(memory_space=pl.ANY)
    dma = pltpu.SemaphoreType.DMA
    n_uq, n_qr = heads * nope // Q_BLOCK, heads * rope // Q_BLOCK
    lat_width = rank + 128
    assert n_ctx == 8 and rope <= 128
    gain = jnp.broadcast_to(jnp.concatenate([g_kv, g_q]).astype(f32)[None], (8, rank + q_rank))
    lat, q_t = pl.pallas_call(
        functools.partial(latent_kernel, n_ctx),
        out_shape=[jax.ShapeDtypeStruct((2 * n_ctx, rows // 2, lat_width), bf16), jax.ShapeDtypeStruct((heads, nope + rope, 2 * rows), bf16)],
        in_specs=[hbm] * 6 + [vmem] * 2,
        out_specs=[hbm, vmem],
        scratch_shapes=[
            pltpu.VMEM((rows, width), bf16), pltpu.VMEM((width, rank), bf16), pltpu.VMEM((rope, width), bf16), pltpu.VMEM((width, q_rank), bf16),
            pltpu.VMEM((n_uq, q_rank, Q_BLOCK), bf16), pltpu.VMEM((n_qr, q_rank, Q_BLOCK), bf16),
            pltpu.VMEM((rows, rank), f32), pltpu.VMEM((rows, rope), f32), pltpu.VMEM((rows, q_rank), f32),
            pltpu.VMEM((4, rows // 2, q_rank), bf16), pltpu.VMEM((rope, 2 * rows), f32), pltpu.VMEM((2 * n_ctx, rows // 2, lat_width), bf16),
            dma((K_CHUNKS,)), dma((K_CHUNKS,)), dma((K_CHUNKS,)), dma((K_CHUNKS,)), dma((n_uq,)), dma((n_qr,)),
            dma((6,)), dma((6,)), dma((8,)), dma((8,)), dma((2,)), dma((2,)), dma((2,)), dma((2,)), dma,
        ],
        compiler_params=pltpu.CompilerParams(collective_id=2, has_side_effects=True, vmem_limit_bytes=62 * 1024 * 1024),
        name='latents',
    )(tok_x, w_dkv, w_kr.T, w_dq, w_uq, w_qr, gain, tab)
    return lat.reshape(n_ctx * rows, lat_width), q_t


def solution(mesh):
    tok_spec = P(('dp', 'ctx'), None)
    pos_spec = P(('dp', 'ctx'))
    full_mat = P(None, None)
    full_vec = P(None)
    col_spec = P(None, 'tp')
    row_spec = P('tp', None)

    def local_step(tok_x, tok_pos, w_dq, g_q, w_uq, w_qr, w_dkv, g_kv, w_kr, w_uk, w_uv, w_o):
        rope_dim = w_kr.shape[1]
        heads_loc = w_qr.shape[1] // rope_dim
        nope_dim = w_uq.shape[1] // heads_loc
        score_scale = (nope_dim + rope_dim) ** -0.5
        n_ctx = mesh.shape['ctx']
        tab = rope_table(tok_pos, rope_dim)
        lat, q_t = latents(tok_x, w_dkv, w_kr, w_dq, w_uq, w_qr, g_q, g_kv, tab, n_ctx)
        return mix(q_t, lat, w_uk, w_uv, w_o, mesh.shape['tp'], n_ctx, score_scale)

    return jax.shard_map(local_step, mesh=mesh,
                         in_specs=(tok_spec, pos_spec, full_mat, full_vec, col_spec, col_spec, full_mat, full_vec, full_mat, col_spec, col_spec, row_spec),
                         out_specs=tok_spec, check_vma=False)
```

```python
import functools

import jax
import jax.numpy as jnp
from jax import lax
from jax.experimental import pallas as pl
from jax.experimental.pallas import tpu as pltpu
from jax.sharding import PartitionSpec as P

ROPE_BASE = 10000.0
NORM_EPS = 1e-6


def rope_table(pos_vals, rope_dim):
    half_dim = rope_dim // 2
    lane = lax.broadcasted_iota(jnp.int32, (1, 128), 1)
    inv_freq = ROPE_BASE ** (-(lane % half_dim).astype(jnp.float32) * 2.0 / rope_dim)
    angles = pos_vals.astype(jnp.float32)[:, None] * inv_freq
    return jnp.where(lane % rope_dim < half_dim, jnp.cos(angles), jnp.sin(angles))


MESH = pl.DeviceIdType.MESH
KEY_BLOCK = 256
OUT_BLOCK = 512
W_SLOTS = 3
LAG = 3


def mix_kernel(n_tp, n_ctx, n_blk, scale, q_ref, lat_ref, wuk_hbm, wuv_hbm, w_hbm, out_hbm,
               wuk, wuv, wuv_t, lat_t, kcat, v_t, s_buf, p_buf, o_buf, o_all, wbuf, part, recv, ybuf,
               up_sem, w_sem, o_send, o_recv, rs_send, rs_recv, ag_send, ag_recv, out_sem):
    f32, bf16 = jnp.float32, jnp.bfloat16
    ctx = lax.axis_index('ctx')
    col = ctx // 2
    core = lax.rem(ctx, 2)
    mate = ctx + 1 - 2 * core
    n_col = n_ctx // 2
    me = lax.axis_index('tp')
    right = lax.rem(me + 1, n_tp)
    left = lax.rem(me + n_tp - 1, n_tp)
    across = lax.rem(me + 2, n_tp)
    peer = (right, left)
    step_of = (n_tp - 1, 1)
    heads = q_ref.shape[0]
    n_hp = heads // 2
    rank = wuk.shape[1]
    v_dim = v_t.shape[0] // 2
    nope = wuk.shape[2] // 2
    rope = q_ref.shape[1] - nope
    exp_scale = scale * 1.4426950408889634
    blk = wbuf.shape[2]
    rows = part.shape[3]
    n_pair = n_blk // 2
    half = o_all.shape[2]

    def up_copy(src, dst, which, hp):
        cols = dst.shape[2]
        return pltpu.make_async_copy(src.at[:, pl.ds(pl.multiple_of((core * n_hp + hp) * cols, cols), cols)], dst.at[hp], up_sem.at[which, hp])

    def w_copy(i):
        b = lax.rem(i, n_blk)
        slot = lax.rem(i, W_SLOTS)
        return pltpu.make_async_copy(w_hbm.at[:, pl.ds(pl.multiple_of(b * blk, blk), blk)], wbuf.at[slot], w_sem.at[slot])

    def chunk_at(way, hop):
        return lax.rem(me + (hop + 1) * step_of[way], n_tp)

    def rs_first(sel, b, way):
        return pltpu.make_async_remote_copy(src_ref=part.at[sel, b, chunk_at(way, 0)], dst_ref=recv.at[sel, b, 0], send_sem=rs_send.at[sel, b, 0],
                                            recv_sem=rs_recv.at[sel, b, 0], device_id={'tp': peer[way]}, device_id_type=MESH)

    def rs_next(sel, b, way, hop):
        return pltpu.make_async_remote_copy(src_ref=recv.at[sel, b, hop - 1], dst_ref=recv.at[sel, b, hop], send_sem=rs_send.at[sel, b, hop],
                                            recv_sem=rs_recv.at[sel, b, hop], device_id={'tp': peer[way]}, device_id_type=MESH)

    def rs_arrived(sel, b, way, hop):
        pltpu.make_async_remote_copy(src_ref=recv.at[sel, b, hop], dst_ref=recv.at[sel, b, hop], send_sem=rs_send.at[sel, b, hop],
                                     recv_sem=rs_recv.at[sel, b, hop], device_id={'tp': peer[way]}, device_id_type=MESH).wait_recv()

    def ag_copy(sel, b, slot, way, chunk):
        return pltpu.make_async_remote_copy(src_ref=ybuf.at[sel, chunk, b], dst_ref=ybuf.at[sel, chunk, b], send_sem=ag_send.at[sel, b, slot],
                                            recv_sem=ag_recv.at[sel, b, slot], device_id={'tp': peer[way]}, device_id_type=MESH)

    def out_copy(sel, b, chunk):
        return pltpu.make_async_copy(ybuf.at[sel, chunk, b],
                                     out_hbm.at[pl.ds(pl.multiple_of(sel * half + chunk * rows, rows), rows), pl.ds(pl.multiple_of(b * blk, blk), blk)],
                                     out_sem.at[sel, chunk, b])

    own_at = (core, 3 - core)
    mate_at = (1 - core, 2 + core)

    def o_share(sel):
        return pltpu.make_async_remote_copy(src_ref=o_buf.at[pl.ds(pl.multiple_of(mate_at[sel] * half, half), half)], dst_ref=o_all.at[sel, core],
                                            send_sem=o_send.at[sel], recv_sem=o_recv.at[sel], device_id={'ctx': mate}, device_id_type=MESH)

    for hp in range(n_hp):
        up_copy(wuk_hbm, wuk, 0, hp).start()
        up_copy(wuv_hbm, wuv, 1, hp).start()
    barrier = pltpu.get_barrier_semaphore()
    for neighbour in peer:
        pl.semaphore_signal(barrier, inc=1, device_id={'tp': neighbour}, device_id_type=MESH)
    pl.semaphore_signal(barrier, inc=1, device_id={'ctx': mate}, device_id_type=MESH)
    for i in range(lat_ref.shape[0] // KEY_BLOCK):
        lat_t[:, i * KEY_BLOCK:(i + 1) * KEY_BLOCK] = lat_ref[i * KEY_BLOCK:(i + 1) * KEY_BLOCK, 0:rank].T
        for g in range(2):
            kcat[g, i * KEY_BLOCK:(i + 1) * KEY_BLOCK, nope:nope + rope] = lat_ref[i * KEY_BLOCK:(i + 1) * KEY_BLOCK, rank:rank + rope]
    for hp in range(n_hp):
        up_copy(wuk_hbm, wuk, 0, hp).wait()
        up_copy(wuv_hbm, wuv, 1, hp).wait()
        wuv_t[hp] = wuv[hp].T
    for i in range(W_SLOTS):
        w_copy(i).start()
    pl.semaphore_wait(barrier, 3)

    def attend(sel, n_key, serve):
        q_cols = slice(sel * KEY_BLOCK, (sel + 1) * KEY_BLOCK)
        key_i = lax.broadcasted_iota(jnp.int32, (KEY_BLOCK, KEY_BLOCK), 0)
        q_i = lax.broadcasted_iota(jnp.int32, (KEY_BLOCK, KEY_BLOCK), 1)
        visible = key_i <= q_i

        def pair_step(hp, _):
            span = n_key * KEY_BLOCK
            k2 = jnp.dot(lat_ref[0:span, 0:rank], wuk[hp], preferred_element_type=f32).astype(bf16)
            kcat[0, 0:span, 0:nope] = k2[:, :nope]
            kcat[1, 0:span, 0:nope] = k2[:, nope:]
            v_t[:, 0:span] = jnp.dot(wuv_t[hp], lat_t[:, 0:span], preferred_element_type=f32).astype(bf16)
            for g in range(2):
                s_buf[g, 0:span] = jnp.dot(kcat[g, 0:span, 0:nope + rope], q_ref[2 * hp + g, :, q_cols], preferred_element_type=f32)
            total = []
            for g in range(2):
                top8 = None
                for i in range(n_key):
                    s = s_buf[g, i * KEY_BLOCK:(i + 1) * KEY_BLOCK]
                    if i == n_key - 1:
                        s = jnp.where(visible, s, -1e30)
                    blk8 = jnp.max(s.reshape(KEY_BLOCK // 8, 8, KEY_BLOCK), axis=0)
                    top8 = blk8 if top8 is None else jnp.maximum(top8, blk8)
                top = jnp.max(top8, axis=0, keepdims=True) * exp_scale
                sum8 = None
                for i in range(n_key):
                    keys = slice(i * KEY_BLOCK, (i + 1) * KEY_BLOCK)
                    s = s_buf[g, keys]
                    if i == n_key - 1:
                        s = jnp.where(visible, s, -1e30)
                    p = jnp.exp2(s * exp_scale - top)
                    blk8 = jnp.sum(p.reshape(KEY_BLOCK // 8, 8, KEY_BLOCK), axis=0)
                    sum8 = blk8 if sum8 is None else sum8 + blk8
                    p_buf[keys, g * KEY_BLOCK:(g + 1) * KEY_BLOCK] = p.astype(bf16)
                total.append(jnp.sum(sum8, axis=0, keepdims=True))
            o_t = jnp.dot(v_t[:, 0:span], p_buf[0:span], preferred_element_type=f32)
            for g in range(2):
                o_g = o_t[g * v_dim:(g + 1) * v_dim, g * KEY_BLOCK:(g + 1) * KEY_BLOCK] / total[g]
                o_buf[q_cols, pl.ds(pl.multiple_of((2 * hp + g) * v_dim, v_dim), v_dim)] = o_g.T.astype(bf16)
            if serve is not None:
                serve(hp)
            return 0

        lax.fori_loop(0, n_hp, pair_step, 0)

    def exchange(sel):
        o_share(sel).start()
        o_all[sel, core] = o_buf[pl.ds(pl.multiple_of(own_at[sel] * half, half), half), :]
        o_share(sel).wait()

    def product(sel, p):
        for way in range(2):
            b = 2 * p + way
            i = sel * n_blk + b
            slot = lax.rem(i, W_SLOTS)
            w_copy(i).wait()
            depth = o_all.shape[3]
            res = jnp.dot(o_all[sel, 0], wbuf[slot, 0:depth], preferred_element_type=f32) + jnp.dot(o_all[sel, 1], wbuf[slot, depth:], preferred_element_type=f32)
            part[sel, b] = res.reshape(n_tp, rows, blk)

            @pl.when(i + W_SLOTS < 2 * n_blk)
            def _():
                w_copy(i + W_SLOTS).start()

            rs_first(sel, b, way).start()

    def forward(sel, p, hop):
        for way in range(2):
            b = 2 * p + way
            rs_arrived(sel, b, way, hop - 1)
            recv[sel, b, hop - 1] = recv[sel, b, hop - 1] + part[sel, b, chunk_at(way, hop)]
        for way in range(2):
            rs_next(sel, 2 * p + way, way, hop).start()

    def finish(sel, p):
        for way in range(2):
            b = 2 * p + way
            rs_arrived(sel, b, way, n_tp - 2)
            ybuf[sel, me, b] = (recv[sel, b, n_tp - 2] + part[sel, b, me]).astype(ybuf.dtype)
        for way in range(2):
            b = 2 * p + way
            ag_copy(sel, b, 0, 0, me).start()
            ag_copy(sel, b, 1, 1, me).start()
            out_copy(sel, b, me).start()

    def relay(sel, p):
        ag_copy(sel, 2 * p, 0, 0, left).wait_recv()
        ag_copy(sel, 2 * p, 2, 0, left).start()
        ag_copy(sel, 2 * p + 1, 1, 1, right).wait_recv()
        ag_copy(sel, 2 * p + 1, 2, 1, right).start()
        out_copy(sel, 2 * p, left).start()
        out_copy(sel, 2 * p + 1, right).start()

    def drain(sel, p):
        ag_copy(sel, 2 * p, 1, 1, right).wait_recv()
        out_copy(sel, 2 * p, right).start()
        ag_copy(sel, 2 * p + 1, 0, 0, left).wait_recv()
        out_copy(sel, 2 * p + 1, left).start()
        for way in range(2):
            b = 2 * p + way
            ag_copy(sel, b, 2, way, across).wait_recv()
            out_copy(sel, b, across).start()

    def settle(sel, p):
        for way in range(2):
            b = 2 * p + way
            rs_first(sel, b, way).wait_send()
            for hop in range(1, n_tp - 1):
                rs_next(sel, b, way, hop).wait_send()
            ag_copy(sel, b, 0, 0, me).wait_send()
            ag_copy(sel, b, 1, 1, me).wait_send()
            ag_copy(sel, b, 2, way, left if way == 0 else right).wait_send()
            for chunk in range(n_tp):
                out_copy(sel, b, chunk).wait()

    def loop(start, stop, body):
        def step(p, _):
            body(p)
            return 0
        lax.fori_loop(start, stop, step, 0)

    for v in range(n_col):
        pl.when(col == v)(functools.partial(attend, 0, v + 1, None))
    exchange(0)

    def early(p):
        product(0, p)

        @pl.when(p >= LAG)
        def _():
            forward(0, p - LAG, 1)

    loop(0, n_pair, early)
    hop1_left = n_pair - LAG

    def serve(hp):
        for j in range(2):
            n = hop1_left + 2 * hp + j
            pl.when(n < n_pair)(lambda: forward(0, n, 1))
            pl.when((n >= n_pair) & (n < 2 * n_pair))(lambda: forward(0, n - n_pair, 2))
            pl.when((n >= 2 * n_pair) & (n < 3 * n_pair))(lambda: finish(0, n - 2 * n_pair))

    for v in range(n_col):
        pl.when(col == v)(functools.partial(attend, 1, 2 * n_col - v, serve))
    served = min(hop1_left + 2 * n_hp, 3 * n_pair) - 2 * n_pair
    exchange(1)

    def late(p):
        product(1, p)
        pl.when(p + served < n_pair)(lambda: finish(0, p + served))

        @pl.when(p >= LAG)
        def _():
            forward(1, p - LAG, 1)

        relay(0, p)

    loop(0, n_pair, late)
    loop(hop1_left, n_pair, lambda p: forward(1, p, 1))
    loop(0, n_pair, lambda p: forward(1, p, 2))

    def close(p):
        finish(1, p)
        pl.when(p > 0)(lambda: relay(1, p - 1))
        drain(0, p)

    loop(0, n_pair, close)
    relay(1, n_pair - 1)
    loop(0, n_pair, lambda p: drain(1, p))
    o_wait = n_pair
    loop(0, o_wait, lambda p: settle(0, p))
    loop(0, o_wait, lambda p: settle(1, p))


def mix(q_t, lat, w_uk, w_uv, w_o, n_tp, n_ctx, scale):
    heads, q_dim, q_count = q_t.shape
    keys, rank = lat.shape[0], w_uk.shape[0]
    nope = w_uk.shape[1] // (2 * heads)
    rope = q_dim - nope
    v_dim = w_uv.shape[1] // (2 * heads)
    n_hp = heads // 2
    depth, width = w_o.shape
    n_blk = width // OUT_BLOCK
    half = q_count // 4
    rows = half // n_tp
    assert n_tp == 4 and n_blk % 2 == 0 and width % OUT_BLOCK == 0
    assert q_count == 2 * KEY_BLOCK and keys == n_ctx * KEY_BLOCK
    bf16, f32 = jnp.bfloat16, jnp.float32
    vmem = pl.BlockSpec(memory_space=pltpu.VMEM)
    hbm = pl.BlockSpec(memory_space=pl.ANY)
    dma = pltpu.SemaphoreType.DMA
    return pl.pallas_call(
        functools.partial(mix_kernel, n_tp, n_ctx, n_blk, scale),
        out_shape=jax.ShapeDtypeStruct((2 * half, width), bf16),
        in_specs=[vmem, vmem, hbm, hbm, hbm],
        out_specs=hbm,
        scratch_shapes=[
            pltpu.VMEM((n_hp, rank, 2 * nope), bf16), pltpu.VMEM((n_hp, rank, 2 * v_dim), bf16), pltpu.VMEM((n_hp, 2 * v_dim, rank), bf16),
            pltpu.VMEM((rank, keys), bf16), pltpu.VMEM((2, keys, nope + rope), bf16), pltpu.VMEM((2 * v_dim, keys), bf16),
            pltpu.VMEM((2, keys, KEY_BLOCK), f32), pltpu.VMEM((keys, 2 * KEY_BLOCK), bf16),
            pltpu.VMEM((q_count, heads * v_dim), bf16), pltpu.VMEM((2, 2, half, depth // 2), bf16),
            pltpu.VMEM((W_SLOTS, depth, OUT_BLOCK), bf16),
            pltpu.VMEM((2, n_blk, n_tp, rows, OUT_BLOCK), f32),
            pltpu.VMEM((2, n_blk, n_tp - 1, rows, OUT_BLOCK), f32),
            pltpu.VMEM((2, n_tp, n_blk, rows, OUT_BLOCK), bf16),
            dma((2, n_hp)), dma((W_SLOTS,)), dma((2,)), dma((2,)), dma((2, n_blk, n_tp - 1)), dma((2, n_blk, n_tp - 1)),
            dma((2, n_blk, 3)), dma((2, n_blk, 3)), dma((2, n_tp, n_blk)),
        ],
        compiler_params=pltpu.CompilerParams(collective_id=1, has_side_effects=True, vmem_limit_bytes=63 * 1024 * 1024),
        name='mix',
    )(q_t, lat, w_uk, w_uv, w_o)


K_CHUNKS = 4
Q_BLOCK = 256


def latent_kernel(n_ctx, x_hbm, wdkv_hbm, wkr_hbm, wdq_hbm, wuq_hbm, wqr_hbm, gain_ref, tab_ref, lat_hbm, q_ref,
                  x_v, wdkv, wkr, wdq, wuq, wqr, kv_acc, kr_acc, cq_acc, cq_all, tab_all, lat,
                  x_sem, dkv_sem, kr_sem, dq_sem, uq_sem, qr_sem, ring_send, ring_recv, mate_send, mate_recv, cq_send, cq_recv, tab_send, tab_recv, lat_sem):
    me = lax.axis_index('ctx')
    part = lax.rem(me, 2)
    mate = me + 1 - 2 * part
    right = lax.rem(me + 2, n_ctx)
    left = lax.rem(me + n_ctx - 2, n_ctx)
    far = lax.rem(me + 4, n_ctx)
    f32 = jnp.float32
    rows, width = x_v.shape
    half = rows // 2
    rank = kv_acc.shape[1]
    rope = kr_acc.shape[1]
    rot = rope // 2
    kc = width // K_CHUNKS
    n_uq, n_qr = wuq.shape[0], wqr.shape[0]
    nope = q_ref.shape[1] - rope

    def kcols(k):
        return pl.ds(k * kc, kc)

    x_copy = [pltpu.make_async_copy(x_hbm.at[:, kcols(k)], x_v.at[:, kcols(k)], x_sem.at[k]) for k in range(K_CHUNKS)]
    dkv_copy = [pltpu.make_async_copy(wdkv_hbm.at[kcols(k)], wdkv.at[kcols(k)], dkv_sem.at[k]) for k in range(K_CHUNKS)]
    kr_copy = [pltpu.make_async_copy(wkr_hbm.at[:, kcols(k)], wkr.at[:, kcols(k)], kr_sem.at[k]) for k in range(K_CHUNKS)]
    dq_copy = [pltpu.make_async_copy(wdq_hbm.at[kcols(k)], wdq.at[kcols(k)], dq_sem.at[k]) for k in range(K_CHUNKS)]
    uq_copy = [pltpu.make_async_copy(wuq_hbm.at[:, pl.ds(pl.multiple_of((part * n_uq + b) * Q_BLOCK, Q_BLOCK), Q_BLOCK)], wuq.at[b], uq_sem.at[b]) for b in range(n_uq)]
    qr_copy = [pltpu.make_async_copy(wqr_hbm.at[:, pl.ds(pl.multiple_of((part * n_qr + b) * Q_BLOCK, Q_BLOCK), Q_BLOCK)], wqr.at[b], qr_sem.at[b]) for b in range(n_qr)]

    def piece(dev, sub):
        return dev if sub == 0 else 2 * n_ctx - 1 - dev

    def send(src, dst, send_sem, recv_sem, dev):
        return pltpu.make_async_remote_copy(src_ref=src, dst_ref=dst, send_sem=send_sem, recv_sem=recv_sem, device_id={'ctx': dev}, device_id_type=MESH)

    def ring(slot, src_dev, sub, dev):
        return send(lat.at[piece(src_dev, sub)], lat.at[piece(src_dev, sub)], ring_send.at[slot], ring_recv.at[slot], dev)

    def share(slot, src_dev, sub):
        return send(lat.at[piece(src_dev, sub)], lat.at[piece(src_dev, sub)], mate_send.at[slot], mate_recv.at[slot], mate)

    to_right = [ring(0, me, 0, right), ring(1, me, 1, right)]
    to_left = [ring(2, me, 0, left), ring(3, me, 1, left)]
    on_right = ring(4, left, 0, right)
    on_left = ring(5, right, 1, left)
    order = [(me, 0), (me, 1), (left, 0), (right, 1), (left, 1), (right, 0), (far, 0), (far, 1)]
    shares = [share(i, d, s) for i, (d, s) in enumerate(order)]
    slot_of = (part, 3 - part)
    cq_share = [send(cq_all.at[slot_of[s]], cq_all.at[slot_of[s]], cq_send.at[s], cq_recv.at[s], mate) for s in range(2)]

    def lanes(s):
        return pl.ds(pl.multiple_of(slot_of[s] * half, half), half)

    tab_share = [send(tab_all.at[:, lanes(s)], tab_all.at[:, lanes(s)], tab_send.at[s], tab_recv.at[s], mate) for s in range(2)]

    def fetch(k):
        if k < K_CHUNKS:
            group = [x_copy[k], dkv_copy[k], kr_copy[k]]
        elif k < 2 * K_CHUNKS:
            group = [dq_copy[k - K_CHUNKS]]
        else:
            group = qr_copy if k == 2 * K_CHUNKS else uq_copy
        for c in group:
            c.start()

    fetch(0)
    fetch(1)
    barrier = pltpu.get_barrier_semaphore()
    for dev in (mate, right, left):
        pl.semaphore_signal(barrier, inc=1, device_id={'ctx': dev}, device_id_type=MESH)
    for s in range(2):
        tab_all[:, lanes(s)] = tab_ref[s * half:(s + 1) * half].T[0:rope]

    for k in range(K_CHUNKS):
        cols = slice(k * kc, (k + 1) * kc)
        x_copy[k].wait()
        dkv_copy[k].wait()
        kr_copy[k].wait()
        fetch(k + 2)
        kv_new = jnp.dot(x_v[:, cols], wdkv[cols], preferred_element_type=f32)
        kr_new = lax.dot_general(x_v[:, cols], wkr[:, cols], (((1,), (1,)), ((), ())), preferred_element_type=f32)
        if k == 0:
            kv_acc[...] = kv_new
            kr_acc[...] = kr_new
        else:
            kv_acc[...] += kv_new
            kr_acc[...] += kr_new
    kv = kv_acc[...]
    c_kv = (kv * lax.rsqrt(jnp.mean(kv * kv, axis=-1, keepdims=True) + NORM_EPS) * gain_ref[0:1, 0:rank]).astype(jnp.bfloat16)
    kr = kr_acc[...]
    cos_k, sin_k = tab_ref[:, :rot], tab_ref[:, rot:rope]
    k_lo = (kr[:, :rot] * cos_k - kr[:, rot:] * sin_k).astype(jnp.bfloat16)
    k_hi = (kr[:, rot:] * cos_k + kr[:, :rot] * sin_k).astype(jnp.bfloat16)
    pad = jnp.zeros((half, lat.shape[2] - rank - rope), jnp.bfloat16)
    for s in range(2):
        own = slice(s * half, (s + 1) * half)
        lat[piece(me, s), :, 0:rank] = c_kv[own]
        lat[piece(me, s), :, rank:] = jnp.concatenate([k_lo[own], k_hi[own], pad], axis=1)

    pl.semaphore_wait(barrier, 3)
    for s in range(2):
        to_right[s].start()
        to_left[1 - s].start()
    for s in range(2):
        tab_share[s].start()
        shares[s].start()

    for k in range(K_CHUNKS):
        cols = slice(k * kc, (k + 1) * kc)
        dq_copy[k].wait()
        fetch(K_CHUNKS + k + 2)
        cq_new = jnp.dot(x_v[:, cols], wdq[cols], preferred_element_type=f32)
        if k == 0:
            cq_acc[...] = cq_new
        else:
            cq_acc[...] += cq_new
    for s in range(2):
        own = slice(s * half, (s + 1) * half)
        cq = cq_acc[own]
        cq_all[slot_of[s]] = (cq * lax.rsqrt(jnp.mean(cq * cq, axis=-1, keepdims=True) + NORM_EPS) * gain_ref[0:1, rank:]).astype(jnp.bfloat16)
        cq_share[s].start()

    to_right[0].wait_recv()
    on_right.start()
    to_left[1].wait_recv()
    on_left.start()
    shares[2].start()
    shares[3].start()
    for s in range(2):
        cq_share[s].wait_recv()
        tab_share[s].wait_recv()

    def rotary(b, _):
        pltpu.make_async_copy(wqr_hbm.at[:, pl.ds(0, Q_BLOCK)], wqr.at[b], qr_sem.at[b]).wait()
        res = jnp.dot(cq_all[...].reshape(2 * rows, cq_all.shape[2]), wqr[b], preferred_element_type=f32).T
        cos_q, sin_q = tab_all[0:rot], tab_all[rot:rope]
        for i in range(Q_BLOCK // rope):
            lo = res[i * rope:i * rope + rot]
            hi = res[i * rope + rot:(i + 1) * rope]
            h = b * (Q_BLOCK // rope) + i
            q_ref[h, nope:nope + rot, :] = (lo * cos_q - hi * sin_q).astype(jnp.bfloat16)
            q_ref[h, nope + rot:nope + rope, :] = (hi * cos_q + lo * sin_q).astype(jnp.bfloat16)
        return 0

    lax.fori_loop(0, n_qr, rotary, 0)
    to_right[1].wait_recv()
    to_left[0].wait_recv()
    shares[4].start()
    shares[5].start()

    def plain(b, _):
        pltpu.make_async_copy(wuq_hbm.at[:, pl.ds(0, Q_BLOCK)], wuq.at[b], uq_sem.at[b]).wait()
        res = jnp.dot(cq_all[...].reshape(2 * rows, cq_all.shape[2]), wuq[b], preferred_element_type=f32).astype(jnp.bfloat16).T
        for i in range(Q_BLOCK // nope):
            q_ref[b * (Q_BLOCK // nope) + i, 0:nope, :] = res[i * nope:(i + 1) * nope]
        return 0

    lax.fori_loop(0, n_uq // 2, plain, 0)
    on_right.wait_recv()
    on_left.wait_recv()
    shares[6].start()
    shares[7].start()
    lax.fori_loop(n_uq // 2, n_uq, plain, 0)
    for i in range(8):
        shares[i].wait_recv()
    out = pltpu.make_async_copy(lat, lat_hbm, lat_sem)
    out.start()
    for c in to_right + to_left + [on_right, on_left] + shares + cq_share + tab_share:
        c.wait_send()
    out.wait()


def latents(tok_x, w_dkv, w_kr, w_dq, w_uq, w_qr, g_q, g_kv, tab, n_ctx):
    rows, width = tok_x.shape
    rank, rope, q_rank = w_dkv.shape[1], w_kr.shape[1], w_dq.shape[1]
    heads = w_qr.shape[1] // rope // 2
    nope = w_uq.shape[1] // heads // 2
    bf16, f32 = jnp.bfloat16, jnp.float32
    vmem = pl.BlockSpec(memory_space=pltpu.VMEM)
    hbm = pl.BlockSpec(memory_space=pl.ANY)
    dma = pltpu.SemaphoreType.DMA
    n_uq, n_qr = heads * nope // Q_BLOCK, heads * rope // Q_BLOCK
    lat_width = rank + 128
    assert n_ctx == 8 and rope <= 128
    gain = jnp.broadcast_to(jnp.concatenate([g_kv, g_q]).astype(f32)[None], (8, rank + q_rank))
    lat, q_t = pl.pallas_call(
        functools.partial(latent_kernel, n_ctx),
        out_shape=[jax.ShapeDtypeStruct((2 * n_ctx, rows // 2, lat_width), bf16), jax.ShapeDtypeStruct((heads, nope + rope, 2 * rows), bf16)],
        in_specs=[hbm] * 6 + [vmem] * 2,
        out_specs=[hbm, vmem],
        scratch_shapes=[
            pltpu.VMEM((rows, width), bf16), pltpu.VMEM((width, rank), bf16), pltpu.VMEM((rope, width), bf16), pltpu.VMEM((width, q_rank), bf16),
            pltpu.VMEM((n_uq, q_rank, Q_BLOCK), bf16), pltpu.VMEM((n_qr, q_rank, Q_BLOCK), bf16),
            pltpu.VMEM((rows, rank), f32), pltpu.VMEM((rows, rope), f32), pltpu.VMEM((rows, q_rank), f32),
            pltpu.VMEM((4, rows // 2, q_rank), bf16), pltpu.VMEM((rope, 2 * rows), f32), pltpu.VMEM((2 * n_ctx, rows // 2, lat_width), bf16),
            dma((K_CHUNKS,)), dma((K_CHUNKS,)), dma((K_CHUNKS,)), dma((K_CHUNKS,)), dma((n_uq,)), dma((n_qr,)),
            dma((6,)), dma((6,)), dma((8,)), dma((8,)), dma((2,)), dma((2,)), dma((2,)), dma((2,)), dma,
        ],
        compiler_params=pltpu.CompilerParams(collective_id=2, has_side_effects=True, vmem_limit_bytes=62 * 1024 * 1024),
        name='latents',
    )(tok_x, w_dkv, w_kr.T, w_dq, w_uq, w_qr, gain, tab)
    return lat.reshape(n_ctx * rows, lat_width), q_t


def solution(mesh):
    tok_spec = P(('dp', 'ctx'), None)
    pos_spec = P(('dp', 'ctx'))
    full_mat = P(None, None)
    full_vec = P(None)
    col_spec = P(None, 'tp')
    row_spec = P('tp', None)

    def local_step(tok_x, tok_pos, w_dq, g_q, w_uq, w_qr, w_dkv, g_kv, w_kr, w_uk, w_uv, w_o):
        rope_dim = w_kr.shape[1]
        heads_loc = w_qr.shape[1] // rope_dim
        nope_dim = w_uq.shape[1] // heads_loc
        score_scale = (nope_dim + rope_dim) ** -0.5
        n_ctx = mesh.shape['ctx']
        tab = rope_table(tok_pos, rope_dim)
        lat, q_t = latents(tok_x, w_dkv, w_kr, w_dq, w_uq, w_qr, g_q, g_kv, tab, n_ctx)
        return mix(q_t, lat, w_uk, w_uv, w_o, mesh.shape['tp'], n_ctx, score_scale)

    return jax.shard_map(local_step, mesh=mesh,
                         in_specs=(tok_spec, pos_spec, full_mat, full_vec, col_spec, col_spec, full_mat, full_vec, full_mat, col_spec, col_spec, row_spec),
                         out_specs=tok_spec, check_vma=False)
```

```python
import functools

import jax
import jax.numpy as jnp
from jax import lax
from jax.experimental import pallas as pl
from jax.experimental.pallas import tpu as pltpu
from jax.sharding import PartitionSpec as P

ROPE_BASE = 10000.0
NORM_EPS = 1e-6


def rope_table(pos_vals, rope_dim):
    half_dim = rope_dim // 2
    lane = lax.broadcasted_iota(jnp.int32, (1, 128), 1)
    inv_freq = ROPE_BASE ** (-(lane % half_dim).astype(jnp.float32) * 2.0 / rope_dim)
    angles = pos_vals.astype(jnp.float32)[:, None] * inv_freq
    return jnp.where(lane % rope_dim < half_dim, jnp.cos(angles), jnp.sin(angles))


MESH = pl.DeviceIdType.MESH
KEY_BLOCK = 256
OUT_BLOCK = 512
W_SLOTS = 3
LAG = 3


def mix_kernel(n_tp, n_ctx, n_blk, scale, q_hbm, lat_hbm, wuk_hbm, wuv_hbm, w_hbm, out_hbm,
               q_ref, lat_ref, in_sem, wuk, wuv, wuv_t, lat_t, kcat, v_t, s_buf, p_buf, o_buf, o_all, wbuf, part, recv, ybuf,
               up_sem, w_sem, o_send, o_recv, rs_send, rs_recv, ag_send, ag_recv, out_sem):
    f32, bf16 = jnp.float32, jnp.bfloat16
    ctx = lax.axis_index('ctx')
    col = ctx // 2
    core = lax.rem(ctx, 2)
    mate = ctx + 1 - 2 * core
    n_col = n_ctx // 2
    me = lax.axis_index('tp')
    right = lax.rem(me + 1, n_tp)
    left = lax.rem(me + n_tp - 1, n_tp)
    across = lax.rem(me + 2, n_tp)
    peer = (right, left)
    step_of = (n_tp - 1, 1)
    heads = q_ref.shape[0]
    n_hp = heads // 2
    rank = wuk.shape[1]
    v_dim = v_t.shape[0] // 2
    nope = wuk.shape[2] // 2
    rope = q_ref.shape[1] - nope
    exp_scale = scale * 1.4426950408889634
    blk = wbuf.shape[2]
    rows = part.shape[3]
    n_pair = n_blk // 2
    half = o_all.shape[2]

    def up_copy(src, dst, which, hp):
        cols = dst.shape[2]
        return pltpu.make_async_copy(src.at[:, pl.ds(pl.multiple_of((core * n_hp + hp) * cols, cols), cols)], dst.at[hp], up_sem.at[which, hp])

    def w_copy(i):
        b = lax.rem(i, n_blk)
        slot = lax.rem(i, W_SLOTS)
        return pltpu.make_async_copy(w_hbm.at[:, pl.ds(pl.multiple_of(b * blk, blk), blk)], wbuf.at[slot], w_sem.at[slot])

    def chunk_at(way, hop):
        return lax.rem(me + (hop + 1) * step_of[way], n_tp)

    def rs_first(sel, b, way):
        return pltpu.make_async_remote_copy(src_ref=part.at[sel, b, chunk_at(way, 0)], dst_ref=recv.at[sel, b, 0], send_sem=rs_send.at[sel, b, 0],
                                            recv_sem=rs_recv.at[sel, b, 0], device_id={'tp': peer[way]}, device_id_type=MESH)

    def rs_next(sel, b, way, hop):
        return pltpu.make_async_remote_copy(src_ref=recv.at[sel, b, hop - 1], dst_ref=recv.at[sel, b, hop], send_sem=rs_send.at[sel, b, hop],
                                            recv_sem=rs_recv.at[sel, b, hop], device_id={'tp': peer[way]}, device_id_type=MESH)

    def rs_arrived(sel, b, way, hop):
        pltpu.make_async_remote_copy(src_ref=recv.at[sel, b, hop], dst_ref=recv.at[sel, b, hop], send_sem=rs_send.at[sel, b, hop],
                                     recv_sem=rs_recv.at[sel, b, hop], device_id={'tp': peer[way]}, device_id_type=MESH).wait_recv()

    def ag_copy(sel, b, slot, way, chunk):
        return pltpu.make_async_remote_copy(src_ref=ybuf.at[sel, chunk, b], dst_ref=ybuf.at[sel, chunk, b], send_sem=ag_send.at[sel, b, slot],
                                            recv_sem=ag_recv.at[sel, b, slot], device_id={'tp': peer[way]}, device_id_type=MESH)

    def out_copy(sel, b, chunk):
        return pltpu.make_async_copy(ybuf.at[sel, chunk, b],
                                     out_hbm.at[pl.ds(pl.multiple_of(sel * half + chunk * rows, rows), rows), pl.ds(pl.multiple_of(b * blk, blk), blk)],
                                     out_sem.at[sel, chunk, b])

    own_at = (core, 3 - core)
    mate_at = (1 - core, 2 + core)

    def o_share(sel):
        return pltpu.make_async_remote_copy(src_ref=o_buf.at[pl.ds(pl.multiple_of(mate_at[sel] * half, half), half)], dst_ref=o_all.at[sel, core],
                                            send_sem=o_send.at[sel], recv_sem=o_recv.at[sel], device_id={'ctx': mate}, device_id_type=MESH)

    lat_in = pltpu.make_async_copy(lat_hbm, lat_ref, in_sem.at[0])
    q_in = pltpu.make_async_copy(q_hbm, q_ref, in_sem.at[1])
    lat_in.start()
    for hp in range(n_hp):
        up_copy(wuk_hbm, wuk, 0, hp).start()
        up_copy(wuv_hbm, wuv, 1, hp).start()
    q_in.start()
    barrier = pltpu.get_barrier_semaphore()
    for neighbour in peer:
        pl.semaphore_signal(barrier, inc=1, device_id={'tp': neighbour}, device_id_type=MESH)
    pl.semaphore_signal(barrier, inc=1, device_id={'ctx': mate}, device_id_type=MESH)
    lat_in.wait()
    for i in range(lat_ref.shape[0] // KEY_BLOCK):
        lat_t[:, i * KEY_BLOCK:(i + 1) * KEY_BLOCK] = lat_ref[i * KEY_BLOCK:(i + 1) * KEY_BLOCK, 0:rank].T
        for g in range(2):
            kcat[g, i * KEY_BLOCK:(i + 1) * KEY_BLOCK, nope:nope + rope] = lat_ref[i * KEY_BLOCK:(i + 1) * KEY_BLOCK, rank:rank + rope]
    for hp in range(n_hp):
        up_copy(wuk_hbm, wuk, 0, hp).wait()
        up_copy(wuv_hbm, wuv, 1, hp).wait()
        wuv_t[hp] = wuv[hp].T
    q_in.wait()
    for i in range(W_SLOTS):
        w_copy(i).start()
    pl.semaphore_wait(barrier, 3)

    def attend(sel, n_key, serve):
        q_cols = slice(sel * KEY_BLOCK, (sel + 1) * KEY_BLOCK)
        key_i = lax.broadcasted_iota(jnp.int32, (KEY_BLOCK, KEY_BLOCK), 0)
        q_i = lax.broadcasted_iota(jnp.int32, (KEY_BLOCK, KEY_BLOCK), 1)
        visible = key_i <= q_i

        def pair_step(hp, _):
            span = n_key * KEY_BLOCK
            k2 = jnp.dot(lat_ref[0:span, 0:rank], wuk[hp], preferred_element_type=f32).astype(bf16)
            kcat[0, 0:span, 0:nope] = k2[:, :nope]
            kcat[1, 0:span, 0:nope] = k2[:, nope:]
            v_t[:, 0:span] = jnp.dot(wuv_t[hp], lat_t[:, 0:span], preferred_element_type=f32).astype(bf16)
            for g in range(2):
                s_buf[g, 0:span] = jnp.dot(kcat[g, 0:span, 0:nope + rope], q_ref[2 * hp + g, :, q_cols], preferred_element_type=f32)
            total = []
            for g in range(2):
                top8 = None
                for i in range(n_key):
                    s = s_buf[g, i * KEY_BLOCK:(i + 1) * KEY_BLOCK]
                    if i == n_key - 1:
                        s = jnp.where(visible, s, -1e30)
                    blk8 = jnp.max(s.reshape(KEY_BLOCK // 8, 8, KEY_BLOCK), axis=0)
                    top8 = blk8 if top8 is None else jnp.maximum(top8, blk8)
                top = jnp.max(top8, axis=0, keepdims=True) * exp_scale
                sum8 = None
                for i in range(n_key):
                    keys = slice(i * KEY_BLOCK, (i + 1) * KEY_BLOCK)
                    s = s_buf[g, keys]
                    if i == n_key - 1:
                        s = jnp.where(visible, s, -1e30)
                    p = jnp.exp2(s * exp_scale - top)
                    blk8 = jnp.sum(p.reshape(KEY_BLOCK // 8, 8, KEY_BLOCK), axis=0)
                    sum8 = blk8 if sum8 is None else sum8 + blk8
                    p_buf[keys, g * KEY_BLOCK:(g + 1) * KEY_BLOCK] = p.astype(bf16)
                total.append(jnp.sum(sum8, axis=0, keepdims=True))
            o_t = jnp.dot(v_t[:, 0:span], p_buf[0:span], preferred_element_type=f32)
            for g in range(2):
                o_g = o_t[g * v_dim:(g + 1) * v_dim, g * KEY_BLOCK:(g + 1) * KEY_BLOCK] / total[g]
                o_buf[q_cols, pl.ds(pl.multiple_of((2 * hp + g) * v_dim, v_dim), v_dim)] = o_g.T.astype(bf16)
            if serve is not None:
                serve(hp)
            return 0

        lax.fori_loop(0, n_hp, pair_step, 0)

    def exchange(sel):
        o_share(sel).start()
        o_all[sel, core] = o_buf[pl.ds(pl.multiple_of(own_at[sel] * half, half), half), :]
        o_share(sel).wait()

    def product(sel, p):
        for way in range(2):
            b = 2 * p + way
            i = sel * n_blk + b
            slot = lax.rem(i, W_SLOTS)
            w_copy(i).wait()
            depth = o_all.shape[3]
            res = jnp.dot(o_all[sel, 0], wbuf[slot, 0:depth], preferred_element_type=f32) + jnp.dot(o_all[sel, 1], wbuf[slot, depth:], preferred_element_type=f32)
            part[sel, b] = res.reshape(n_tp, rows, blk)

            @pl.when(i + W_SLOTS < 2 * n_blk)
            def _():
                w_copy(i + W_SLOTS).start()

            rs_first(sel, b, way).start()

    def forward(sel, p, hop):
        for way in range(2):
            b = 2 * p + way
            rs_arrived(sel, b, way, hop - 1)
            recv[sel, b, hop - 1] = recv[sel, b, hop - 1] + part[sel, b, chunk_at(way, hop)]
        for way in range(2):
            rs_next(sel, 2 * p + way, way, hop).start()

    def finish(sel, p):
        for way in range(2):
            b = 2 * p + way
            rs_arrived(sel, b, way, n_tp - 2)
            ybuf[sel, me, b] = (recv[sel, b, n_tp - 2] + part[sel, b, me]).astype(ybuf.dtype)
        for way in range(2):
            b = 2 * p + way
            ag_copy(sel, b, 0, 0, me).start()
            ag_copy(sel, b, 1, 1, me).start()
            out_copy(sel, b, me).start()

    def relay(sel, p):
        ag_copy(sel, 2 * p, 0, 0, left).wait_recv()
        ag_copy(sel, 2 * p, 2, 0, left).start()
        ag_copy(sel, 2 * p + 1, 1, 1, right).wait_recv()
        ag_copy(sel, 2 * p + 1, 2, 1, right).start()
        out_copy(sel, 2 * p, left).start()
        out_copy(sel, 2 * p + 1, right).start()

    def drain(sel, p):
        ag_copy(sel, 2 * p, 1, 1, right).wait_recv()
        out_copy(sel, 2 * p, right).start()
        ag_copy(sel, 2 * p + 1, 0, 0, left).wait_recv()
        out_copy(sel, 2 * p + 1, left).start()
        for way in range(2):
            b = 2 * p + way
            ag_copy(sel, b, 2, way, across).wait_recv()
            out_copy(sel, b, across).start()

    def settle(sel, p):
        for way in range(2):
            b = 2 * p + way
            rs_first(sel, b, way).wait_send()
            for hop in range(1, n_tp - 1):
                rs_next(sel, b, way, hop).wait_send()
            ag_copy(sel, b, 0, 0, me).wait_send()
            ag_copy(sel, b, 1, 1, me).wait_send()
            ag_copy(sel, b, 2, way, left if way == 0 else right).wait_send()
            for chunk in range(n_tp):
                out_copy(sel, b, chunk).wait()

    def loop(start, stop, body):
        def step(p, _):
            body(p)
            return 0
        lax.fori_loop(start, stop, step, 0)

    for v in range(n_col):
        pl.when(col == v)(functools.partial(attend, 0, v + 1, None))
    exchange(0)

    def early(p):
        product(0, p)

        @pl.when(p >= LAG)
        def _():
            forward(0, p - LAG, 1)

    loop(0, n_pair, early)
    hop1_left = n_pair - LAG

    def serve(hp):
        for j in range(2):
            n = hop1_left + 2 * hp + j
            pl.when(n < n_pair)(lambda: forward(0, n, 1))
            pl.when((n >= n_pair) & (n < 2 * n_pair))(lambda: forward(0, n - n_pair, 2))
            pl.when((n >= 2 * n_pair) & (n < 3 * n_pair))(lambda: finish(0, n - 2 * n_pair))

    for v in range(n_col):
        pl.when(col == v)(functools.partial(attend, 1, 2 * n_col - v, serve))
    served = min(hop1_left + 2 * n_hp, 3 * n_pair) - 2 * n_pair
    exchange(1)

    def late(p):
        product(1, p)
        pl.when(p + served < n_pair)(lambda: finish(0, p + served))

        @pl.when(p >= LAG)
        def _():
            forward(1, p - LAG, 1)

        relay(0, p)

    loop(0, n_pair, late)
    loop(hop1_left, n_pair, lambda p: forward(1, p, 1))
    loop(0, n_pair, lambda p: forward(1, p, 2))

    def close(p):
        finish(1, p)
        pl.when(p > 0)(lambda: relay(1, p - 1))
        drain(0, p)

    loop(0, n_pair, close)
    relay(1, n_pair - 1)
    loop(0, n_pair, lambda p: drain(1, p))
    o_wait = n_pair
    loop(0, o_wait, lambda p: settle(0, p))
    loop(0, o_wait, lambda p: settle(1, p))


def mix(q_t, lat, w_uk, w_uv, w_o, n_tp, n_ctx, scale):
    heads, q_dim, q_count = q_t.shape
    keys, rank = lat.shape[0], w_uk.shape[0]
    nope = w_uk.shape[1] // (2 * heads)
    rope = q_dim - nope
    v_dim = w_uv.shape[1] // (2 * heads)
    n_hp = heads // 2
    depth, width = w_o.shape
    n_blk = width // OUT_BLOCK
    half = q_count // 4
    rows = half // n_tp
    assert n_tp == 4 and n_blk % 2 == 0 and width % OUT_BLOCK == 0
    assert q_count == 2 * KEY_BLOCK and keys == n_ctx * KEY_BLOCK
    bf16, f32 = jnp.bfloat16, jnp.float32
    hbm = pl.BlockSpec(memory_space=pl.ANY)
    dma = pltpu.SemaphoreType.DMA
    return pl.pallas_call(
        functools.partial(mix_kernel, n_tp, n_ctx, n_blk, scale),
        out_shape=jax.ShapeDtypeStruct((2 * half, width), bf16),
        in_specs=[hbm] * 5,
        out_specs=hbm,
        scratch_shapes=[
            pltpu.VMEM(q_t.shape, bf16), pltpu.VMEM(lat.shape, bf16), dma((2,)),
            pltpu.VMEM((n_hp, rank, 2 * nope), bf16), pltpu.VMEM((n_hp, rank, 2 * v_dim), bf16), pltpu.VMEM((n_hp, 2 * v_dim, rank), bf16),
            pltpu.VMEM((rank, keys), bf16), pltpu.VMEM((2, keys, nope + rope), bf16), pltpu.VMEM((2 * v_dim, keys), bf16),
            pltpu.VMEM((2, keys, KEY_BLOCK), f32), pltpu.VMEM((keys, 2 * KEY_BLOCK), bf16),
            pltpu.VMEM((q_count, heads * v_dim), bf16), pltpu.VMEM((2, 2, half, depth // 2), bf16),
            pltpu.VMEM((W_SLOTS, depth, OUT_BLOCK), bf16),
            pltpu.VMEM((2, n_blk, n_tp, rows, OUT_BLOCK), f32),
            pltpu.VMEM((2, n_blk, n_tp - 1, rows, OUT_BLOCK), f32),
            pltpu.VMEM((2, n_tp, n_blk, rows, OUT_BLOCK), bf16),
            dma((2, n_hp)), dma((W_SLOTS,)), dma((2,)), dma((2,)), dma((2, n_blk, n_tp - 1)), dma((2, n_blk, n_tp - 1)),
            dma((2, n_blk, 3)), dma((2, n_blk, 3)), dma((2, n_tp, n_blk)),
        ],
        compiler_params=pltpu.CompilerParams(collective_id=1, has_side_effects=True, vmem_limit_bytes=63 * 1024 * 1024),
        name='mix',
    )(q_t, lat, w_uk, w_uv, w_o)


K_CHUNKS = 4
Q_BLOCK = 256


def latent_kernel(n_ctx, x_hbm, wdkv_hbm, wkr_hbm, wdq_hbm, wuq_hbm, wqr_hbm, gain_ref, tab_ref, lat_hbm, q_ref,
                  x_v, wdkv, wkr, wdq, wuq, wqr, kv_acc, kr_acc, cq_acc, cq_all, tab_all, lat,
                  x_sem, dkv_sem, kr_sem, dq_sem, uq_sem, qr_sem, ring_send, ring_recv, mate_send, mate_recv, cq_send, cq_recv, tab_send, tab_recv, lat_sem):
    me = lax.axis_index('ctx')
    part = lax.rem(me, 2)
    mate = me + 1 - 2 * part
    right = lax.rem(me + 2, n_ctx)
    left = lax.rem(me + n_ctx - 2, n_ctx)
    far = lax.rem(me + 4, n_ctx)
    f32 = jnp.float32
    rows, width = x_v.shape
    half = rows // 2
    rank = kv_acc.shape[1]
    rope = kr_acc.shape[1]
    rot = rope // 2
    kc = width // K_CHUNKS
    n_uq, n_qr = wuq.shape[0], wqr.shape[0]
    nope = q_ref.shape[1] - rope

    def kcols(k):
        return pl.ds(k * kc, kc)

    x_copy = [pltpu.make_async_copy(x_hbm.at[:, kcols(k)], x_v.at[:, kcols(k)], x_sem.at[k]) for k in range(K_CHUNKS)]
    dkv_copy = [pltpu.make_async_copy(wdkv_hbm.at[kcols(k)], wdkv.at[kcols(k)], dkv_sem.at[k]) for k in range(K_CHUNKS)]
    kr_copy = [pltpu.make_async_copy(wkr_hbm.at[:, kcols(k)], wkr.at[:, kcols(k)], kr_sem.at[k]) for k in range(K_CHUNKS)]
    dq_copy = [pltpu.make_async_copy(wdq_hbm.at[kcols(k)], wdq.at[kcols(k)], dq_sem.at[k]) for k in range(K_CHUNKS)]
    uq_copy = [pltpu.make_async_copy(wuq_hbm.at[:, pl.ds(pl.multiple_of((part * n_uq + b) * Q_BLOCK, Q_BLOCK), Q_BLOCK)], wuq.at[b], uq_sem.at[b]) for b in range(n_uq)]
    qr_copy = [pltpu.make_async_copy(wqr_hbm.at[:, pl.ds(pl.multiple_of((part * n_qr + b) * Q_BLOCK, Q_BLOCK), Q_BLOCK)], wqr.at[b], qr_sem.at[b]) for b in range(n_qr)]

    def piece(dev, sub):
        return dev if sub == 0 else 2 * n_ctx - 1 - dev

    def send(src, dst, send_sem, recv_sem, dev):
        return pltpu.make_async_remote_copy(src_ref=src, dst_ref=dst, send_sem=send_sem, recv_sem=recv_sem, device_id={'ctx': dev}, device_id_type=MESH)

    def ring(slot, src_dev, sub, dev):
        return send(lat.at[piece(src_dev, sub)], lat.at[piece(src_dev, sub)], ring_send.at[slot], ring_recv.at[slot], dev)

    def share(slot, src_dev, sub):
        return send(lat.at[piece(src_dev, sub)], lat.at[piece(src_dev, sub)], mate_send.at[slot], mate_recv.at[slot], mate)

    to_right = [ring(0, me, 0, right), ring(1, me, 1, right)]
    to_left = [ring(2, me, 0, left), ring(3, me, 1, left)]
    on_right = ring(4, left, 0, right)
    on_left = ring(5, right, 1, left)
    order = [(me, 0), (me, 1), (left, 0), (right, 1), (left, 1), (right, 0), (far, 0), (far, 1)]
    shares = [share(i, d, s) for i, (d, s) in enumerate(order)]
    slot_of = (part, 3 - part)
    cq_share = [send(cq_all.at[slot_of[s]], cq_all.at[slot_of[s]], cq_send.at[s], cq_recv.at[s], mate) for s in range(2)]

    def lanes(s):
        return pl.ds(pl.multiple_of(slot_of[s] * half, half), half)

    tab_share = [send(tab_all.at[:, lanes(s)], tab_all.at[:, lanes(s)], tab_send.at[s], tab_recv.at[s], mate) for s in range(2)]

    def fetch(k):
        if k < K_CHUNKS:
            group = [x_copy[k], dkv_copy[k], kr_copy[k]]
        elif k < 2 * K_CHUNKS:
            group = [dq_copy[k - K_CHUNKS]]
        else:
            group = qr_copy if k == 2 * K_CHUNKS else uq_copy
        for c in group:
            c.start()

    fetch(0)
    fetch(1)
    barrier = pltpu.get_barrier_semaphore()
    for dev in (mate, right, left):
        pl.semaphore_signal(barrier, inc=1, device_id={'ctx': dev}, device_id_type=MESH)
    for s in range(2):
        tab_all[:, lanes(s)] = tab_ref[s * half:(s + 1) * half].T[0:rope]

    for k in range(K_CHUNKS):
        cols = slice(k * kc, (k + 1) * kc)
        x_copy[k].wait()
        dkv_copy[k].wait()
        kr_copy[k].wait()
        fetch(k + 2)
        kv_new = jnp.dot(x_v[:, cols], wdkv[cols], preferred_element_type=f32)
        kr_new = lax.dot_general(x_v[:, cols], wkr[:, cols], (((1,), (1,)), ((), ())), preferred_element_type=f32)
        if k == 0:
            kv_acc[...] = kv_new
            kr_acc[...] = kr_new
        else:
            kv_acc[...] += kv_new
            kr_acc[...] += kr_new
    kv = kv_acc[...]
    c_kv = (kv * lax.rsqrt(jnp.mean(kv * kv, axis=-1, keepdims=True) + NORM_EPS) * gain_ref[0:1, 0:rank]).astype(jnp.bfloat16)
    kr = kr_acc[...]
    cos_k, sin_k = tab_ref[:, :rot], tab_ref[:, rot:rope]
    k_lo = (kr[:, :rot] * cos_k - kr[:, rot:] * sin_k).astype(jnp.bfloat16)
    k_hi = (kr[:, rot:] * cos_k + kr[:, :rot] * sin_k).astype(jnp.bfloat16)
    pad = jnp.zeros((half, lat.shape[2] - rank - rope), jnp.bfloat16)
    for s in range(2):
        own = slice(s * half, (s + 1) * half)
        lat[piece(me, s), :, 0:rank] = c_kv[own]
        lat[piece(me, s), :, rank:] = jnp.concatenate([k_lo[own], k_hi[own], pad], axis=1)

    pl.semaphore_wait(barrier, 3)
    for s in range(2):
        to_right[s].start()
        to_left[1 - s].start()
    for s in range(2):
        tab_share[s].start()
        shares[s].start()

    for k in range(K_CHUNKS):
        cols = slice(k * kc, (k + 1) * kc)
        dq_copy[k].wait()
        fetch(K_CHUNKS + k + 2)
        cq_new = jnp.dot(x_v[:, cols], wdq[cols], preferred_element_type=f32)
        if k == 0:
            cq_acc[...] = cq_new
        else:
            cq_acc[...] += cq_new
    for s in range(2):
        own = slice(s * half, (s + 1) * half)
        cq = cq_acc[own]
        cq_all[slot_of[s]] = (cq * lax.rsqrt(jnp.mean(cq * cq, axis=-1, keepdims=True) + NORM_EPS) * gain_ref[0:1, rank:]).astype(jnp.bfloat16)
        cq_share[s].start()

    to_right[0].wait_recv()
    on_right.start()
    to_left[1].wait_recv()
    on_left.start()
    shares[2].start()
    shares[3].start()
    for s in range(2):
        cq_share[s].wait_recv()
        tab_share[s].wait_recv()

    def rotary(b, _):
        pltpu.make_async_copy(wqr_hbm.at[:, pl.ds(0, Q_BLOCK)], wqr.at[b], qr_sem.at[b]).wait()
        res = jnp.dot(cq_all[...].reshape(2 * rows, cq_all.shape[2]), wqr[b], preferred_element_type=f32).T
        cos_q, sin_q = tab_all[0:rot], tab_all[rot:rope]
        for i in range(Q_BLOCK // rope):
            lo = res[i * rope:i * rope + rot]
            hi = res[i * rope + rot:(i + 1) * rope]
            h = b * (Q_BLOCK // rope) + i
            q_ref[h, nope:nope + rot, :] = (lo * cos_q - hi * sin_q).astype(jnp.bfloat16)
            q_ref[h, nope + rot:nope + rope, :] = (hi * cos_q + lo * sin_q).astype(jnp.bfloat16)
        return 0

    lax.fori_loop(0, n_qr, rotary, 0)
    to_right[1].wait_recv()
    to_left[0].wait_recv()
    shares[4].start()
    shares[5].start()

    def plain(b, _):
        pltpu.make_async_copy(wuq_hbm.at[:, pl.ds(0, Q_BLOCK)], wuq.at[b], uq_sem.at[b]).wait()
        res = jnp.dot(cq_all[...].reshape(2 * rows, cq_all.shape[2]), wuq[b], preferred_element_type=f32).astype(jnp.bfloat16).T
        for i in range(Q_BLOCK // nope):
            q_ref[b * (Q_BLOCK // nope) + i, 0:nope, :] = res[i * nope:(i + 1) * nope]
        return 0

    lax.fori_loop(0, n_uq // 2, plain, 0)
    on_right.wait_recv()
    on_left.wait_recv()
    shares[6].start()
    shares[7].start()
    lax.fori_loop(n_uq // 2, n_uq, plain, 0)
    for i in range(8):
        shares[i].wait_recv()
    out = pltpu.make_async_copy(lat, lat_hbm, lat_sem)
    out.start()
    for c in to_right + to_left + [on_right, on_left] + shares + cq_share + tab_share:
        c.wait_send()
    out.wait()


def latents(tok_x, w_dkv, w_kr, w_dq, w_uq, w_qr, g_q, g_kv, tab, n_ctx):
    rows, width = tok_x.shape
    rank, rope, q_rank = w_dkv.shape[1], w_kr.shape[1], w_dq.shape[1]
    heads = w_qr.shape[1] // rope // 2
    nope = w_uq.shape[1] // heads // 2
    bf16, f32 = jnp.bfloat16, jnp.float32
    vmem = pl.BlockSpec(memory_space=pltpu.VMEM)
    hbm = pl.BlockSpec(memory_space=pl.ANY)
    dma = pltpu.SemaphoreType.DMA
    n_uq, n_qr = heads * nope // Q_BLOCK, heads * rope // Q_BLOCK
    lat_width = rank + 128
    assert n_ctx == 8 and rope <= 128
    gain = jnp.broadcast_to(jnp.concatenate([g_kv, g_q]).astype(f32)[None], (8, rank + q_rank))
    lat, q_t = pl.pallas_call(
        functools.partial(latent_kernel, n_ctx),
        out_shape=[jax.ShapeDtypeStruct((2 * n_ctx, rows // 2, lat_width), bf16), jax.ShapeDtypeStruct((heads, nope + rope, 2 * rows), bf16)],
        in_specs=[hbm] * 6 + [vmem] * 2,
        out_specs=[hbm, vmem],
        scratch_shapes=[
            pltpu.VMEM((rows, width), bf16), pltpu.VMEM((width, rank), bf16), pltpu.VMEM((rope, width), bf16), pltpu.VMEM((width, q_rank), bf16),
            pltpu.VMEM((n_uq, q_rank, Q_BLOCK), bf16), pltpu.VMEM((n_qr, q_rank, Q_BLOCK), bf16),
            pltpu.VMEM((rows, rank), f32), pltpu.VMEM((rows, rope), f32), pltpu.VMEM((rows, q_rank), f32),
            pltpu.VMEM((4, rows // 2, q_rank), bf16), pltpu.VMEM((rope, 2 * rows), f32), pltpu.VMEM((2 * n_ctx, rows // 2, lat_width), bf16),
            dma((K_CHUNKS,)), dma((K_CHUNKS,)), dma((K_CHUNKS,)), dma((K_CHUNKS,)), dma((n_uq,)), dma((n_qr,)),
            dma((6,)), dma((6,)), dma((8,)), dma((8,)), dma((2,)), dma((2,)), dma((2,)), dma((2,)), dma,
        ],
        compiler_params=pltpu.CompilerParams(collective_id=2, has_side_effects=True, vmem_limit_bytes=62 * 1024 * 1024),
        name='latents',
    )(tok_x, w_dkv, w_kr.T, w_dq, w_uq, w_qr, gain, tab)
    return lat.reshape(n_ctx * rows, lat_width), q_t


def solution(mesh):
    tok_spec = P(('dp', 'ctx'), None)
    pos_spec = P(('dp', 'ctx'))
    full_mat = P(None, None)
    full_vec = P(None)
    col_spec = P(None, 'tp')
    row_spec = P('tp', None)

    def local_step(tok_x, tok_pos, w_dq, g_q, w_uq, w_qr, w_dkv, g_kv, w_kr, w_uk, w_uv, w_o):
        rope_dim = w_kr.shape[1]
        heads_loc = w_qr.shape[1] // rope_dim
        nope_dim = w_uq.shape[1] // heads_loc
        score_scale = (nope_dim + rope_dim) ** -0.5
        n_ctx = mesh.shape['ctx']
        tab = rope_table(tok_pos, rope_dim)
        lat, q_t = latents(tok_x, w_dkv, w_kr, w_dq, w_uq, w_qr, g_q, g_kv, tab, n_ctx)
        return mix(q_t, lat, w_uk, w_uv, w_o, mesh.shape['tp'], n_ctx, score_scale)

    return jax.shard_map(local_step, mesh=mesh,
                         in_specs=(tok_spec, pos_spec, full_mat, full_vec, col_spec, col_spec, full_mat, full_vec, full_mat, col_spec, col_spec, row_spec),
                         out_specs=tok_spec, check_vma=False)
```
